32 devices in a mesh: genome: 8 (over z, x), anc: 4 (over y, core), trait: 1.
Axes of the slice: x: 2, y: 2, z: 4, core: 2. Of those that a mesh axis runs over, the one named last changes fastest.
Arguments:
- coefficients: float32 [4, 128, 16384], P('anc', 'trait', 'genome'), may hold values from -3 to 3
- sumstats: float32 [4, 128, 16384], P('anc', 'trait', 'genome'), may hold values from -12 to 12
- linkage: bfloat16 [4, 16384, 4096], P('anc', 'genome'), may hold values from -0.09375 to 0.09375
- band_start: int32 [4, 64], P('anc', 'genome'), may hold values from 0 to 12288, as said below
- group_ids: int32 [4, 16384], P('anc', 'genome'), may hold values from 0 to 15, never falling along the last dimension, each value on 1 to 8192 neighbouring positions
- group_weight: float32 [4, 16], P('anc'), may hold values from 0.1 to 1.5
- dosage: bfloat16 [4, 2048, 16384], P('anc', None, 'genome'), may hold values from 0 to 2
Outputs:
- updated: float32 [4, 128, 16384], P('anc', 'trait', 'genome')
- scores: float32 [4, 128, 2048], P('anc', 'trait', 'genome')
The draws below stay inside these ranges and needn't reach their ends.
Inputs may be any that keep to these rules, and one draw needn't show every extreme that they name: band_start[a, u] is the first of the 4096 consecutive SNP columns stored in linkage[a] for row block u, the SNPs u * 256 to u * 256 + 255; these columns always include the block's own SNPs. `group_ids`: group ids never fall along the SNPs of an ancestry, so each group is one run of consecutive SNPs.
All inputs are finite; a program needn't handle non-finite values.
Results may differ from the reference program's by a relative error of at most 0.003.
Values may be sent and summed in bfloat16 or wider, within the bound.
A program may use at most 128 MiB of HBM per device.

```python
import math
import jax
import jax.numpy as jnp
import numpy as np
from jax import lax

TRAITS = 128
ANC = 4
W = 4096
TILE = 256
M_DEV = 2048
PERSONS = 2048
SNPS = 16384
GROUPS = 16


def draw_band_start(key, part):
    block_count = SNPS // TILE
    spare = W - TILE
    anchors = jnp.arange(block_count, dtype=jnp.int32) * TILE
    jitter = jax.random.randint(key, (ANC, block_count), 0, spare + 1, dtype=jnp.int32)
    raw_start = anchors[None, :] - jitter
    return jnp.minimum(jnp.maximum(raw_start, 0), SNPS - W).astype(jnp.int32)


def draw_sumstats(key, part):
    block_count = SNPS // TILE
    key_noise = jax.random.fold_in(key, 11)
    key_scale = jax.random.fold_in(key, 23)
    noise = jnp.clip(jax.random.normal(key_noise, (ANC, TRAITS, SNPS), jnp.float32), -4.0, 4.0)
    block_scale = jnp.exp(jax.random.uniform(key_scale, (ANC, 1, block_count), jnp.float32, -0.69, 0.69))
    block_scale = jnp.repeat(block_scale, TILE, axis=2)
    trend = 3.0 ** (jnp.arange(SNPS, dtype=jnp.float32) / SNPS)
    return (0.5 * noise * block_scale * trend[None, None, :]).astype(jnp.float32)


def levels(key, shape, shards, smallest, largest):
    def one(axis_at, blocks):
        draws = jax.random.uniform(jax.random.fold_in(jax.random.fold_in(key, 6), axis_at), (blocks,), jnp.float32, smallest / len(shards), largest / len(shards))
        return jnp.repeat(jnp.exp(draws), shape[axis_at] // blocks).reshape((-1,) + (1,) * (len(shape) - axis_at - 1))

    level = one(*shards[0])
    for cut in shards[1:]:
        level = level * one(*cut)
    return level


def length_profile(number_of, total, most, lean):
    weights = [(1 << 20) // math.isqrt(rank ** lean) + 1 for rank in range(2, number_of + 1)]
    surplus, given = total - most - (number_of - 1), [1] * (number_of - 1)
    while surplus > 0:
        movable = [i for i in range(number_of - 1) if given[i] < most]
        mass, budget = sum([weights[i] for i in movable]), surplus
        for i in movable:
            extra = min(most - given[i], max(1, budget * weights[i] // mass), surplus)
            given[i] = given[i] + extra
            surplus = surplus - extra
    return np.array([most] + given)


def ragged_sizes(rng, count, total, bound, lean):
    if count == 2:
        one = jax.random.randint(rng, (), max(1, total - bound), min(bound, total - 1) + 1)
        return jnp.stack([one, total - one])
    tallies = jnp.asarray(length_profile(count, total, bound, lean), jnp.int32)
    couples = (count - 1) // 2
    source_of, taker = tallies[1:1 + 2 * couples:2], tallies[2:2 + 2 * couples:2]
    margin = jnp.minimum(source_of - 1, bound - taker)
    shifted = jax.random.randint(jax.random.fold_in(rng, 1), (couples,), 0, 1 << 20) % (margin + 1)
    tallies = tallies.at[1:1 + 2 * couples:2].set(source_of - shifted).at[2:2 + 2 * couples:2].set(taker + shifted)
    return tallies[jax.random.permutation(jax.random.fold_in(rng, 2), count)]


def gaussian(key, shape, scale, most, split=(), kind=jnp.bfloat16):
    entries = jax.random.normal(key, shape, jnp.float32) * scale
    if len(split) > 0:
        entries = levels(key, shape, split, -0.22, 0.18) * entries
    return jnp.clip(entries, min=-most, max=most).astype(kind)


def setup_inputs(seed: int = 0) -> dict:
    splits = jax.random.split(jax.random.key(seed), 8)
    coefficients = gaussian(splits[0], (ANC, TRAITS, SNPS), 0.5, 3.0, ((0, 4), (2, 8)), jnp.float32)
    sumstats = draw_sumstats(jax.random.fold_in(splits[7], 71), 0)
    linkage = gaussian(splits[2], (ANC, SNPS, W), W ** -0.5, 0.09375, ((0, 4), (1, 8)))
    band_start = draw_band_start(jax.random.fold_in(splits[7], 71), 0)
    group_ids = jax.vmap(lambda own: jnp.searchsorted(jnp.cumsum(ragged_sizes(own, GROUPS, SNPS, 4 * M_DEV, 2)), jnp.arange(SNPS), side="right"))(jax.random.split(splits[4], ANC)).reshape((ANC, SNPS)).astype(jnp.int32)
    group_weight = jnp.clip(jnp.exp(math.log(1.5) - 2.7080502 * jax.random.uniform(splits[5], (ANC, GROUPS), jnp.float32) ** levels(splits[5], (ANC, GROUPS), ((0, 4),), -0.2, 0.2)), 0.1, 1.5)
    dosage = jnp.clip(2.0 * jax.random.uniform(splits[6], (ANC, PERSONS, SNPS), jnp.float32) ** levels(splits[6], (ANC, PERSONS, SNPS), ((0, 4), (2, 8)), -0.2, 0.2), 0.0, 2.0).astype(jnp.bfloat16)
    return dict(coefficients=coefficients, sumstats=sumstats, linkage=linkage, band_start=band_start, group_ids=group_ids, group_weight=group_weight, dosage=dosage)


step_size = 0.5
merging = 0.5
epsilon = 1e-06

def band_apply(low_copy, band, starts):
    padded = jnp.pad(low_copy.astype(jnp.float32), ((0, 0), (W, W)))
    band_tiles = band.reshape(SNPS // TILE, TILE, W)

    def per_tile(tile_item):
        block_rows, begin_at = tile_item
        window = lax.dynamic_slice_in_dim(padded, (begin_at + W).astype(jnp.int32), W, 1)
        return jnp.dot(window, block_rows.astype(jnp.float32).T, precision=lax.Precision.HIGHEST)
    products = lax.map(per_tile, (band_tiles, starts))
    return jnp.transpose(products, (1, 0, 2)).reshape(TRAITS, SNPS)

def reference(coefficients, sumstats, linkage, band_start, group_ids, group_weight, dosage):
    mean_coef = lax.optimization_barrier(jnp.sum(coefficients, axis=0)) / ANC
    update_list = []
    score_list = []
    for ancestry in range(ANC):
        current = coefficients[ancestry]
        band_product = band_apply(current.astype(jnp.bfloat16), linkage[ancestry], band_start[ancestry])
        gradient = current + band_product - sumstats[ancestry] + merging * (current - mean_coef)
        proposal = current - step_size * gradient
        trait_total = lax.optimization_barrier(jnp.sum(proposal * proposal, axis=0))
        group_list = group_ids[ancestry]
        squares = jax.ops.segment_sum(trait_total, group_list, num_segments=GROUPS)
        counts = jax.ops.segment_sum(jnp.ones_like(trait_total), group_list, num_segments=GROUPS)
        threshold = step_size * group_weight[ancestry] * jnp.sqrt(counts * TRAITS)
        factor = jnp.maximum(0.0, 1.0 - threshold / jnp.sqrt(squares + epsilon))
        updated = proposal * factor[group_list][None, :]
        genotype = dosage[ancestry]
        scores = jnp.dot(updated.astype(jnp.bfloat16), genotype.T, preferred_element_type=jnp.float32) / math.sqrt(SNPS)
        update_list.append(updated)
        score_list.append(scores)
    return (jnp.stack(update_list), jnp.stack(score_list))
```

```python
import functools
import math

import jax
import jax.numpy as jnp
from jax import lax
from jax.experimental import pallas as pl
from jax.experimental.pallas import tpu as pltpu
from jax.sharding import PartitionSpec as P

step_size = 0.5
merging = 0.5
epsilon = 1e-06
longest_run = 8192

MESH = pl.DeviceIdType.MESH
F32 = jnp.float32
BF16 = jnp.bfloat16


def step_kernel(
    sizes,
    coef_hbm, sums_hbm, link_hbm, starts_hbm, ids_hbm, weight_hbm, dosage_hbm,
    updated_ref, score_ref,
    coef, sums, link, starts_ref, ids_ref, weight_ref, dosage, ext, extf, pair, mean, pair_out, pair_in,
    proposal, low, row, stats_out, stats_in, side_out, side_in, part_out, part_in,
    coef_sem, load_sem, link_sem, ready,
    halo_send, halo_recv, pair_send, pair_recv, stats_send, stats_recv, side_send, side_recv, part_send, part_recv,
):
    genomes, ancs, traits_n, reach, tile, groups = sizes
    traits_here, snps = coef.shape
    width = link.shape[1]
    tiles = snps // tile
    persons_per = part_out.shape[2]
    pairs = genomes // 2
    g = lax.axis_index("genome")
    a = lax.axis_index("anc")
    t = lax.axis_index("trait")
    core, side = lax.rem(a, 2), a // 2
    parity = lax.rem(g, 2)
    even = 1 - 2 * parity
    near, far, back, across = g + even, g + 2 * even, g - 2 * even, g - even

    def in_range(p):
        return jnp.logical_and(p >= 0, p < genomes)

    def genome(p):
        return {"genome": jnp.clip(p, 0, genomes - 1)}

    group_reach = min(-(-longest_run // snps), genomes - 1)
    stat_peers = [
        (d, m) for m in range(traits_n) for d in range(-group_reach, group_reach + 1) if (d, m) != (0, 0)
    ]
    if genomes > 8 or traits_n > 1:
        greet = [(k, m) for m in range(traits_n) for k in range(genomes) if (k, m) != (0, 0)]
    else:
        greet = []

    coef_parts = coef_sem.shape[0]
    part_cols = snps // coef_parts

    def coef_copy(i):
        cols = pl.ds(i * part_cols, part_cols)
        return pltpu.make_async_copy(coef_hbm.at[0, :, cols], coef.at[:, cols], coef_sem.at[i])

    for i in range(coef_parts):
        coef_copy(i).start()
    barrier = pltpu.get_barrier_semaphore()
    if greet:
        for k, m in greet:
            pl.semaphore_signal(
                barrier, inc=1, device_id_type=MESH,
                device_id={"genome": lax.rem(g + k, genomes), "trait": lax.rem(t + m, traits_n)},
            )
        expected = len(greet)
    else:
        pl.semaphore_signal(barrier, inc=1, device_id=genome(near), device_id_type=MESH)
        for peer in (far, back):
            @pl.when(in_range(peer))
            def _(peer=peer):
                pl.semaphore_signal(barrier, inc=1, device_id=genome(peer), device_id_type=MESH)
        expected = 1 + in_range(far).astype(jnp.int32) + in_range(back).astype(jnp.int32)

    @pl.when(core == 0)
    def _():
        pl.semaphore_signal(barrier, inc=1, device_id={"anc": a + 1}, device_id_type=MESH)

    @pl.when(jnp.logical_and(core == 1, side == 1))
    def _():
        pl.semaphore_signal(barrier, inc=1, device_id={"anc": a - 2}, device_id_type=MESH)

    expected = expected + core + core * (1 - side)

    load_small = [
        pltpu.make_async_copy(starts_hbm, starts_ref, load_sem.at[0]),
        pltpu.make_async_copy(ids_hbm, ids_ref, load_sem.at[1]),
        pltpu.make_async_copy(weight_hbm, weight_ref, load_sem.at[2]),
    ]
    load_sums = pltpu.make_async_copy(sums_hbm.at[0], sums, load_sem.at[3])
    load_dosage = pltpu.make_async_copy(dosage_hbm.at[0], dosage, load_sem.at[4])

    def link_copy(u):
        rows = pl.ds(pl.multiple_of(u * tile, tile), tile)
        return pltpu.make_async_copy(link_hbm.at[0, rows, :], link.at[rows, :], link_sem.at[u])

    def own_block(u, carry):
        cols = pl.ds(pl.multiple_of(u * tile, tile), tile)
        flat = coef[:, cols].T.astype(BF16)
        ext[reach, cols, :] = flat
        extf[pl.ds(pl.multiple_of(reach * snps + u * tile, tile), tile), :] = flat.astype(F32)
        return carry

    for i in range(coef_parts):
        coef_copy(i).wait()
        lax.fori_loop(i * tiles // coef_parts, (i + 1) * tiles // coef_parts, own_block, 0, unroll=2)

    unit = snps // 16
    far_rows = width - tile - snps
    f_rows, n_rows = 9 * unit, 7 * unit
    rest = far_rows - n_rows
    half_far = far_rows // 2

    def piece(p, odd):
        f_base, n_base = (1 - odd) * n_rows, odd * f_rows
        if p < 3:
            at, size = f_base + p * 3 * unit, 3 * unit
        elif p == 3:
            at, size = n_base, 4 * unit
        elif p == 4:
            at, size = n_base + 4 * unit, 3 * unit
        elif p == 5:
            at, size = (1 - odd) * n_rows + odd * (snps - far_rows), rest
        else:
            at, size = (1 - odd) * (snps - far_rows) + (p - 6) * half_far, half_far
        return pl.multiple_of(at, unit), size

    def halo_copy(src_slot, dst_slot, p, odd, peer, send):
        at, size = piece(p, odd)
        rows = pl.ds(at, size)
        return pltpu.make_async_remote_copy(
            src_ref=ext.at[src_slot, rows, :], dst_ref=ext.at[dst_slot, rows, :],
            send_sem=halo_send.at[send], recv_sem=halo_recv.at[dst_slot, p],
            device_id=genome(peer), device_id_type=MESH,
        )

    def near_copy(p):
        return halo_copy(reach, reach - even, p, parity, near, p)

    def back_copy(p):
        return halo_copy(reach, reach + 2 * even, p, parity, back, 5 + p - 3)

    def far_copy(p):
        return halo_copy(reach, reach - 2 * even, p, parity, far, 8 + p - 6)

    def relay_far(p):
        return halo_copy(reach + even, reach - even, p, 1 - parity, far, 10 + p)

    def relay_near(p):
        return halo_copy(reach + 2 * even, reach + even, p, parity, near, 13 + p - 3)

    def arrived(slot, p, odd):
        halo_copy(reach, slot, p, odd, near, 0).wait_recv()

    has_far, has_back = in_range(far), in_range(back)

    pl.semaphore_wait(barrier, expected)

    def start_back(p):
        @pl.when(has_back)
        def _():
            back_copy(p).start()

    def start_far(p):
        @pl.when(has_far)
        def _():
            far_copy(p).start()

    near_copy(0).start()
    start_back(3)
    start_far(6)
    near_copy(1).start()
    start_back(4)
    start_far(7)
    near_copy(2).start()
    start_back(5)
    near_copy(3).start()
    near_copy(4).start()

    @pl.when(core == 1)
    def _():
        pl.semaphore_signal(ready, inc=1, device_id={"anc": a - 1}, device_id_type=MESH)

    @pl.when(jnp.logical_and(core == 1, side == 0))
    def _():
        pl.semaphore_signal(ready, inc=1, device_id={"anc": a + 2}, device_id_type=MESH)

    for load in load_small:
        load.start()
    load_sums.start()
    for u in range(tiles):
        link_copy(u).start()
    load_dosage.start()

    other_core = {"anc": a + 1 - 2 * core}
    other_side = {"anc": lax.rem(a + 2, ancs)}
    up_copy = pltpu.make_async_remote_copy(
        src_ref=coef, dst_ref=pair, send_sem=pair_send.at[0], recv_sem=pair_recv.at[0],
        device_id=other_core, device_id_type=MESH,
    )
    over_copy = pltpu.make_async_remote_copy(
        src_ref=pair_out, dst_ref=pair_in, send_sem=pair_send.at[1], recv_sem=pair_recv.at[1],
        device_id=other_side, device_id_type=MESH,
    )
    down_copy = pltpu.make_async_remote_copy(
        src_ref=mean, dst_ref=mean, send_sem=pair_send.at[2], recv_sem=pair_recv.at[2],
        device_id=other_core, device_id_type=MESH,
    )

    chunk = unit

    def widen(slot, p, odd):
        at, size = piece(p, odd)

        def part(i, carry):
            r = pl.multiple_of(at + i * chunk, chunk)
            extf[pl.ds(pl.multiple_of(slot * snps + r, chunk), chunk), :] = ext[slot, pl.ds(r, chunk), :].astype(F32)
            return carry

        lax.fori_loop(0, size // chunk, part, 0)

    def clear(slot):
        def part(i, carry):
            at = pl.multiple_of(slot * snps + i * chunk, chunk)
            extf[pl.ds(at, chunk), :] = jnp.zeros((chunk, traits_here), F32)
            return carry

        lax.fori_loop(0, snps // chunk, part, 0)

    for d in (-1, 1):
        @pl.when(jnp.logical_not(in_range(g + d)))
        def _(d=d):
            clear(reach + d)

    clear(0)
    clear(2 * reach)

    for i, (d, m) in enumerate(stat_peers):
        @pl.when(jnp.logical_not(in_range(g - d)))
        def _(i=i):
            stats_in[i] = jnp.zeros(stats_in.shape[1:], F32)

    def pass_on(p):
        if p < 3:
            arrived(reach + even, p, 1 - parity)

            @pl.when(has_far)
            def _():
                relay_far(p).start()
        else:
            @pl.when(has_far)
            def _():
                arrived(reach + 2 * even, p, parity)
                relay_near(p).start()

    pass_on(0)
    pass_on(3)

    @pl.when(core == 0)
    def _():
        pl.semaphore_wait(ready, 1)
        up_copy.start()

    pass_on(1)
    pass_on(4)

    @pl.when(core == 1)
    def _():
        up_copy.wait_recv()

        def add(u, carry):
            cols = pl.ds(pl.multiple_of(u * tile, tile), tile)
            value = coef[:, cols] + pair[:, cols]
            pair[:, cols] = value
            pair_out[:, cols] = value.astype(BF16)
            return carry

        lax.fori_loop(0, tiles, add, 0)

        @pl.when(side == 1)
        def _():
            pl.semaphore_wait(ready, 1)

        over_copy.start()

    pass_on(2)
    for p in range(3):
        widen(reach + even, p, 1 - parity)

    @pl.when(has_far)
    def _():
        arrived(reach + 2 * even, 5, parity)
        for p in (3, 4, 5):
            widen(reach + 2 * even, p, parity)

    for p in (3, 4):
        arrived(reach + even, p, 1 - parity)
        widen(reach + even, p, 1 - parity)

    @pl.when(has_back)
    def _():
        for p in (6, 7):
            arrived(reach - 2 * even, p, parity)
            widen(reach - 2 * even, p, parity)

    @pl.when(core == 1)
    def _():
        over_copy.wait_recv()

        def add(u, carry):
            cols = pl.ds(pl.multiple_of(u * tile, tile), tile)
            mean[:, cols] = (pair[:, cols] + pair_in[:, cols].astype(F32)) / ancs
            return carry

        lax.fori_loop(0, tiles, add, 0)
        down_copy.start()

    @pl.when(core == 0)
    def _():
        down_copy.wait_recv()

    load_sums.wait()
    for load in load_small:
        load.wait()

    def prepare(u, carry):
        cols = pl.ds(pl.multiple_of(u * tile, tile), tile)
        proposal[:, cols] = (
            (1.0 - step_size - step_size * merging) * coef[:, cols]
            + step_size * sums[:, cols] + (step_size * merging) * mean[:, cols]
        )
        return carry

    lax.fori_loop(0, tiles, prepare, 0)

    @pl.when(has_back)
    def _():
        for p in range(5):
            arrived(reach - even, p, 1 - parity)
            widen(reach - even, p, 1 - parity)

    def band_tile(u, carry):
        link_copy(u).wait()
        rows = pl.ds(pl.multiple_of(u * tile, tile), tile)
        begin = jnp.clip(starts_ref[0, u] - g * snps + reach * snps, 0, extf.shape[0] - width)
        depth = 512
        total = jnp.zeros((tile, traits_here), F32)
        for c in range(0, width, depth):
            window = extf[pl.ds(begin + c, depth), :].astype(BF16)
            total = total + jnp.dot(
                link[rows, c:c + depth], window, preferred_element_type=F32
            )
        value = proposal[:, rows] - step_size * total.T
        proposal[:, rows] = value
        row[:, rows] = jnp.sum(value * value, axis=0, keepdims=True)
        return carry

    lax.fori_loop(0, tiles, band_tile, 0, unroll=2)

    lanes = stats_out.shape[1]
    mine = lax.broadcasted_iota(jnp.int32, (groups, snps), 0) == ids_ref[...]
    squares = jnp.sum(jnp.where(mine, row[...], 0.0), axis=1, keepdims=True)
    counts = jnp.sum(jnp.where(mine, 1.0, 0.0), axis=1, keepdims=True)
    on_lane = lax.broadcasted_iota(jnp.int32, (groups, lanes), 0) == lax.broadcasted_iota(
        jnp.int32, (groups, lanes), 1
    )
    stats_out[0:1, :] = jnp.sum(jnp.where(on_lane, squares, 0.0), axis=0, keepdims=True)
    stats_out[1:2, :] = jnp.sum(jnp.where(on_lane, counts, 0.0), axis=0, keepdims=True)

    def stats_copy(i):
        d, m = stat_peers[i]
        return pltpu.make_async_remote_copy(
            src_ref=stats_out, dst_ref=stats_in.at[i],
            send_sem=stats_send.at[i], recv_sem=stats_recv.at[i],
            device_id={**genome(g + d), "trait": lax.rem(t + m, traits_n)}, device_id_type=MESH,
        )

    for i, (d, m) in enumerate(stat_peers):
        @pl.when(in_range(g + d))
        def _(i=i):
            stats_copy(i).start()

    load_dosage.wait()
    for i, (d, m) in enumerate(stat_peers):
        @pl.when(in_range(g - d))
        def _(i=i):
            stats_copy(i).wait_recv()

    stats = stats_out[...]
    for i in range(len(stat_peers)):
        stats = stats + stats_in[i]
    all_squares = stats[0:1, :groups]
    all_counts = stats[1:2, :groups] / traits_n
    threshold = step_size * weight_ref[...] * jnp.sqrt(all_counts * (traits_here * traits_n))
    shrink = jnp.maximum(0.0, 1.0 - threshold / jnp.sqrt(all_squares + epsilon))
    same = lax.broadcasted_iota(jnp.int32, (groups, groups), 0) == lax.broadcasted_iota(
        jnp.int32, (groups, groups), 1
    )
    shrink = jnp.sum(jnp.where(same, shrink, 0.0), axis=1, keepdims=True)
    row[...] = jnp.sum(jnp.where(mine, shrink, 0.0), axis=0, keepdims=True)

    def shrink_tile(u, carry):
        cols = pl.ds(pl.multiple_of(u * tile, tile), tile)
        value = proposal[:, cols] * row[:, cols]
        updated_ref[0, :, cols] = value
        low[:, cols] = value.astype(BF16)
        return carry

    lax.fori_loop(0, tiles, shrink_tile, 0, unroll=2)

    scale = 1.0 / math.sqrt(snps * genomes)
    own_side, other_side_g = parity, lax.rem(near, 2)

    def pair_at(i):
        k = pairs // 2 + (1 - 2 * lax.rem(i, 2)) * ((i + 1) // 2)
        return lax.rem(g // 2 + k + pairs, pairs)

    def partial(person):
        at = pl.ds(pl.multiple_of(person * persons_per, persons_per), persons_per)
        return lax.dot_general(
            low[...], dosage[at, :], (((1,), (1,)), ((), ())), preferred_element_type=F32
        ) * scale

    def side_copy(i):
        return pltpu.make_async_remote_copy(
            src_ref=side_out.at[i], dst_ref=side_in.at[i],
            send_sem=side_send.at[i], recv_sem=side_recv.at[i],
            device_id={"genome": near}, device_id_type=MESH,
        )

    def part_copy(i):
        return pltpu.make_async_remote_copy(
            src_ref=part_out.at[i], dst_ref=part_in.at[i],
            send_sem=part_send.at[i], recv_sem=part_recv.at[i],
            device_id={"genome": 2 * pair_at(i) + own_side}, device_id_type=MESH,
        )

    def send_side(i, carry):
        side_out[i] = partial(2 * pair_at(i) + other_side_g).astype(BF16)
        side_copy(i).start()
        return carry

    def pair_sum(i):
        mine_here = partial(2 * pair_at(i) + own_side)
        side_copy(i).wait_recv()
        return mine_here + side_in[i].astype(F32)

    def send_part(i, carry):
        part_out[i] = pair_sum(i).astype(BF16)
        part_copy(i).start()
        return carry

    lax.fori_loop(0, pairs, send_side, 0)
    lax.fori_loop(0, pairs - 1, send_part, 0)

    def add_part(i, total):
        part_copy(i).wait_recv()
        return total + part_in[i].astype(F32)

    score_ref[0] = lax.fori_loop(0, pairs - 1, add_part, pair_sum(pairs - 1))

    for p in range(5):
        near_copy(p).wait_send()

    @pl.when(has_back)
    def _():
        for p in (3, 4, 5):
            back_copy(p).wait_send()

    @pl.when(has_far)
    def _():
        for p in (6, 7):
            far_copy(p).wait_send()
        for p in (0, 1, 2):
            relay_far(p).wait_send()
        for p in (3, 4):
            relay_near(p).wait_send()

    @pl.when(core == 0)
    def _():
        up_copy.wait_send()

    @pl.when(core == 1)
    def _():
        over_copy.wait_send()
        down_copy.wait_send()

    for i, (d, m) in enumerate(stat_peers):
        @pl.when(in_range(g + d))
        def _(i=i):
            stats_copy(i).wait_send()

    def sent_side(i, carry):
        side_copy(i).wait_send()
        return carry

    def sent_part(i, carry):
        part_copy(i).wait_send()
        return carry

    lax.fori_loop(0, pairs, sent_side, 0)
    lax.fori_loop(0, pairs - 1, sent_part, 0)


def store_kernel(updated_in, score_in, updated_out, score_out, sem):
    copies = [
        pltpu.make_async_copy(updated_in, updated_out, sem.at[0]),
        pltpu.make_async_copy(score_in, score_out, sem.at[1]),
    ]
    for copy in copies:
        copy.start()
    for copy in copies:
        copy.wait()


def per_device(coefficients, sumstats, linkage, band_start, group_ids, group_weight, dosage):
    _, traits_here, snps = coefficients.shape
    width = linkage.shape[2]
    genomes = lax.axis_size("genome")
    ancs = lax.axis_size("anc")
    traits_n = lax.axis_size("trait")
    persons = dosage.shape[1]
    persons_per = persons // genomes
    groups = group_weight.shape[1]
    reach = -(-width // snps)
    assert reach == 2 and genomes % 2 == 0 and coefficients.shape[0] == 1 and ancs == 4
    tile = snps // band_start.shape[1]
    slots = 2 * reach + 1
    pairs = genomes // 2
    group_reach = min(-(-longest_run // snps), genomes - 1)
    stat_n = (2 * group_reach + 1) * traits_n - 1
    lanes = -(-groups // 128) * 128
    sizes = (genomes, ancs, traits_n, reach, tile, groups)
    hbm = pl.BlockSpec(memory_space=pltpu.HBM)
    vmem = pl.BlockSpec(memory_space=pltpu.VMEM)
    dma = pltpu.SemaphoreType.DMA
    args = (coefficients, sumstats, linkage, band_start, group_ids, group_weight, dosage)
    args = tuple(pltpu.with_memory_space_constraint(x, pltpu.HBM) for x in args)
    out_shape = (
        jax.ShapeDtypeStruct((1, traits_here, snps), F32),
        jax.ShapeDtypeStruct((1, traits_here, persons_per), F32),
    )
    updated, scores = pl.pallas_call(
        functools.partial(step_kernel, sizes),
        out_shape=out_shape,
        in_specs=[hbm] * 7,
        out_specs=(vmem, vmem),
        scratch_shapes=[
            pltpu.VMEM((traits_here, snps), F32),
            pltpu.VMEM((traits_here, snps), F32),
            pltpu.VMEM((snps, width), BF16),
            pltpu.SMEM(band_start.shape, jnp.int32),
            pltpu.VMEM(group_ids.shape, jnp.int32),
            pltpu.VMEM(group_weight.shape, F32),
            pltpu.VMEM((persons, snps), BF16),
            pltpu.VMEM((slots, snps, traits_here), BF16),
            pltpu.VMEM((slots * snps, traits_here), F32),
            pltpu.VMEM((traits_here, snps), F32),
            pltpu.VMEM((traits_here, snps), F32),
            pltpu.VMEM((traits_here, snps), BF16),
            pltpu.VMEM((traits_here, snps), BF16),
            pltpu.VMEM((traits_here, snps), F32),
            pltpu.VMEM((traits_here, snps), BF16),
            pltpu.VMEM((1, snps), F32),
            pltpu.VMEM((2, lanes), F32),
            pltpu.VMEM((stat_n, 2, lanes), F32),
            pltpu.VMEM((pairs, traits_here, persons_per), BF16),
            pltpu.VMEM((pairs, traits_here, persons_per), BF16),
            pltpu.VMEM((pairs - 1, traits_here, persons_per), BF16),
            pltpu.VMEM((pairs - 1, traits_here, persons_per), BF16),
            dma((4,)), dma((5,)), dma((snps // tile,)), pltpu.SemaphoreType.REGULAR,
            dma((15,)), dma((slots, 8)), dma((3,)), dma((3,)),
            dma((stat_n,)), dma((stat_n,)), dma((pairs,)), dma((pairs,)), dma((pairs - 1,)), dma((pairs - 1,)),
        ],
        compiler_params=pltpu.CompilerParams(
            collective_id=0, has_side_effects=True, vmem_limit_bytes=52 * 1024 * 1024
        ),
    )(*args)
    return pl.pallas_call(
        store_kernel,
        out_shape=out_shape,
        in_specs=[vmem, vmem],
        out_specs=(hbm, hbm),
        scratch_shapes=[dma((2,))],
    )(*(pltpu.with_memory_space_constraint(x, pltpu.VMEM) for x in (updated, scores)))


def solution(mesh):
    in_specs = (
        P("anc", "trait", "genome"),
        P("anc", "trait", "genome"),
        P("anc", "genome", None),
        P("anc", "genome"),
        P("anc", "genome"),
        P("anc", None),
        P("anc", None, "genome"),
    )
    out_specs = (P("anc", "trait", "genome"), P("anc", "trait", "genome"))
    return jax.shard_map(
        per_device, mesh=mesh, in_specs=in_specs, out_specs=out_specs, check_vma=False
    )
```

```python
import functools
import math

import jax
import jax.numpy as jnp
from jax import lax
from jax.experimental import pallas as pl
from jax.experimental.pallas import tpu as pltpu
from jax.sharding import PartitionSpec as P

step_size = 0.5
merging = 0.5
epsilon = 1e-06
longest_run = 8192

MESH = pl.DeviceIdType.MESH
F32 = jnp.float32
BF16 = jnp.bfloat16


def step_kernel(
    sizes,
    coef_hbm, sums_hbm, link_hbm, starts_hbm, ids_hbm, weight_hbm, dosage_hbm,
    updated_ref, score_ref,
    coef, sums, link_first, link_second, starts_ref, ids_ref, weight_ref, dosage, ext, field, band, pair, mean, pair_out, pair_in,
    proposal, low, row, stats_out, stats_in, side_out, side_in, part_out, part_in,
    coef_sem, load_sem, link_sem, ready,
    halo_send, halo_recv, pair_send, pair_recv, stats_send, stats_recv, side_send, side_recv, part_send, part_recv,
):
    genomes, ancs, traits_n, reach, tile, groups = sizes
    traits_here, snps = coef.shape
    links = (link_first, link_second)
    width = link_first.shape[1]
    tiles = snps // tile
    half = tiles // 2
    persons_per = part_out.shape[2]
    pairs = genomes // 2
    g = lax.axis_index("genome")
    a = lax.axis_index("anc")
    t = lax.axis_index("trait")
    core, side = lax.rem(a, 2), a // 2
    parity = lax.rem(g, 2)
    even = 1 - 2 * parity
    near, far, back, across = g + even, g + 2 * even, g - 2 * even, g - even

    def in_range(p):
        return jnp.logical_and(p >= 0, p < genomes)

    def genome(p):
        return {"genome": jnp.clip(p, 0, genomes - 1)}

    group_reach = min(-(-longest_run // snps), genomes - 1)
    stat_peers = [
        (d, m) for m in range(traits_n) for d in range(-group_reach, group_reach + 1) if (d, m) != (0, 0)
    ]
    if genomes > 8 or traits_n > 1:
        greet = [(k, m) for m in range(traits_n) for k in range(genomes) if (k, m) != (0, 0)]
    else:
        greet = []

    coef_parts = coef_sem.shape[0]
    part_cols = snps // coef_parts

    def coef_copy(i):
        cols = pl.ds(i * part_cols, part_cols)
        return pltpu.make_async_copy(coef_hbm.at[0, :, cols], coef.at[:, cols], coef_sem.at[i])

    for i in range(coef_parts):
        coef_copy(i).start()
    barrier = pltpu.get_barrier_semaphore()
    if greet:
        for k, m in greet:
            pl.semaphore_signal(
                barrier, inc=1, device_id_type=MESH,
                device_id={"genome": lax.rem(g + k, genomes), "trait": lax.rem(t + m, traits_n)},
            )
        expected = len(greet)
    else:
        pl.semaphore_signal(barrier, inc=1, device_id=genome(near), device_id_type=MESH)
        for peer in (far, back):
            @pl.when(in_range(peer))
            def _(peer=peer):
                pl.semaphore_signal(barrier, inc=1, device_id=genome(peer), device_id_type=MESH)
        expected = 1 + in_range(far).astype(jnp.int32) + in_range(back).astype(jnp.int32)

    @pl.when(core == 0)
    def _():
        pl.semaphore_signal(barrier, inc=1, device_id={"anc": a + 1}, device_id_type=MESH)

    @pl.when(jnp.logical_and(core == 1, side == 1))
    def _():
        pl.semaphore_signal(barrier, inc=1, device_id={"anc": a - 2}, device_id_type=MESH)

    expected = expected + core + core * (1 - side)

    load_small = [
        pltpu.make_async_copy(starts_hbm, starts_ref, load_sem.at[0]),
        pltpu.make_async_copy(ids_hbm, ids_ref, load_sem.at[1]),
        pltpu.make_async_copy(weight_hbm, weight_ref, load_sem.at[2]),
    ]
    load_sums = pltpu.make_async_copy(sums_hbm.at[0], sums, load_sem.at[3])
    load_dosage = pltpu.make_async_copy(dosage_hbm.at[0], dosage, load_sem.at[4])

    def link_copy(u):
        return pltpu.make_async_copy(
            link_hbm.at[0, pl.ds(u * tile, tile), :], links[u // half].at[pl.ds(u % half * tile, tile), :],
            link_sem.at[u],
        )

    unit = snps // 16
    far_rows = width - tile - snps
    ahead = 11 * unit
    behind = snps - ahead
    deep = [r + 128 for r in (snps, ahead, behind)]
    own_at = deep[0]
    partner_at = own_at + snps + deep[0]
    back_at = partner_at + snps + deep[0]
    across_a = back_at + snps + deep[0]
    far_a = across_a + ahead + deep[1]
    across_b = far_a + ahead + deep[1]
    far_b = across_b + behind + deep[2]
    assert far_b + behind + deep[2] == field.shape[0] and 13 * unit < far_rows <= 16 * unit

    def own_block(u, carry):
        cols = pl.ds(pl.multiple_of(u * tile, tile), tile)
        flat = coef[:, cols].T.astype(BF16)
        ext[reach, cols, :] = flat
        field[pl.ds(pl.multiple_of(own_at + u * tile, unit), tile), :] = flat.astype(F32)
        return carry

    for i in range(coef_parts):
        coef_copy(i).wait()
        lax.fori_loop(i * tiles // coef_parts, (i + 1) * tiles // coef_parts, own_block, 0, unroll=2)

    pieces = [
        (5 * unit, 6 * unit), (13 * unit, 3 * unit), (0, 5 * unit), (11 * unit, 2 * unit),
        (5 * unit, 6 * unit), (13 * unit, far_rows - 13 * unit),
        (snps - far_rows, far_rows // 2), (snps - far_rows + far_rows // 2, far_rows // 2),
    ]

    def piece(p, odd):
        at, size = pieces[p]
        return pl.multiple_of((1 - odd) * at + odd * (snps - at - size), unit), size

    def halo_copy(src_slot, dst_slot, p, odd, peer, send):
        at, size = piece(p, odd)
        rows = pl.ds(at, size)
        return pltpu.make_async_remote_copy(
            src_ref=ext.at[src_slot, rows, :], dst_ref=ext.at[dst_slot, rows, :],
            send_sem=halo_send.at[send], recv_sem=halo_recv.at[dst_slot, p],
            device_id=genome(peer), device_id_type=MESH,
        )

    def near_copy(p):
        return halo_copy(reach, reach - even, p, parity, near, p)

    def back_copy(p):
        return halo_copy(reach, reach + 2 * even, p, parity, back, 4 + p - 2)

    def far_copy(p):
        return halo_copy(reach, reach - 2 * even, p, parity, far, 8 + p - 6)

    def relay_far(p):
        return halo_copy(reach + even, reach - even, p, 1 - parity, far, 10 + p)

    def relay_near(p):
        return halo_copy(reach + 2 * even, reach + even, p, parity, near, 12 + p - 2)

    def arrived(slot, p, odd):
        halo_copy(reach, slot, p, odd, near, 0).wait_recv()

    has_far, has_back = in_range(far), in_range(back)

    pl.semaphore_wait(barrier, expected)

    for p, q in ((0, 2), (1, 3), (2, 4), (3, 5)):
        near_copy(p).start()

        @pl.when(has_back)
        def _(q=q):
            back_copy(q).start()

        if p < 2:
            @pl.when(has_far)
            def _(p=p):
                far_copy(6 + p).start()

    @pl.when(core == 1)
    def _():
        pl.semaphore_signal(ready, inc=1, device_id={"anc": a - 1}, device_id_type=MESH)

    @pl.when(jnp.logical_and(core == 1, side == 0))
    def _():
        pl.semaphore_signal(ready, inc=1, device_id={"anc": a + 2}, device_id_type=MESH)

    for load in load_small:
        load.start()
    for u in range(tiles):
        link_copy(u).start()
    load_sums.start()
    load_dosage.start()

    other_core = {"anc": a + 1 - 2 * core}
    other_side = {"anc": lax.rem(a + 2, ancs)}
    up_copy = pltpu.make_async_remote_copy(
        src_ref=coef, dst_ref=pair, send_sem=pair_send.at[0], recv_sem=pair_recv.at[0],
        device_id=other_core, device_id_type=MESH,
    )
    over_copy = pltpu.make_async_remote_copy(
        src_ref=pair_out, dst_ref=pair_in, send_sem=pair_send.at[1], recv_sem=pair_recv.at[1],
        device_id=other_side, device_id_type=MESH,
    )
    down_copy = pltpu.make_async_remote_copy(
        src_ref=mean, dst_ref=mean, send_sem=pair_send.at[2], recv_sem=pair_recv.at[2],
        device_id=other_core, device_id_type=MESH,
    )

    def clear(first, last):
        def part(i, carry):
            at = pl.multiple_of(first + i * unit, unit)
            field[pl.ds(at, unit), :] = jnp.zeros((unit, traits_here), F32)
            return carry

        lax.fori_loop(0, (last - first) // unit, part, 0, unroll=4)

    clear(0, own_at)
    clear(own_at + snps, field.shape[0])

    for i, (d, m) in enumerate(stat_peers):
        @pl.when(jnp.logical_not(in_range(g - d)))
        def _(i=i):
            stats_in[i] = jnp.zeros(stats_in.shape[1:], F32)

    @pl.when(core == 0)
    def _():
        pl.semaphore_wait(ready, 1)
        up_copy.start()

    @pl.when(core == 1)
    def _():
        up_copy.wait_recv()

        def add(u, carry):
            cols = pl.ds(pl.multiple_of(u * tile, tile), tile)
            value = coef[:, cols] + pair[:, cols]
            pair[:, cols] = value
            pair_out[:, cols] = value.astype(BF16)
            return carry

        lax.fori_loop(0, tiles, add, 0, unroll=2)

        @pl.when(side == 1)
        def _():
            pl.semaphore_wait(ready, 1)

        over_copy.start()

    def pass_on(p):
        if p < 2:
            arrived(reach + even, p, 1 - parity)

            @pl.when(has_far)
            def _():
                relay_far(p).start()
        else:
            @pl.when(has_far)
            def _():
                arrived(reach + 2 * even, p, parity)
                relay_near(p).start()

    def widen(slot, p, odd, base):
        at, size = piece(p, odd)

        def part(i, carry):
            r = pl.multiple_of(at + i * unit, unit)
            field[pl.ds(pl.multiple_of(base + r, unit), unit), :] = ext[slot, pl.ds(r, unit), :].astype(F32)
            return carry

        lax.fori_loop(0, size // unit, part, 0)

    def base_a(base, odd):
        return base - odd * behind

    def base_b(base, odd):
        return base - (1 - odd) * ahead

    def range_product(link, u, length, first, second=None):
        depth = length + 128
        within = pl.ds(pl.multiple_of(lax.rem(u, half) * tile, tile), tile)
        rows = pl.ds(pl.multiple_of(u * tile, tile), tile)
        begin = starts_ref[0, u] - g * snps + reach * snps
        where, at = first
        if second is not None:
            here = jnp.clip(begin + width - where, 0, 1) * jnp.clip(where + length - begin, 0, 1)
            where = second[0] + here * (where - second[0])
            at = second[1] + here * (at - second[1])
        skip = lax.div(jnp.clip(where - begin, 0, width - depth), 128) * 128
        from_row = at + jnp.clip(begin + skip - where, -depth, length)
        total = jnp.zeros((tile, traits_here), F32)
        for c in range(0, depth, 512):
            step = min(512, depth - c)
            window = field[pl.ds(from_row + c, step), :].astype(BF16)
            total = total + jnp.dot(
                link[within, pl.ds(skip + c, step)], window, preferred_element_type=F32
            )
        return rows, total

    pass_on(0)
    pass_on(2)
    load_small[0].wait()

    def own_tile(link, u, carry):
        rows, total = range_product(link, u, snps, (reach * snps, own_at))
        band[rows, :] = total
        return carry

    def each_tile(body, waits=False):
        for i, link in enumerate(links):
            if waits:
                for u in range(i * half, (i + 1) * half):
                    link_copy(u).wait()
            lax.fori_loop(i * half, (i + 1) * half, functools.partial(body, link), 0, unroll=2)

    each_tile(own_tile, waits=True)
    pass_on(1)
    pass_on(3)

    for p in range(4):
        if p > 1:
            arrived(reach + even, p, 1 - parity)
        widen(reach + even, p, 1 - parity, partner_at)

    @pl.when(has_back)
    def _():
        for p in (6, 7):
            arrived(reach - 2 * even, p, parity)
            widen(reach - 2 * even, p, parity, back_at)

    @pl.when(core == 1)
    def _():
        over_copy.wait_recv()

        def add(u, carry):
            cols = pl.ds(pl.multiple_of(u * tile, tile), tile)
            mean[:, cols] = (pair[:, cols] + pair_in[:, cols].astype(F32)) / ancs
            return carry

        lax.fori_loop(0, tiles, add, 0, unroll=2)
        down_copy.start()

    def side_tile(link, u, carry):
        rows, total = range_product(
            link, u, snps, ((reach + even) * snps, partner_at), ((reach - 2 * even) * snps, back_at)
        )
        band[rows, :] = band[rows, :] + total
        return carry

    each_tile(side_tile)

    @pl.when(has_far)
    def _():
        for p in (4, 5):
            arrived(reach + 2 * even, p, parity)
        for p in (2, 4):
            widen(reach + 2 * even, p, parity, base_a(far_a, parity))
        for p in (3, 5):
            widen(reach + 2 * even, p, parity, base_b(far_b, parity))

    @pl.when(has_back)
    def _():
        for p in (0, 2):
            arrived(reach - even, p, 1 - parity)
            widen(reach - even, p, 1 - parity, base_a(across_a, 1 - parity))

    def first_tile(link, u, carry):
        rows, total = range_product(
            link, u, ahead,
            ((reach - even) * snps + (1 - parity) * behind, across_a),
            ((reach + 2 * even) * snps + parity * behind, far_a),
        )
        band[rows, :] = band[rows, :] + total
        return carry

    each_tile(first_tile)

    @pl.when(core == 0)
    def _():
        down_copy.wait_recv()

    load_sums.wait()
    for load in load_small[1:]:
        load.wait()

    def prepare(u, carry):
        cols = pl.ds(pl.multiple_of(u * tile, tile), tile)
        proposal[:, cols] = (
            (1.0 - step_size - step_size * merging) * coef[:, cols]
            + step_size * sums[:, cols] + (step_size * merging) * mean[:, cols]
        )
        return carry

    lax.fori_loop(0, tiles, prepare, 0, unroll=2)

    @pl.when(has_back)
    def _():
        for p in (1, 3):
            arrived(reach - even, p, 1 - parity)
            widen(reach - even, p, 1 - parity, base_b(across_b, 1 - parity))

    def last_tile(link, u, carry):
        rows, total = range_product(
            link, u, behind,
            ((reach - even) * snps + parity * ahead, across_b),
            ((reach + 2 * even) * snps + (1 - parity) * ahead, far_b),
        )
        value = proposal[:, rows] - step_size * (band[rows, :] + total).T
        proposal[:, rows] = value
        row[:, rows] = jnp.sum(value * value, axis=0, keepdims=True)
        return carry

    each_tile(last_tile)

    lanes = stats_out.shape[1]
    mine = lax.broadcasted_iota(jnp.int32, (groups, snps), 0) == ids_ref[...]
    squares = jnp.sum(jnp.where(mine, row[...], 0.0), axis=1, keepdims=True)
    counts = jnp.sum(jnp.where(mine, 1.0, 0.0), axis=1, keepdims=True)
    on_lane = lax.broadcasted_iota(jnp.int32, (groups, lanes), 0) == lax.broadcasted_iota(
        jnp.int32, (groups, lanes), 1
    )
    stats_out[0:1, :] = jnp.sum(jnp.where(on_lane, squares, 0.0), axis=0, keepdims=True)
    stats_out[1:2, :] = jnp.sum(jnp.where(on_lane, counts, 0.0), axis=0, keepdims=True)

    def stats_copy(i):
        d, m = stat_peers[i]
        return pltpu.make_async_remote_copy(
            src_ref=stats_out, dst_ref=stats_in.at[i],
            send_sem=stats_send.at[i], recv_sem=stats_recv.at[i],
            device_id={**genome(g + d), "trait": lax.rem(t + m, traits_n)}, device_id_type=MESH,
        )

    for i, (d, m) in enumerate(stat_peers):
        @pl.when(in_range(g + d))
        def _(i=i):
            stats_copy(i).start()

    load_dosage.wait()
    for i, (d, m) in enumerate(stat_peers):
        @pl.when(in_range(g - d))
        def _(i=i):
            stats_copy(i).wait_recv()

    stats = stats_out[...]
    for i in range(len(stat_peers)):
        stats = stats + stats_in[i]
    all_squares = stats[0:1, :groups]
    all_counts = stats[1:2, :groups] / traits_n
    threshold = step_size * weight_ref[...] * jnp.sqrt(all_counts * (traits_here * traits_n))
    shrink = jnp.maximum(0.0, 1.0 - threshold / jnp.sqrt(all_squares + epsilon))
    same = lax.broadcasted_iota(jnp.int32, (groups, groups), 0) == lax.broadcasted_iota(
        jnp.int32, (groups, groups), 1
    )
    shrink = jnp.sum(jnp.where(same, shrink, 0.0), axis=1, keepdims=True)
    row[...] = jnp.sum(jnp.where(mine, shrink, 0.0), axis=0, keepdims=True)

    def shrink_tile(u, carry):
        cols = pl.ds(pl.multiple_of(u * tile, tile), tile)
        value = proposal[:, cols] * row[:, cols]
        updated_ref[0, :, cols] = value
        low[:, cols] = value.astype(BF16)
        return carry

    lax.fori_loop(0, tiles, shrink_tile, 0, unroll=2)

    scale = 1.0 / math.sqrt(snps * genomes)
    own_side, other_side_g = parity, lax.rem(near, 2)

    def pair_at(i):
        k = pairs // 2 + (1 - 2 * lax.rem(i, 2)) * ((i + 1) // 2)
        return lax.rem(g // 2 + k + pairs, pairs)

    def partial(person):
        at = pl.ds(pl.multiple_of(person * persons_per, persons_per), persons_per)
        return lax.dot_general(
            low[...], dosage[at, :], (((1,), (1,)), ((), ())), preferred_element_type=F32
        ) * scale

    def side_copy(i):
        return pltpu.make_async_remote_copy(
            src_ref=side_out.at[i], dst_ref=side_in.at[i],
            send_sem=side_send.at[i], recv_sem=side_recv.at[i],
            device_id={"genome": near}, device_id_type=MESH,
        )

    def part_copy(i):
        return pltpu.make_async_remote_copy(
            src_ref=part_out.at[i], dst_ref=part_in.at[i],
            send_sem=part_send.at[i], recv_sem=part_recv.at[i],
            device_id={"genome": 2 * pair_at(i) + own_side}, device_id_type=MESH,
        )

    def send_side(i, carry):
        side_out[i] = partial(2 * pair_at(i) + other_side_g).astype(BF16)
        side_copy(i).start()
        return carry

    def pair_sum(i):
        mine_here = partial(2 * pair_at(i) + own_side)
        side_copy(i).wait_recv()
        return mine_here + side_in[i].astype(F32)

    def send_part(i, carry):
        part_out[i] = pair_sum(i).astype(BF16)
        part_copy(i).start()
        return carry

    lax.fori_loop(0, pairs, send_side, 0)
    lax.fori_loop(0, pairs - 1, send_part, 0)

    def add_part(i, total):
        part_copy(i).wait_recv()
        return total + part_in[i].astype(F32)

    score_ref[0] = lax.fori_loop(0, pairs - 1, add_part, pair_sum(pairs - 1))

    for p in range(4):
        near_copy(p).wait_send()

    @pl.when(has_back)
    def _():
        for p in (2, 3, 4, 5):
            back_copy(p).wait_send()

    @pl.when(has_far)
    def _():
        for p in (6, 7):
            far_copy(p).wait_send()
        for p in (0, 1):
            relay_far(p).wait_send()
        for p in (2, 3):
            relay_near(p).wait_send()

    @pl.when(core == 0)
    def _():
        up_copy.wait_send()

    @pl.when(core == 1)
    def _():
        over_copy.wait_send()
        down_copy.wait_send()

    for i, (d, m) in enumerate(stat_peers):
        @pl.when(in_range(g + d))
        def _(i=i):
            stats_copy(i).wait_send()

    def sent_side(i, carry):
        side_copy(i).wait_send()
        return carry

    def sent_part(i, carry):
        part_copy(i).wait_send()
        return carry

    lax.fori_loop(0, pairs, sent_side, 0)
    lax.fori_loop(0, pairs - 1, sent_part, 0)


def store_kernel(updated_in, score_in, updated_out, score_out, sem):
    copies = [
        pltpu.make_async_copy(updated_in, updated_out, sem.at[0]),
        pltpu.make_async_copy(score_in, score_out, sem.at[1]),
    ]
    for copy in copies:
        copy.start()
    for copy in copies:
        copy.wait()


def per_device(coefficients, sumstats, linkage, band_start, group_ids, group_weight, dosage):
    _, traits_here, snps = coefficients.shape
    width = linkage.shape[2]
    genomes = lax.axis_size("genome")
    ancs = lax.axis_size("anc")
    traits_n = lax.axis_size("trait")
    persons = dosage.shape[1]
    persons_per = persons // genomes
    groups = group_weight.shape[1]
    reach = -(-width // snps)
    assert reach == 2 and genomes % 2 == 0 and coefficients.shape[0] == 1 and ancs == 4
    tile = snps // band_start.shape[1]
    slots = 2 * reach + 1
    pairs = genomes // 2
    ahead = snps // 16 * 11
    field_rows = 3 * snps + 4 * (snps + 128) + 4 * ahead + 4 * (snps - ahead) + 4 * 128
    group_reach = min(-(-longest_run // snps), genomes - 1)
    stat_n = (2 * group_reach + 1) * traits_n - 1
    lanes = -(-groups // 128) * 128
    sizes = (genomes, ancs, traits_n, reach, tile, groups)
    hbm = pl.BlockSpec(memory_space=pltpu.HBM)
    vmem = pl.BlockSpec(memory_space=pltpu.VMEM)
    dma = pltpu.SemaphoreType.DMA
    args = (coefficients, sumstats, linkage, band_start, group_ids, group_weight, dosage)
    args = tuple(pltpu.with_memory_space_constraint(x, pltpu.HBM) for x in args)
    out_shape = (
        jax.ShapeDtypeStruct((1, traits_here, snps), F32),
        jax.ShapeDtypeStruct((1, traits_here, persons_per), F32),
    )
    updated, scores = pl.pallas_call(
        functools.partial(step_kernel, sizes),
        out_shape=out_shape,
        in_specs=[hbm] * 7,
        out_specs=(vmem, vmem),
        scratch_shapes=[
            pltpu.VMEM((traits_here, snps), F32),
            pltpu.VMEM((traits_here, snps), F32),
            pltpu.VMEM((snps // 2, width), BF16),
            pltpu.VMEM((snps // 2, width), BF16),
            pltpu.SMEM(band_start.shape, jnp.int32),
            pltpu.VMEM(group_ids.shape, jnp.int32),
            pltpu.VMEM(group_weight.shape, F32),
            pltpu.VMEM((persons, snps), BF16),
            pltpu.VMEM((slots, snps, traits_here), BF16),
            pltpu.VMEM((field_rows, traits_here), F32),
            pltpu.VMEM((snps, traits_here), F32),
            pltpu.VMEM((traits_here, snps), F32),
            pltpu.VMEM((traits_here, snps), F32),
            pltpu.VMEM((traits_here, snps), BF16),
            pltpu.VMEM((traits_here, snps), BF16),
            pltpu.VMEM((traits_here, snps), F32),
            pltpu.VMEM((traits_here, snps), BF16),
            pltpu.VMEM((1, snps), F32),
            pltpu.VMEM((2, lanes), F32),
            pltpu.VMEM((stat_n, 2, lanes), F32),
            pltpu.VMEM((pairs, traits_here, persons_per), BF16),
            pltpu.VMEM((pairs, traits_here, persons_per), BF16),
            pltpu.VMEM((pairs - 1, traits_here, persons_per), BF16),
            pltpu.VMEM((pairs - 1, traits_here, persons_per), BF16),
            dma((4,)), dma((5,)), dma((snps // tile,)), pltpu.SemaphoreType.REGULAR,
            dma((14,)), dma((slots, 8)), dma((3,)), dma((3,)),
            dma((stat_n,)), dma((stat_n,)), dma((pairs,)), dma((pairs,)), dma((pairs - 1,)), dma((pairs - 1,)),
        ],
        compiler_params=pltpu.CompilerParams(
            collective_id=0, has_side_effects=True, vmem_limit_bytes=52 * 1024 * 1024
        ),
    )(*args)
    return pl.pallas_call(
        store_kernel,
        out_shape=out_shape,
        in_specs=[vmem, vmem],
        out_specs=(hbm, hbm),
        scratch_shapes=[dma((2,))],
    )(*(pltpu.with_memory_space_constraint(x, pltpu.VMEM) for x in (updated, scores)))


def solution(mesh):
    in_specs = (
        P("anc", "trait", "genome"),
        P("anc", "trait", "genome"),
        P("anc", "genome", None),
        P("anc", "genome"),
        P("anc", "genome"),
        P("anc", None),
        P("anc", None, "genome"),
    )
    out_specs = (P("anc", "trait", "genome"), P("anc", "trait", "genome"))
    return jax.shard_map(
        per_device, mesh=mesh, in_specs=in_specs, out_specs=out_specs, check_vma=False
    )
```

```python
import functools
import math

import jax
import jax.numpy as jnp
from jax import lax
from jax.experimental import pallas as pl
from jax.experimental.pallas import tpu as pltpu
from jax.sharding import PartitionSpec as P

step_size = 0.5
merging = 0.5
epsilon = 1e-06
longest_run = 8192

MESH = pl.DeviceIdType.MESH
F32 = jnp.float32
BF16 = jnp.bfloat16


def step_kernel(
    sizes,
    coef_hbm, sums_hbm, link_hbm, starts_hbm, ids_hbm, weight_hbm, dosage_hbm,
    updated_ref, score_ref,
    coef, sums, link_first, link_second, starts_ref, ids_ref, weight_ref, dosage, ext, field, band, mean, pair_out, pair_low, pair_in,
    proposal, low, row, stats_out, stats_in, side_out, side_in, part_out, part_in,
    coef_sem, load_sem, link_sem, ready,
    halo_send, halo_recv, pair_send, pair_recv, stats_send, stats_recv, side_send, side_recv, part_send, part_recv,
):
    genomes, ancs, traits_n, reach, tile, groups = sizes
    traits_here, snps = coef.shape
    links = (link_first, link_second)
    width = link_first.shape[1]
    tiles = snps // tile
    half = tiles // 2
    persons_per = part_out.shape[2]
    pairs = genomes // 2
    g = lax.axis_index("genome")
    a = lax.axis_index("anc")
    t = lax.axis_index("trait")
    core, side = lax.rem(a, 2), a // 2
    parity = lax.rem(g, 2)
    even = 1 - 2 * parity
    near, far, back, across = g + even, g + 2 * even, g - 2 * even, g - even

    def in_range(p):
        return jnp.logical_and(p >= 0, p < genomes)

    def genome(p):
        return {"genome": jnp.clip(p, 0, genomes - 1)}

    group_reach = min(-(-longest_run // snps), genomes - 1)
    stat_peers = [
        (d, m) for m in range(traits_n) for d in range(-group_reach, group_reach + 1) if (d, m) != (0, 0)
    ]
    if genomes > 8 or traits_n > 1:
        greet = [(k, m) for m in range(traits_n) for k in range(genomes) if (k, m) != (0, 0)]
    else:
        greet = []

    coef_parts = coef_sem.shape[0]
    part_cols = snps // coef_parts

    def coef_copy(i):
        cols = pl.ds(i * part_cols, part_cols)
        return pltpu.make_async_copy(coef_hbm.at[0, :, cols], coef.at[:, cols], coef_sem.at[i])

    for i in range(coef_parts):
        coef_copy(i).start()
    barrier = pltpu.get_barrier_semaphore()
    if greet:
        for k, m in greet:
            pl.semaphore_signal(
                barrier, inc=1, device_id_type=MESH,
                device_id={"genome": lax.rem(g + k, genomes), "trait": lax.rem(t + m, traits_n)},
            )
        expected = len(greet)
    else:
        pl.semaphore_signal(barrier, inc=1, device_id=genome(near), device_id_type=MESH)
        for peer in (far, back):
            @pl.when(in_range(peer))
            def _(peer=peer):
                pl.semaphore_signal(barrier, inc=1, device_id=genome(peer), device_id_type=MESH)
        expected = 1 + in_range(far).astype(jnp.int32) + in_range(back).astype(jnp.int32)

    @pl.when(core == 0)
    def _():
        pl.semaphore_signal(barrier, inc=1, device_id={"anc": a + 1}, device_id_type=MESH)

    @pl.when(jnp.logical_and(core == 0, side == 1))
    def _():
        pl.semaphore_signal(barrier, inc=1, device_id={"anc": a - 2}, device_id_type=MESH)

    expected = expected + core + (1 - core) * (1 - side)

    load_small = [
        pltpu.make_async_copy(starts_hbm, starts_ref, load_sem.at[0]),
        pltpu.make_async_copy(ids_hbm, ids_ref, load_sem.at[1]),
        pltpu.make_async_copy(weight_hbm, weight_ref, load_sem.at[2]),
    ]
    load_sums = pltpu.make_async_copy(sums_hbm.at[0], sums, load_sem.at[3])
    load_dosage = pltpu.make_async_copy(dosage_hbm.at[0], dosage, load_sem.at[4])

    def link_copy(u):
        return pltpu.make_async_copy(
            link_hbm.at[0, pl.ds(u * tile, tile), :], links[u // half].at[pl.ds(u % half * tile, tile), :],
            link_sem.at[u],
        )

    unit = snps // 16
    far_rows = width - tile - snps
    ahead = 11 * unit
    behind = snps - ahead
    deep = [r + 128 for r in (snps, ahead, behind)]
    own_at = deep[0]
    partner_a = own_at + snps + deep[0]
    back_a = partner_a + ahead + deep[1]
    across_a = back_a + ahead + deep[1]
    far_a = across_a + ahead + deep[1]
    partner_b = far_a + ahead + deep[1]
    back_b = partner_b + behind + deep[2]
    across_b = back_b + behind + deep[2]
    far_b = across_b + behind + deep[2]
    assert far_b + behind + deep[2] == field.shape[0] and 13 * unit < far_rows <= 16 * unit

    def own_block(u, carry):
        cols = pl.ds(pl.multiple_of(u * tile, tile), tile)
        flat = coef[:, cols].T.astype(BF16)
        ext[reach, cols, :] = flat
        field[pl.ds(pl.multiple_of(own_at + u * tile, unit), tile), :] = flat.astype(F32)
        return carry

    for i in range(coef_parts):
        coef_copy(i).wait()
        if i == coef_parts - 1:
            for load in load_small:
                load.start()
            for u in range(tiles):
                link_copy(u).start()
            load_sums.start()
            load_dosage.start()
        lax.fori_loop(i * tiles // coef_parts, (i + 1) * tiles // coef_parts, own_block, 0, unroll=2)

    pieces = [
        (5 * unit, 6 * unit), (13 * unit, 3 * unit), (0, 5 * unit), (11 * unit, 2 * unit),
        (5 * unit, 6 * unit), (13 * unit, far_rows - 13 * unit),
        (snps - far_rows, ahead + far_rows - snps), (ahead, behind),
    ]

    def piece(p, odd):
        at, size = pieces[p]
        return pl.multiple_of((1 - odd) * at + odd * (snps - at - size), unit), size

    def halo_copy(src_slot, dst_slot, p, odd, peer, send):
        at, size = piece(p, odd)
        rows = pl.ds(at, size)
        return pltpu.make_async_remote_copy(
            src_ref=ext.at[src_slot, rows, :], dst_ref=ext.at[dst_slot, rows, :],
            send_sem=halo_send.at[send], recv_sem=halo_recv.at[dst_slot, p],
            device_id=genome(peer), device_id_type=MESH,
        )

    def near_copy(p):
        return halo_copy(reach, reach - even, p, parity, near, p)

    def back_copy(p):
        return halo_copy(reach, reach + 2 * even, p, parity, back, 4 + p - 2)

    def far_copy(p):
        return halo_copy(reach, reach - 2 * even, p, parity, far, 8 + p - 6)

    def relay_far(p):
        return halo_copy(reach + even, reach - even, p, 1 - parity, far, 10 + p)

    def relay_near(p):
        return halo_copy(reach + 2 * even, reach + even, p, parity, near, 12 + p - 2)

    def arrived(slot, p, odd):
        halo_copy(reach, slot, p, odd, near, 0).wait_recv()

    has_far, has_back = in_range(far), in_range(back)

    pl.semaphore_wait(barrier, expected)

    def send_halo():
        for p, q in ((0, 2), (2, 3), (1, 4), (3, 5)):
            near_copy(p).start()

            @pl.when(has_back)
            def _(q=q):
                back_copy(q).start()

            if q < 4:
                @pl.when(has_far)
                def _(q=q):
                    far_copy(4 + q).start()

    other_core = {"anc": a + 1 - 2 * core}
    other_side = {"anc": lax.rem(a + 2, ancs)}
    up_copy = pltpu.make_async_remote_copy(
        src_ref=pair_out, dst_ref=pair_low, send_sem=pair_send.at[0], recv_sem=pair_recv.at[0],
        device_id=other_core, device_id_type=MESH,
    )
    over_copy = pltpu.make_async_remote_copy(
        src_ref=pair_out, dst_ref=pair_in, send_sem=pair_send.at[1], recv_sem=pair_recv.at[1],
        device_id=other_side, device_id_type=MESH,
    )
    down_copy = pltpu.make_async_remote_copy(
        src_ref=mean, dst_ref=mean, send_sem=pair_send.at[2], recv_sem=pair_recv.at[2],
        device_id=other_core, device_id_type=MESH,
    )

    @pl.when(core == 0)
    def _():
        send_halo()

        @pl.when(side == 0)
        def _():
            pl.semaphore_signal(ready, inc=1, device_id={"anc": a + 2}, device_id_type=MESH)

    @pl.when(core == 1)
    def _():
        def round_tile(u, carry):
            cols = pl.ds(pl.multiple_of(u * tile, tile), tile)
            pair_out[:, cols] = coef[:, cols].astype(BF16)
            return carry

        lax.fori_loop(0, tiles, round_tile, 0, unroll=2)
        up_copy.start()

    def clear(first, last):
        def part(i, carry):
            at = pl.multiple_of(first + i * unit, unit)
            field[pl.ds(at, unit), :] = jnp.zeros((unit, traits_here), F32)
            return carry

        lax.fori_loop(0, (last - first) // unit, part, 0, unroll=4)

    clear(0, own_at)
    clear(own_at + snps, field.shape[0])

    for i, (d, m) in enumerate(stat_peers):
        @pl.when(jnp.logical_not(in_range(g - d)))
        def _(i=i):
            stats_in[i] = jnp.zeros(stats_in.shape[1:], F32)

    @pl.when(core == 0)
    def _():
        up_copy.wait_recv()

        def add(u, carry):
            cols = pl.ds(pl.multiple_of(u * tile, tile), tile)
            value = coef[:, cols] + pair_low[:, cols].astype(F32)
            mean[:, cols] = value
            pair_out[:, cols] = value.astype(BF16)
            return carry

        lax.fori_loop(0, tiles, add, 0, unroll=2)

        @pl.when(side == 1)
        def _():
            pl.semaphore_wait(ready, 1)

        over_copy.start()

    def pass_on(p):
        if p < 2:
            arrived(reach + even, p, 1 - parity)

            @pl.when(has_far)
            def _():
                relay_far(p).start()
        else:
            @pl.when(has_far)
            def _():
                arrived(reach + 2 * even, p, parity)
                relay_near(p).start()

    def widen(slot, p, odd, base):
        at, size = piece(p, odd)

        def part(i, carry):
            r = pl.multiple_of(at + i * unit, unit)
            field[pl.ds(pl.multiple_of(base + r, unit), unit), :] = ext[slot, pl.ds(r, unit), :].astype(F32)
            return carry

        lax.fori_loop(0, size // unit, part, 0)

    def base_a(base, odd):
        return base - odd * behind

    def base_b(base, odd):
        return base - (1 - odd) * ahead

    def range_product(link, u, length, first, second=None):
        depth = length + 128
        within = pl.ds(pl.multiple_of(lax.rem(u, half) * tile, tile), tile)
        rows = pl.ds(pl.multiple_of(u * tile, tile), tile)
        begin = starts_ref[0, u] - g * snps + reach * snps
        where, at = first
        if second is not None:
            here = jnp.clip(begin + width - where, 0, 1) * jnp.clip(where + length - begin, 0, 1)
            where = second[0] + here * (where - second[0])
            at = second[1] + here * (at - second[1])
        skip = lax.div(jnp.clip(where - begin, 0, width - depth), 128) * 128
        from_row = at + jnp.clip(begin + skip - where, -depth, length)
        total = jnp.zeros((tile, traits_here), F32)
        for c in range(0, depth, 512):
            step = min(512, depth - c)
            window = field[pl.ds(from_row + c, step), :].astype(BF16)
            total = total + jnp.dot(
                link[within, pl.ds(skip + c, step)], window, preferred_element_type=F32
            )
        return rows, total

    def own_tile(link, u, carry):
        rows, total = range_product(link, u, snps, (reach * snps, own_at))
        band[rows, :] = total
        return carry

    def each_tile(body, parts=(0, 1)):
        for i in parts:
            lax.fori_loop(i * half, (i + 1) * half, functools.partial(body, links[i]), 0, unroll=2)

    def own_pass(i):
        for u in range(i * half, (i + 1) * half):
            link_copy(u).wait()
        each_tile(own_tile, (i,))

    load_small[0].wait()
    own_pass(0)

    @pl.when(core == 1)
    def _():
        pl.semaphore_wait(ready, 1)
        send_halo()

    for p in (0, 2, 1, 3):
        pass_on(p)
    own_pass(1)

    @pl.when(core == 0)
    def _():
        near_copy(3).wait_send()

        @pl.when(has_far)
        def _():
            relay_far(0).wait_send()
            relay_near(2).wait_send()

        pl.semaphore_signal(ready, inc=1, device_id=other_core, device_id_type=MESH)

    def side_product(link, u, carry, length, offsets, bases):
        rows, total = range_product(
            link, u, length,
            ((reach + even) * snps + offsets[1], bases[0]), ((reach - 2 * even) * snps + offsets[0], bases[1]),
        )
        band[rows, :] = band[rows, :] + total
        return carry

    starts_a = (parity * behind, (1 - parity) * behind)
    starts_b = ((1 - parity) * ahead, parity * ahead)

    for pieces_here, piece_back, base_of, bases, length, offsets in (
        ((0, 2), 6, base_a, (partner_a, back_a), ahead, starts_a),
        ((1, 3), 7, base_b, (partner_b, back_b), behind, starts_b),
    ):
        for p in pieces_here:
            if p > 1:
                arrived(reach + even, p, 1 - parity)
            widen(reach + even, p, 1 - parity, base_of(bases[0], 1 - parity))

        @pl.when(has_back)
        def _():
            arrived(reach - 2 * even, piece_back, parity)
            widen(reach - 2 * even, piece_back, parity, base_of(bases[1], parity))

        each_tile(functools.partial(side_product, length=length, offsets=offsets, bases=bases))

    @pl.when(has_far)
    def _():
        for p in (4, 5):
            arrived(reach + 2 * even, p, parity)
        for p in (2, 4):
            widen(reach + 2 * even, p, parity, base_a(far_a, parity))
        for p in (3, 5):
            widen(reach + 2 * even, p, parity, base_b(far_b, parity))

    @pl.when(has_back)
    def _():
        for p in (0, 2):
            arrived(reach - even, p, 1 - parity)
            widen(reach - even, p, 1 - parity, base_a(across_a, 1 - parity))

    def first_tile(link, u, carry):
        rows, total = range_product(
            link, u, ahead,
            ((reach - even) * snps + starts_a[1], across_a), ((reach + 2 * even) * snps + starts_a[0], far_a),
        )
        band[rows, :] = band[rows, :] + total
        return carry

    each_tile(first_tile)

    @pl.when(core == 0)
    def _():
        over_copy.wait_recv()

        def add(u, carry):
            cols = pl.ds(pl.multiple_of(u * tile, tile), tile)
            mean[:, cols] = (mean[:, cols] + pair_in[:, cols].astype(F32)) / ancs
            return carry

        lax.fori_loop(0, tiles, add, 0, unroll=2)
        down_copy.start()

    @pl.when(core == 1)
    def _():
        down_copy.wait_recv()

    load_sums.wait()
    for load in load_small[1:]:
        load.wait()

    def prepare(u, carry):
        cols = pl.ds(pl.multiple_of(u * tile, tile), tile)
        proposal[:, cols] = (
            (1.0 - step_size - step_size * merging) * coef[:, cols]
            + step_size * sums[:, cols] + (step_size * merging) * mean[:, cols]
        )
        return carry

    lax.fori_loop(0, tiles, prepare, 0, unroll=2)

    @pl.when(has_back)
    def _():
        for p in (1, 3):
            arrived(reach - even, p, 1 - parity)
            widen(reach - even, p, 1 - parity, base_b(across_b, 1 - parity))

    def last_tile(link, u, carry):
        rows, total = range_product(
            link, u, behind,
            ((reach - even) * snps + starts_b[1], across_b), ((reach + 2 * even) * snps + starts_b[0], far_b),
        )
        value = proposal[:, rows] - step_size * (band[rows, :] + total).T
        proposal[:, rows] = value
        row[:, rows] = jnp.sum(value * value, axis=0, keepdims=True)
        return carry

    each_tile(last_tile)

    lanes = stats_out.shape[1]
    mine = lax.broadcasted_iota(jnp.int32, (groups, snps), 0) == ids_ref[...]
    squares = jnp.sum(jnp.where(mine, row[...], 0.0), axis=1, keepdims=True)
    counts = jnp.sum(jnp.where(mine, 1.0, 0.0), axis=1, keepdims=True)
    on_lane = lax.broadcasted_iota(jnp.int32, (groups, lanes), 0) == lax.broadcasted_iota(
        jnp.int32, (groups, lanes), 1
    )
    stats_out[0:1, :] = jnp.sum(jnp.where(on_lane, squares, 0.0), axis=0, keepdims=True)
    stats_out[1:2, :] = jnp.sum(jnp.where(on_lane, counts, 0.0), axis=0, keepdims=True)

    def stats_copy(i):
        d, m = stat_peers[i]
        return pltpu.make_async_remote_copy(
            src_ref=stats_out, dst_ref=stats_in.at[i],
            send_sem=stats_send.at[i], recv_sem=stats_recv.at[i],
            device_id={**genome(g + d), "trait": lax.rem(t + m, traits_n)}, device_id_type=MESH,
        )

    for i, (d, m) in enumerate(stat_peers):
        @pl.when(in_range(g + d))
        def _(i=i):
            stats_copy(i).start()

    load_dosage.wait()
    for i, (d, m) in enumerate(stat_peers):
        @pl.when(in_range(g - d))
        def _(i=i):
            stats_copy(i).wait_recv()

    stats = stats_out[...]
    for i in range(len(stat_peers)):
        stats = stats + stats_in[i]
    all_squares = stats[0:1, :groups]
    all_counts = stats[1:2, :groups] / traits_n
    threshold = step_size * weight_ref[...] * jnp.sqrt(all_counts * (traits_here * traits_n))
    shrink = jnp.maximum(0.0, 1.0 - threshold / jnp.sqrt(all_squares + epsilon))
    same = lax.broadcasted_iota(jnp.int32, (groups, groups), 0) == lax.broadcasted_iota(
        jnp.int32, (groups, groups), 1
    )
    shrink = jnp.sum(jnp.where(same, shrink, 0.0), axis=1, keepdims=True)
    row[...] = jnp.sum(jnp.where(mine, shrink, 0.0), axis=0, keepdims=True)

    def shrink_tile(u, carry):
        cols = pl.ds(pl.multiple_of(u * tile, tile), tile)
        value = proposal[:, cols] * row[:, cols]
        updated_ref[0, :, cols] = value
        low[:, cols] = value.astype(BF16)
        return carry

    lax.fori_loop(0, tiles, shrink_tile, 0, unroll=2)

    scale = 1.0 / math.sqrt(snps * genomes)
    own_side, other_side_g = parity, lax.rem(near, 2)

    def pair_at(i):
        here = g // 2
        below, above = here, pairs - 1 - here
        wide = jnp.maximum(below, above)
        single = wide - jnp.minimum(below, above)
        up = 2 * jnp.clip(above - below, 0, 1) - 1
        alone = jnp.clip(single - i, 0, 1)
        two = jnp.maximum(i - single, 0)
        away = alone * (wide - i) + (1 - alone) * (wide - single - lax.div(two, 2))
        return here + up * (1 - 2 * (1 - alone) * lax.rem(two, 2)) * away

    def partial(person):
        at = pl.ds(pl.multiple_of(person * persons_per, persons_per), persons_per)
        return lax.dot_general(
            low[...], dosage[at, :], (((1,), (1,)), ((), ())), preferred_element_type=F32
        ) * scale

    def side_copy(i):
        return pltpu.make_async_remote_copy(
            src_ref=side_out.at[i], dst_ref=side_in.at[i],
            send_sem=side_send.at[i], recv_sem=side_recv.at[i],
            device_id={"genome": near}, device_id_type=MESH,
        )

    def part_copy(i):
        to = pair_at(i)
        slot = lax.rem(g // 2 - to + pairs, pairs) - 1
        return pltpu.make_async_remote_copy(
            src_ref=part_out.at[i], dst_ref=part_in.at[slot],
            send_sem=part_send.at[i], recv_sem=part_recv.at[slot],
            device_id={"genome": 2 * to + own_side}, device_id_type=MESH,
        )

    def send_side(i, carry):
        side_out[i] = partial(2 * pair_at(i) + other_side_g).astype(BF16)
        side_copy(i).start()
        return carry

    def pair_sum(i):
        mine_here = partial(2 * pair_at(i) + own_side)
        side_copy(i).wait_recv()
        return mine_here + side_in[i].astype(F32)

    def send_part(i, carry):
        part_out[i] = pair_sum(i).astype(BF16)
        part_copy(i).start()
        return carry

    lax.fori_loop(0, pairs, send_side, 0)
    lax.fori_loop(0, pairs - 1, send_part, 0)

    def part_arrived(i):
        return pltpu.make_async_remote_copy(
            src_ref=part_out.at[i], dst_ref=part_in.at[i],
            send_sem=part_send.at[i], recv_sem=part_recv.at[i],
            device_id={"genome": near}, device_id_type=MESH,
        )

    def add_part(i, total):
        part_arrived(i).wait_recv()
        return total + part_in[i].astype(F32)

    score_ref[0] = lax.fori_loop(0, pairs - 1, add_part, pair_sum(pairs - 1))

    for p in range(3):
        near_copy(p).wait_send()

    @pl.when(has_back)
    def _():
        for p in (2, 3, 4, 5):
            back_copy(p).wait_send()

    @pl.when(has_far)
    def _():
        for p in (6, 7):
            far_copy(p).wait_send()
        relay_far(1).wait_send()
        relay_near(3).wait_send()

    @pl.when(core == 1)
    def _():
        near_copy(3).wait_send()

        @pl.when(has_far)
        def _():
            relay_far(0).wait_send()
            relay_near(2).wait_send()

        up_copy.wait_send()

    @pl.when(core == 0)
    def _():
        over_copy.wait_send()
        down_copy.wait_send()

    for i, (d, m) in enumerate(stat_peers):
        @pl.when(in_range(g + d))
        def _(i=i):
            stats_copy(i).wait_send()

    def sent_side(i, carry):
        side_copy(i).wait_send()
        return carry

    def sent_part(i, carry):
        part_copy(i).wait_send()
        return carry

    lax.fori_loop(0, pairs, sent_side, 0)
    lax.fori_loop(0, pairs - 1, sent_part, 0)


def store_kernel(updated_in, score_in, updated_out, score_out, sem):
    copies = [
        pltpu.make_async_copy(updated_in, updated_out, sem.at[0]),
        pltpu.make_async_copy(score_in, score_out, sem.at[1]),
    ]
    for copy in copies:
        copy.start()
    for copy in copies:
        copy.wait()


def per_device(coefficients, sumstats, linkage, band_start, group_ids, group_weight, dosage):
    _, traits_here, snps = coefficients.shape
    width = linkage.shape[2]
    genomes = lax.axis_size("genome")
    ancs = lax.axis_size("anc")
    traits_n = lax.axis_size("trait")
    persons = dosage.shape[1]
    persons_per = persons // genomes
    groups = group_weight.shape[1]
    reach = -(-width // snps)
    assert reach == 2 and genomes % 2 == 0 and coefficients.shape[0] == 1 and ancs == 4
    tile = snps // band_start.shape[1]
    slots = 2 * reach + 1
    pairs = genomes // 2
    ahead = snps // 16 * 11
    field_rows = snps + 2 * (snps + 128) + 8 * snps + 8 * 128
    group_reach = min(-(-longest_run // snps), genomes - 1)
    stat_n = (2 * group_reach + 1) * traits_n - 1
    lanes = -(-groups // 128) * 128
    sizes = (genomes, ancs, traits_n, reach, tile, groups)
    hbm = pl.BlockSpec(memory_space=pltpu.HBM)
    vmem = pl.BlockSpec(memory_space=pltpu.VMEM)
    dma = pltpu.SemaphoreType.DMA
    args = (coefficients, sumstats, linkage, band_start, group_ids, group_weight, dosage)
    args = tuple(pltpu.with_memory_space_constraint(x, pltpu.HBM) for x in args)
    out_shape = (
        jax.ShapeDtypeStruct((1, traits_here, snps), F32),
        jax.ShapeDtypeStruct((1, traits_here, persons_per), F32),
    )
    updated, scores = pl.pallas_call(
        functools.partial(step_kernel, sizes),
        out_shape=out_shape,
        in_specs=[hbm] * 7,
        out_specs=(vmem, vmem),
        scratch_shapes=[
            pltpu.VMEM((traits_here, snps), F32),
            pltpu.VMEM((traits_here, snps), F32),
            pltpu.VMEM((snps // 2, width), BF16),
            pltpu.VMEM((snps // 2, width), BF16),
            pltpu.SMEM(band_start.shape, jnp.int32),
            pltpu.VMEM(group_ids.shape, jnp.int32),
            pltpu.VMEM(group_weight.shape, F32),
            pltpu.VMEM((persons, snps), BF16),
            pltpu.VMEM((slots, snps, traits_here), BF16),
            pltpu.VMEM((field_rows, traits_here), F32),
            pltpu.VMEM((snps, traits_here), F32),
            pltpu.VMEM((traits_here, snps), F32),
            pltpu.VMEM((traits_here, snps), BF16),
            pltpu.VMEM((traits_here, snps), BF16),
            pltpu.VMEM((traits_here, snps), BF16),
            pltpu.VMEM((traits_here, snps), F32),
            pltpu.VMEM((traits_here, snps), BF16),
            pltpu.VMEM((1, snps), F32),
            pltpu.VMEM((2, lanes), F32),
            pltpu.VMEM((stat_n, 2, lanes), F32),
            pltpu.VMEM((pairs, traits_here, persons_per), BF16),
            pltpu.VMEM((pairs, traits_here, persons_per), BF16),
            pltpu.VMEM((pairs - 1, traits_here, persons_per), BF16),
            pltpu.VMEM((pairs - 1, traits_here, persons_per), BF16),
            dma((4,)), dma((5,)), dma((snps // tile,)), pltpu.SemaphoreType.REGULAR,
            dma((14,)), dma((slots, 8)), dma((3,)), dma((3,)),
            dma((stat_n,)), dma((stat_n,)), dma((pairs,)), dma((pairs,)), dma((pairs - 1,)), dma((pairs - 1,)),
        ],
        compiler_params=pltpu.CompilerParams(
            collective_id=0, has_side_effects=True, vmem_limit_bytes=52 * 1024 * 1024
        ),
    )(*args)
    return pl.pallas_call(
        store_kernel,
        out_shape=out_shape,
        in_specs=[vmem, vmem],
        out_specs=(hbm, hbm),
        scratch_shapes=[dma((2,))],
    )(*(pltpu.with_memory_space_constraint(x, pltpu.VMEM) for x in (updated, scores)))


def solution(mesh):
    in_specs = (
        P("anc", "trait", "genome"),
        P("anc", "trait", "genome"),
        P("anc", "genome", None),
        P("anc", "genome"),
        P("anc", "genome"),
        P("anc", None),
        P("anc", None, "genome"),
    )
    out_specs = (P("anc", "trait", "genome"), P("anc", "trait", "genome"))
    return jax.shard_map(
        per_device, mesh=mesh, in_specs=in_specs, out_specs=out_specs, check_vma=False
    )
```

```python
import functools
import math

import jax
import jax.numpy as jnp
from jax import lax
from jax.experimental import pallas as pl
from jax.experimental.pallas import tpu as pltpu
from jax.sharding import PartitionSpec as P

step_size = 0.5
merging = 0.5
epsilon = 1e-06
longest_run = 8192

MESH = pl.DeviceIdType.MESH
F32 = jnp.float32
BF16 = jnp.bfloat16


def step_kernel(
    sizes,
    coef_hbm, sums_hbm, link_hbm, starts_hbm, ids_hbm, weight_hbm, dosage_hbm,
    updated_ref, score_ref,
    coef, sums, link_first, link_second, starts_ref, ids_ref, weight_ref, dosage, ext, field, band, mean, pair_out, pair_low, pair_in,
    proposal, low, row, stats_out, stats_in, side_out, side_in, part_out, part_in,
    coef_sem, load_sem, link_sem, ready,
    halo_send, halo_recv, pair_send, pair_recv, stats_send, stats_recv, side_send, side_recv, part_send, part_recv,
):
    genomes, ancs, traits_n, reach, tile, groups = sizes
    traits_here, snps = coef.shape
    links = (link_first, link_second)
    width = link_first.shape[1]
    tiles = snps // tile
    half = tiles // 2
    persons_per = dosage.shape[0] // genomes
    pairs = genomes // 2
    g = lax.axis_index("genome")
    a = lax.axis_index("anc")
    t = lax.axis_index("trait")
    core, side = lax.rem(a, 2), a // 2
    parity = lax.rem(g, 2)
    even = 1 - 2 * parity
    near, far, back, across = g + even, g + 2 * even, g - 2 * even, g - even

    def in_range(p):
        return jnp.logical_and(p >= 0, p < genomes)

    def genome(p):
        return {"genome": jnp.clip(p, 0, genomes - 1)}

    group_reach = min(-(-longest_run // snps), genomes - 1)
    stat_peers = [
        (d, m) for m in range(traits_n) for d in range(-group_reach, group_reach + 1) if (d, m) != (0, 0)
    ]
    if genomes > 8 or traits_n > 1:
        greet = [(k, m) for m in range(traits_n) for k in range(genomes) if (k, m) != (0, 0)]
    else:
        greet = []

    coef_parts = coef_sem.shape[0]
    part_cols = snps // coef_parts

    def coef_copy(i):
        cols = pl.ds(i * part_cols, part_cols)
        return pltpu.make_async_copy(coef_hbm.at[0, :, cols], coef.at[:, cols], coef_sem.at[i])

    for i in range(coef_parts):
        coef_copy(i).start()
    barrier = pltpu.get_barrier_semaphore()
    if greet:
        for k, m in greet:
            pl.semaphore_signal(
                barrier, inc=1, device_id_type=MESH,
                device_id={"genome": lax.rem(g + k, genomes), "trait": lax.rem(t + m, traits_n)},
            )
        expected = len(greet)
    else:
        pl.semaphore_signal(barrier, inc=1, device_id=genome(near), device_id_type=MESH)
        for peer in (far, back):
            @pl.when(in_range(peer))
            def _(peer=peer):
                pl.semaphore_signal(barrier, inc=1, device_id=genome(peer), device_id_type=MESH)
        expected = 1 + in_range(far).astype(jnp.int32) + in_range(back).astype(jnp.int32)

    @pl.when(core == 0)
    def _():
        pl.semaphore_signal(barrier, inc=1, device_id={"anc": a + 1}, device_id_type=MESH)

    @pl.when(jnp.logical_and(core == 0, side == 1))
    def _():
        pl.semaphore_signal(barrier, inc=1, device_id={"anc": a - 2}, device_id_type=MESH)

    expected = expected + core + (1 - core) * (1 - side)

    load_small = [
        pltpu.make_async_copy(starts_hbm, starts_ref, load_sem.at[0]),
        pltpu.make_async_copy(ids_hbm, ids_ref, load_sem.at[1]),
        pltpu.make_async_copy(weight_hbm, weight_ref, load_sem.at[2]),
    ]
    load_sums = pltpu.make_async_copy(sums_hbm.at[0], sums, load_sem.at[3])
    load_dosage = pltpu.make_async_copy(dosage_hbm.at[0], dosage, load_sem.at[4])

    def link_copy(u):
        return pltpu.make_async_copy(
            link_hbm.at[0, pl.ds(u * tile, tile), :], links[u // half].at[pl.ds(u % half * tile, tile), :],
            link_sem.at[u],
        )

    unit = snps // 16
    far_rows = width - tile - snps
    ahead = 11 * unit
    behind = snps - ahead
    ahead = 11 * unit
    behind = snps - ahead
    own_at = snps + 128
    at_a = [own_at + 2 * snps + 128 + i * (2 * ahead + 128) for i in range(4)]
    at_b = [at_a[3] + 2 * ahead + 128 + i * (2 * behind + 128) for i in range(4)]
    assert at_b[3] + 2 * behind + 128 == field.shape[0] and 13 * unit < far_rows <= 16 * unit
    first_a = (parity * behind, (1 - parity) * behind)
    first_b = ((1 - parity) * ahead, parity * ahead)

    def own_block(u, carry):
        cols = pl.ds(pl.multiple_of(u * tile, tile), tile)
        flat = coef[:, cols].T.astype(BF16)
        ext[reach, cols, :] = flat
        field[pl.ds(pl.multiple_of(own_at + u * tile, unit), tile), :] = flat.astype(F32)
        return carry

    for i in range(coef_parts):
        coef_copy(i).wait()
        if i == coef_parts - 1:
            for load in load_small:
                load.start()
            for u in range(tiles):
                link_copy(u).start()
            load_sums.start()
            load_dosage.start()
        lax.fori_loop(i * tiles // coef_parts, (i + 1) * tiles // coef_parts, own_block, 0, unroll=2)

    pieces = [
        (5 * unit, 6 * unit), (13 * unit, 3 * unit), (0, 5 * unit), (11 * unit, 2 * unit),
        (5 * unit, 6 * unit), (13 * unit, far_rows - 13 * unit),
        (snps - far_rows, ahead + far_rows - snps), (ahead, behind),
    ]

    def piece(p, odd):
        at, size = pieces[p]
        return pl.multiple_of((1 - odd) * at + odd * (snps - at - size), unit), size

    def halo_copy(src_slot, dst_slot, p, odd, peer, send):
        at, size = piece(p, odd)
        rows = pl.ds(at, size)
        return pltpu.make_async_remote_copy(
            src_ref=ext.at[src_slot, rows, :], dst_ref=ext.at[dst_slot, rows, :],
            send_sem=halo_send.at[send], recv_sem=halo_recv.at[dst_slot, p],
            device_id=genome(peer), device_id_type=MESH,
        )

    def near_copy(p):
        return halo_copy(reach, reach - even, p, parity, near, p)

    def back_copy(p):
        return halo_copy(reach, reach + 2 * even, p, parity, back, 4 + p - 2)

    def far_copy(p):
        return halo_copy(reach, reach - 2 * even, p, parity, far, 8 + p - 6)

    def relay_far(p):
        return halo_copy(reach + even, reach - even, p, 1 - parity, far, 10 + p)

    def relay_near(p):
        return halo_copy(reach + 2 * even, reach + even, p, parity, near, 12 + p - 2)

    def arrived(slot, p, odd):
        halo_copy(reach, slot, p, odd, near, 0).wait_recv()

    has_far, has_back = in_range(far), in_range(back)

    pl.semaphore_wait(barrier, expected)

    rounds = ((0, 2), (2, 3), (1, 4), (3, 5))

    def send_halo(rounds_here):
        for p, q in rounds_here:
            near_copy(p).start()

            @pl.when(has_back)
            def _(q=q):
                back_copy(q).start()

            if q < 4:
                @pl.when(has_far)
                def _(q=q):
                    far_copy(4 + q).start()

    other_core = {"anc": a + 1 - 2 * core}
    other_side = {"anc": lax.rem(a + 2, ancs)}
    up_copy = pltpu.make_async_remote_copy(
        src_ref=pair_out, dst_ref=pair_low, send_sem=pair_send.at[0], recv_sem=pair_recv.at[0],
        device_id=other_core, device_id_type=MESH,
    )
    over_copy = pltpu.make_async_remote_copy(
        src_ref=pair_out, dst_ref=pair_in, send_sem=pair_send.at[1], recv_sem=pair_recv.at[1],
        device_id=other_side, device_id_type=MESH,
    )
    down_copy = pltpu.make_async_remote_copy(
        src_ref=mean, dst_ref=mean, send_sem=pair_send.at[2], recv_sem=pair_recv.at[2],
        device_id=other_core, device_id_type=MESH,
    )

    send_halo(rounds[:1])

    @pl.when(core == 0)
    def _():
        send_halo(rounds[1:])

        @pl.when(side == 0)
        def _():
            pl.semaphore_signal(ready, inc=1, device_id={"anc": a + 2}, device_id_type=MESH)

    @pl.when(core == 1)
    def _():
        def round_tile(u, carry):
            cols = pl.ds(pl.multiple_of(u * tile, tile), tile)
            pair_out[:, cols] = coef[:, cols].astype(BF16)
            return carry

        lax.fori_loop(0, tiles, round_tile, 0, unroll=2)
        up_copy.start()

    def clear(first, last):
        def part(i, carry):
            at = pl.multiple_of(first + i * unit, unit)
            field[pl.ds(at, unit), :] = jnp.zeros((unit, traits_here), F32)
            return carry

        lax.fori_loop(0, (last - first) // unit, part, 0, unroll=4)

    clear(0, own_at)
    clear(own_at + snps, field.shape[0])

    for i, (d, m) in enumerate(stat_peers):
        @pl.when(jnp.logical_not(in_range(g - d)))
        def _(i=i):
            stats_in[i] = jnp.zeros(stats_in.shape[1:], F32)

    @pl.when(core == 0)
    def _():
        up_copy.wait_recv()

        def add(u, carry):
            cols = pl.ds(pl.multiple_of(u * tile, tile), tile)
            value = coef[:, cols] + pair_low[:, cols].astype(F32)
            mean[:, cols] = value
            pair_out[:, cols] = value.astype(BF16)
            return carry

        lax.fori_loop(0, tiles, add, 0, unroll=2)

        @pl.when(side == 1)
        def _():
            pl.semaphore_wait(ready, 1)

        over_copy.start()

    def pass_on(p):
        if p < 2:
            arrived(reach + even, p, 1 - parity)

            @pl.when(has_far)
            def _():
                relay_far(p).start()
        else:
            @pl.when(has_far)
            def _():
                arrived(reach + 2 * even, p, parity)
                relay_near(p).start()

    def widen(slot, p, same, i):
        at, size = piece(p, parity if same else 1 - parity)
        in_a = p in (0, 2, 4, 6)
        base = at_a[i] - first_a[1 - same] if in_a else at_b[i] - first_b[1 - same]

        def part(k, carry):
            r = pl.multiple_of(at + k * unit, unit)
            field[pl.ds(pl.multiple_of(base + r, unit), unit), :] = ext[slot, pl.ds(r, unit), :].astype(F32)
            return carry

        lax.fori_loop(0, size // unit, part, 0)

    def range_product(link, u, length, first, second=None):
        deep = length + 128
        within = pl.ds(pl.multiple_of(lax.rem(u, half) * tile, tile), tile)
        rows = pl.ds(pl.multiple_of(u * tile, tile), tile)
        begin = starts_ref[0, u] - g * snps + reach * snps
        where, at = first
        if second is not None:
            here = jnp.clip(begin + width - where, 0, 1) * jnp.clip(where + length - begin, 0, 1)
            where = second[0] + here * (where - second[0])
            at = second[1] + here * (at - second[1])
        skip = lax.div(jnp.clip(where - begin, 0, width - deep), 128) * 128
        from_row = at + jnp.clip(begin + skip - where, -deep, length)
        total = jnp.zeros((tile, traits_here), F32)
        for c in range(0, deep, 512):
            step = min(512, deep - c)
            window = field[pl.ds(from_row + c, step), :].astype(BF16)
            total = total + jnp.dot(
                link[within, pl.ds(skip + c, step)], window, preferred_element_type=F32
            )
        return rows, total

    def each_tile(body, parts=(0, 1), unroll=2):
        for i in parts:
            lax.fori_loop(i * half, (i + 1) * half, functools.partial(body, links[i]), 0, unroll=unroll)

    def own_tile(link, u, carry):
        rows, total = range_product(link, u, snps, (reach * snps, own_at))
        band[rows, :] = total
        return carry

    def own_pass(i):
        for u in range(i * half, (i + 1) * half):
            link_copy(u).wait()
        each_tile(own_tile, (i,))

    load_small[0].wait()
    own_pass(0)

    @pl.when(core == 0)
    def _():
        pass_on(0)
        pass_on(2)

    own_pass(1)

    @pl.when(core == 0)
    def _():
        pass_on(1)
        pass_on(3)
        pl.semaphore_signal(ready, inc=1, device_id=other_core, device_id_type=MESH)

    @pl.when(core == 1)
    def _():
        pl.semaphore_wait(ready, 1)
        send_halo(rounds[1:])
        pass_on(0)
        pass_on(2)

    def pair_product(link, u, slots_here, i, in_a):
        length, firsts, bases = (ahead, first_a, at_a) if in_a else (behind, first_b, at_b)
        return range_product(
            link, u, length,
            (slots_here[0] * snps + firsts[1], bases[i]), (slots_here[1] * snps + firsts[0], bases[i + 1]),
        )

    beside = (reach + even, reach - 2 * even)
    beyond = (reach - even, reach + 2 * even)

    def add_tile(link, u, carry, slots_here, i, in_a):
        rows, total = pair_product(link, u, slots_here, i, in_a)
        band[rows, :] = band[rows, :] + total
        return carry

    def beside_pass(in_a):
        for p in (0, 2) if in_a else (1, 3):
            widen(beside[0], p, 0, 0)

        @pl.when(has_back)
        def _():
            p = 6 if in_a else 7
            arrived(beside[1], p, parity)
            widen(beside[1], p, 1, 1)

        each_tile(functools.partial(add_tile, slots_here=beside, i=0, in_a=in_a), unroll=4)

    def beyond_ready(in_a):
        @pl.when(has_far)
        def _():
            arrived(beyond[1], 4 if in_a else 5, parity)
            for p in (2, 4) if in_a else (3, 5):
                widen(beyond[1], p, 1, 3)

        @pl.when(has_back)
        def _():
            for p in (0, 2) if in_a else (1, 3):
                arrived(beyond[0], p, 1 - parity)
                widen(beyond[0], p, 0, 2)

    arrived(beside[0], 2, 1 - parity)
    beside_pass(True)

    @pl.when(core == 1)
    def _():
        pass_on(1)
        pass_on(3)

    arrived(beside[0], 3, 1 - parity)
    beside_pass(False)
    beyond_ready(True)
    each_tile(functools.partial(add_tile, slots_here=beyond, i=2, in_a=True), unroll=4)

    @pl.when(core == 0)
    def _():
        over_copy.wait_recv()

        def add(u, carry):
            cols = pl.ds(pl.multiple_of(u * tile, tile), tile)
            mean[:, cols] = (mean[:, cols] + pair_in[:, cols].astype(F32)) / ancs
            return carry

        lax.fori_loop(0, tiles, add, 0, unroll=2)
        down_copy.start()

    @pl.when(core == 1)
    def _():
        down_copy.wait_recv()

    load_sums.wait()
    for load in load_small[1:]:
        load.wait()

    def prepare(u, carry):
        cols = pl.ds(pl.multiple_of(u * tile, tile), tile)
        proposal[:, cols] = (
            (1.0 - step_size - step_size * merging) * coef[:, cols]
            + step_size * sums[:, cols] + (step_size * merging) * mean[:, cols]
        )
        return carry

    lax.fori_loop(0, tiles, prepare, 0, unroll=2)

    beyond_ready(False)

    def last_tile(link, u, carry):
        rows, total = pair_product(link, u, beyond, 2, False)
        value = proposal[:, rows] - step_size * (band[rows, :] + total).T
        proposal[:, rows] = value
        row[:, rows] = jnp.sum(value * value, axis=0, keepdims=True)
        return carry

    each_tile(last_tile, unroll=4)

    lanes = stats_out.shape[1]
    mine = lax.broadcasted_iota(jnp.int32, (groups, snps), 0) == ids_ref[...]
    squares = jnp.sum(jnp.where(mine, row[...], 0.0), axis=1, keepdims=True)
    counts = jnp.sum(jnp.where(mine, 1.0, 0.0), axis=1, keepdims=True)
    on_lane = lax.broadcasted_iota(jnp.int32, (groups, lanes), 0) == lax.broadcasted_iota(
        jnp.int32, (groups, lanes), 1
    )
    stats_out[0:1, :] = jnp.sum(jnp.where(on_lane, squares, 0.0), axis=0, keepdims=True)
    stats_out[1:2, :] = jnp.sum(jnp.where(on_lane, counts, 0.0), axis=0, keepdims=True)

    def stats_copy(i):
        d, m = stat_peers[i]
        return pltpu.make_async_remote_copy(
            src_ref=stats_out, dst_ref=stats_in.at[i],
            send_sem=stats_send.at[i], recv_sem=stats_recv.at[i],
            device_id={**genome(g + d), "trait": lax.rem(t + m, traits_n)}, device_id_type=MESH,
        )

    for i, (d, m) in enumerate(stat_peers):
        @pl.when(in_range(g + d))
        def _(i=i):
            stats_copy(i).start()

    load_dosage.wait()
    for i, (d, m) in enumerate(stat_peers):
        @pl.when(in_range(g - d))
        def _(i=i):
            stats_copy(i).wait_recv()

    stats = stats_out[...]
    for i in range(len(stat_peers)):
        stats = stats + stats_in[i]
    all_squares = stats[0:1, :groups]
    all_counts = stats[1:2, :groups] / traits_n
    threshold = step_size * weight_ref[...] * jnp.sqrt(all_counts * (traits_here * traits_n))
    shrink = jnp.maximum(0.0, 1.0 - threshold / jnp.sqrt(all_squares + epsilon))
    same = lax.broadcasted_iota(jnp.int32, (groups, groups), 0) == lax.broadcasted_iota(
        jnp.int32, (groups, groups), 1
    )
    shrink = jnp.sum(jnp.where(same, shrink, 0.0), axis=1, keepdims=True)
    row[...] = jnp.sum(jnp.where(mine, shrink, 0.0), axis=0, keepdims=True)

    def shrink_tile(u, carry):
        cols = pl.ds(pl.multiple_of(u * tile, tile), tile)
        value = proposal[:, cols] * row[:, cols]
        updated_ref[0, :, cols] = value
        low[:, cols] = value.astype(BF16)
        return carry

    lax.fori_loop(0, tiles, shrink_tile, 0, unroll=2)

    scale = 1.0 / math.sqrt(snps * genomes)
    own_side, other_side_g = parity, lax.rem(near, 2)

    def pair_at(i):
        here = g // 2
        below, above = here, pairs - 1 - here
        wide = jnp.maximum(below, above)
        single = wide - jnp.minimum(below, above)
        up = 2 * jnp.clip(above - below, 0, 1) - 1
        alone = jnp.clip(single - i, 0, 1)
        two = jnp.maximum(i - single, 0)
        away = alone * (wide - i) + (1 - alone) * (wide - single - lax.div(two, 2))
        return here + up * (1 - 2 * (1 - alone) * lax.rem(two, 2)) * away

    cuts = side_out.shape[0] // pairs
    sub = side_out.shape[2]

    def partial(person, i):
        at = pl.ds(pl.multiple_of(person * persons_per + lax.rem(i, cuts) * sub, sub), sub)
        return lax.dot_general(
            low[...], dosage[at, :], (((1,), (1,)), ((), ())), preferred_element_type=F32
        ) * scale

    def side_copy(i):
        return pltpu.make_async_remote_copy(
            src_ref=side_out.at[i], dst_ref=side_in.at[i],
            send_sem=side_send.at[i], recv_sem=side_recv.at[i],
            device_id={"genome": near}, device_id_type=MESH,
        )

    def part_copy(i):
        to = pair_at(i // cuts)
        slot = (lax.rem(g // 2 - to + pairs, pairs) - 1) * cuts + lax.rem(i, cuts)
        return pltpu.make_async_remote_copy(
            src_ref=part_out.at[i], dst_ref=part_in.at[slot],
            send_sem=part_send.at[i], recv_sem=part_recv.at[slot],
            device_id={"genome": 2 * to + own_side}, device_id_type=MESH,
        )

    def part_arrived(i):
        return pltpu.make_async_remote_copy(
            src_ref=part_out.at[i], dst_ref=part_in.at[i],
            send_sem=part_send.at[i], recv_sem=part_recv.at[i],
            device_id={"genome": near}, device_id_type=MESH,
        )

    def send_side(i, carry):
        side_out[i] = partial(2 * pair_at(i // cuts) + other_side_g, i).astype(BF16)
        side_copy(i).start()
        return carry

    def pair_sum(i):
        mine_here = partial(2 * pair_at(i // cuts) + own_side, i)
        side_copy(i).wait_recv()
        return mine_here + side_in[i].astype(F32)

    def send_part(i, carry):
        part_out[i] = pair_sum(i).astype(BF16)
        part_copy(i).start()
        return carry

    n_side, n_part = pairs * cuts, (pairs - 1) * cuts
    lax.fori_loop(0, n_side, send_side, 0)
    lax.fori_loop(0, n_part, send_part, 0)

    totals = [pair_sum(n_part + c) for c in range(cuts)]
    for c in range(cuts):
        def add_part(k, total, c=c):
            part_arrived(k * cuts + c).wait_recv()
            return total + part_in[k * cuts + c].astype(F32)

        score_ref[0, :, c * sub:(c + 1) * sub] = lax.fori_loop(0, pairs - 1, add_part, totals[c])

    for p in range(4):
        near_copy(p).wait_send()

    @pl.when(has_back)
    def _():
        for p in (2, 3, 4, 5):
            back_copy(p).wait_send()

    @pl.when(has_far)
    def _():
        for p in (6, 7):
            far_copy(p).wait_send()
        for p in (0, 1):
            relay_far(p).wait_send()
        for p in (2, 3):
            relay_near(p).wait_send()

    @pl.when(core == 1)
    def _():
        up_copy.wait_send()

    @pl.when(core == 0)
    def _():
        over_copy.wait_send()
        down_copy.wait_send()

    for i, (d, m) in enumerate(stat_peers):
        @pl.when(in_range(g + d))
        def _(i=i):
            stats_copy(i).wait_send()

    def sent_side(i, carry):
        side_copy(i).wait_send()
        return carry

    def sent_part(i, carry):
        part_copy(i).wait_send()
        return carry

    lax.fori_loop(0, n_side, sent_side, 0)
    lax.fori_loop(0, n_part, sent_part, 0)


def store_kernel(updated_in, score_in, updated_out, score_out, sem):
    copies = [
        pltpu.make_async_copy(updated_in, updated_out, sem.at[0]),
        pltpu.make_async_copy(score_in, score_out, sem.at[1]),
    ]
    for copy in copies:
        copy.start()
    for copy in copies:
        copy.wait()


def per_device(coefficients, sumstats, linkage, band_start, group_ids, group_weight, dosage):
    _, traits_here, snps = coefficients.shape
    width = linkage.shape[2]
    genomes = lax.axis_size("genome")
    ancs = lax.axis_size("anc")
    traits_n = lax.axis_size("trait")
    persons = dosage.shape[1]
    persons_per = persons // genomes
    groups = group_weight.shape[1]
    reach = -(-width // snps)
    assert reach == 2 and genomes % 2 == 0 and coefficients.shape[0] == 1 and ancs == 4
    tile = snps // band_start.shape[1]
    slots = 2 * reach + 1
    pairs = genomes // 2
    field_rows = 11 * snps + 10 * 128
    group_reach = min(-(-longest_run // snps), genomes - 1)
    cuts = max(1, persons_per // 128)
    n_side, n_part = pairs * cuts, (pairs - 1) * cuts
    stat_n = (2 * group_reach + 1) * traits_n - 1
    lanes = -(-groups // 128) * 128
    sizes = (genomes, ancs, traits_n, reach, tile, groups)
    hbm = pl.BlockSpec(memory_space=pltpu.HBM)
    vmem = pl.BlockSpec(memory_space=pltpu.VMEM)
    dma = pltpu.SemaphoreType.DMA
    args = (coefficients, sumstats, linkage, band_start, group_ids, group_weight, dosage)
    args = tuple(pltpu.with_memory_space_constraint(x, pltpu.HBM) for x in args)
    out_shape = (
        jax.ShapeDtypeStruct((1, traits_here, snps), F32),
        jax.ShapeDtypeStruct((1, traits_here, persons_per), F32),
    )
    updated, scores = pl.pallas_call(
        functools.partial(step_kernel, sizes),
        out_shape=out_shape,
        in_specs=[hbm] * 7,
        out_specs=(vmem, vmem),
        scratch_shapes=[
            pltpu.VMEM((traits_here, snps), F32),
            pltpu.VMEM((traits_here, snps), F32),
            pltpu.VMEM((snps // 2, width), BF16),
            pltpu.VMEM((snps // 2, width), BF16),
            pltpu.SMEM(band_start.shape, jnp.int32),
            pltpu.VMEM(group_ids.shape, jnp.int32),
            pltpu.VMEM(group_weight.shape, F32),
            pltpu.VMEM((persons, snps), BF16),
            pltpu.VMEM((slots, snps, traits_here), BF16),
            pltpu.VMEM((field_rows, traits_here), F32),
            pltpu.VMEM((snps, traits_here), F32),
            pltpu.VMEM((traits_here, snps), F32),
            pltpu.VMEM((traits_here, snps), BF16),
            pltpu.VMEM((traits_here, snps), BF16),
            pltpu.VMEM((traits_here, snps), BF16),
            pltpu.VMEM((traits_here, snps), F32),
            pltpu.VMEM((traits_here, snps), BF16),
            pltpu.VMEM((1, snps), F32),
            pltpu.VMEM((2, lanes), F32),
            pltpu.VMEM((stat_n, 2, lanes), F32),
            pltpu.VMEM((n_side, traits_here, persons_per // cuts), BF16),
            pltpu.VMEM((n_side, traits_here, persons_per // cuts), BF16),
            pltpu.VMEM((n_part, traits_here, persons_per // cuts), BF16),
            pltpu.VMEM((n_part, traits_here, persons_per // cuts), BF16),
            dma((4,)), dma((5,)), dma((snps // tile,)), pltpu.SemaphoreType.REGULAR,
            dma((14,)), dma((slots, 8)), dma((3,)), dma((3,)),
            dma((stat_n,)), dma((stat_n,)), dma((n_side,)), dma((n_side,)), dma((n_part,)), dma((n_part,)),
        ],
        compiler_params=pltpu.CompilerParams(
            collective_id=0, has_side_effects=True, vmem_limit_bytes=52 * 1024 * 1024
        ),
    )(*args)
    return pl.pallas_call(
        store_kernel,
        out_shape=out_shape,
        in_specs=[vmem, vmem],
        out_specs=(hbm, hbm),
        scratch_shapes=[dma((2,))],
    )(*(pltpu.with_memory_space_constraint(x, pltpu.VMEM) for x in (updated, scores)))


def solution(mesh):
    in_specs = (
        P("anc", "trait", "genome"),
        P("anc", "trait", "genome"),
        P("anc", "genome", None),
        P("anc", "genome"),
        P("anc", "genome"),
        P("anc", None),
        P("anc", None, "genome"),
    )
    out_specs = (P("anc", "trait", "genome"), P("anc", "trait", "genome"))
    return jax.shard_map(
        per_device, mesh=mesh, in_specs=in_specs, out_specs=out_specs, check_vma=False
    )
```

```python
import functools
import math

import jax
import jax.numpy as jnp
from jax import lax
from jax.experimental import pallas as pl
from jax.experimental.pallas import tpu as pltpu
from jax.sharding import PartitionSpec as P

step_size = 0.5
merging = 0.5
epsilon = 1e-06
longest_run = 8192

MESH = pl.DeviceIdType.MESH
F32 = jnp.float32
BF16 = jnp.bfloat16


def step_kernel(
    sizes,
    coef_hbm, sums_hbm, link_hbm, starts_hbm, ids_hbm, weight_hbm, dosage_hbm,
    updated_ref, score_ref,
    coef, sums, link_first, link_second, starts_ref, ids_ref, weight_ref, dosage, ext, field, band, mean, pair_out, pair_low, pair_in,
    proposal, low, row, stats_out, stats_in, side_out, side_in, part_out, part_in,
    coef_sem, load_sem, link_sem, ready,
    halo_send, halo_recv, pair_send, pair_recv, stats_send, stats_recv, side_send, side_recv, part_send, part_recv,
):
    genomes, ancs, traits_n, reach, tile, groups = sizes
    traits_here, snps = coef.shape
    links = (link_first, link_second)
    width = link_first.shape[1]
    tiles = snps // tile
    half = tiles // 2
    persons_per = dosage.shape[0] // genomes
    pairs = genomes // 2
    g = lax.axis_index("genome")
    a = lax.axis_index("anc")
    t = lax.axis_index("trait")
    core, side = lax.rem(a, 2), a // 2
    parity = lax.rem(g, 2)
    even = 1 - 2 * parity
    near, far, back, across = g + even, g + 2 * even, g - 2 * even, g - even

    def in_range(p):
        return jnp.logical_and(p >= 0, p < genomes)

    def genome(p):
        return {"genome": jnp.clip(p, 0, genomes - 1)}

    group_reach = min(-(-longest_run // snps), genomes - 1)
    stat_peers = [
        (d, m) for m in range(traits_n) for d in range(-group_reach, group_reach + 1) if (d, m) != (0, 0)
    ]
    if genomes > 8 or traits_n > 1:
        greet = [(k, m) for m in range(traits_n) for k in range(genomes) if (k, m) != (0, 0)]
    else:
        greet = []

    coef_parts = coef_sem.shape[0]
    part_cols = snps // coef_parts

    def coef_copy(i):
        cols = pl.ds(i * part_cols, part_cols)
        return pltpu.make_async_copy(coef_hbm.at[0, :, cols], coef.at[:, cols], coef_sem.at[i])

    for i in range(coef_parts):
        coef_copy(i).start()
    barrier = pltpu.get_barrier_semaphore()
    if greet:
        for k, m in greet:
            pl.semaphore_signal(
                barrier, inc=1, device_id_type=MESH,
                device_id={"genome": lax.rem(g + k, genomes), "trait": lax.rem(t + m, traits_n)},
            )
        expected = len(greet)
    else:
        pl.semaphore_signal(barrier, inc=1, device_id=genome(near), device_id_type=MESH)
        for peer in (far, back):
            @pl.when(in_range(peer))
            def _(peer=peer):
                pl.semaphore_signal(barrier, inc=1, device_id=genome(peer), device_id_type=MESH)
        expected = 1 + in_range(far).astype(jnp.int32) + in_range(back).astype(jnp.int32)

    @pl.when(core == 0)
    def _():
        pl.semaphore_signal(barrier, inc=1, device_id={"anc": a + 1}, device_id_type=MESH)

    @pl.when(jnp.logical_and(core == 0, side == 1))
    def _():
        pl.semaphore_signal(barrier, inc=1, device_id={"anc": a - 2}, device_id_type=MESH)

    expected = expected + core + (1 - core) * (1 - side)

    load_small = [
        pltpu.make_async_copy(starts_hbm, starts_ref, load_sem.at[0]),
        pltpu.make_async_copy(ids_hbm, ids_ref, load_sem.at[1]),
        pltpu.make_async_copy(weight_hbm, weight_ref, load_sem.at[2]),
    ]
    load_sums = pltpu.make_async_copy(sums_hbm.at[0], sums, load_sem.at[3])
    load_dosage = pltpu.make_async_copy(dosage_hbm.at[0], dosage, load_sem.at[4])

    def link_copy(u):
        return pltpu.make_async_copy(
            link_hbm.at[0, pl.ds(u * tile, tile), :], links[u // half].at[pl.ds(u % half * tile, tile), :],
            link_sem.at[u],
        )

    unit = snps // 16
    far_rows = width - tile - snps
    ahead = 11 * unit
    behind = snps - ahead
    ahead = 11 * unit
    behind = snps - ahead
    own_at = snps + 128
    at_a = [own_at + 2 * snps + 128 + i * (2 * ahead + 128) for i in range(4)]
    at_b = [at_a[3] + 2 * ahead + 128 + i * (2 * behind + 128) for i in range(4)]
    assert at_b[3] + 2 * behind + 128 == field.shape[0] and 13 * unit < far_rows <= 16 * unit
    first_a = (parity * behind, (1 - parity) * behind)
    first_b = ((1 - parity) * ahead, parity * ahead)

    def own_block(u, carry):
        cols = pl.ds(pl.multiple_of(u * tile, tile), tile)
        flat = coef[:, cols].T.astype(BF16)
        ext[reach, cols, :] = flat
        field[pl.ds(pl.multiple_of(own_at + u * tile, unit), tile), :] = flat.astype(F32)
        return carry

    for i in range(coef_parts):
        coef_copy(i).wait()
        if i == coef_parts - 1:
            for load in load_small:
                load.start()
            for u in range(tiles):
                link_copy(u).start()
            load_sums.start()
            load_dosage.start()
        lax.fori_loop(i * tiles // coef_parts, (i + 1) * tiles // coef_parts, own_block, 0, unroll=2)

    pieces = [
        (5 * unit, 6 * unit), (13 * unit, 3 * unit), (0, 5 * unit), (11 * unit, 2 * unit),
        (5 * unit, 6 * unit), (13 * unit, far_rows - 13 * unit),
        (snps - far_rows, ahead + far_rows - snps), (ahead, behind),
    ]

    def piece(p, odd):
        at, size = pieces[p]
        return pl.multiple_of((1 - odd) * at + odd * (snps - at - size), unit), size

    def halo_copy(src_slot, dst_slot, p, odd, peer, send):
        at, size = piece(p, odd)
        rows = pl.ds(at, size)
        return pltpu.make_async_remote_copy(
            src_ref=ext.at[src_slot, rows, :], dst_ref=ext.at[dst_slot, rows, :],
            send_sem=halo_send.at[send], recv_sem=halo_recv.at[dst_slot, p],
            device_id=genome(peer), device_id_type=MESH,
        )

    def near_copy(p):
        return halo_copy(reach, reach - even, p, parity, near, p)

    def back_copy(p):
        return halo_copy(reach, reach + 2 * even, p, parity, back, 4 + p - 2)

    def far_copy(p):
        return halo_copy(reach, reach - 2 * even, p, parity, far, 8 + p - 6)

    def relay_far(p):
        return halo_copy(reach + even, reach - even, p, 1 - parity, far, 10 + p)

    def relay_near(p):
        return halo_copy(reach + 2 * even, reach + even, p, parity, near, 12 + p - 2)

    def arrived(slot, p, odd):
        halo_copy(reach, slot, p, odd, near, 0).wait_recv()

    has_far, has_back = in_range(far), in_range(back)

    pl.semaphore_wait(barrier, expected)

    def send_halo(nears, backs, fars):
        for k in range(4):
            for p in nears[k:k + 1]:
                near_copy(p).start()
            for p in backs[k:k + 1]:
                @pl.when(has_back)
                def _(p=p):
                    back_copy(p).start()
            for p in fars[k:k + 1]:
                @pl.when(has_far)
                def _(p=p):
                    far_copy(p).start()

    other_core = {"anc": a + 1 - 2 * core}
    other_side = {"anc": lax.rem(a + 2, ancs)}
    up_copy = pltpu.make_async_remote_copy(
        src_ref=pair_out, dst_ref=pair_low, send_sem=pair_send.at[0], recv_sem=pair_recv.at[0],
        device_id=other_core, device_id_type=MESH,
    )
    over_copy = pltpu.make_async_remote_copy(
        src_ref=pair_out, dst_ref=pair_in, send_sem=pair_send.at[1], recv_sem=pair_recv.at[1],
        device_id=other_side, device_id_type=MESH,
    )
    down_copy = pltpu.make_async_remote_copy(
        src_ref=mean, dst_ref=mean, send_sem=pair_send.at[2], recv_sem=pair_recv.at[2],
        device_id=other_core, device_id_type=MESH,
    )

    @pl.when(core == 0)
    def _():
        send_halo((0, 2, 1, 3), (2, 3, 4, 5), (6, 7))

        @pl.when(side == 0)
        def _():
            pl.semaphore_signal(ready, inc=1, device_id={"anc": a + 2}, device_id_type=MESH)

    @pl.when(core == 1)
    def _():
        send_halo((0,), (2,), (6,))

        def round_tile(u, carry):
            cols = pl.ds(pl.multiple_of(u * tile, tile), tile)
            pair_out[:, cols] = coef[:, cols].astype(BF16)
            return carry

        lax.fori_loop(0, tiles, round_tile, 0, unroll=2)
        up_copy.start()

    def clear(first, last):
        def part(i, carry):
            at = pl.multiple_of(first + i * unit, unit)
            field[pl.ds(at, unit), :] = jnp.zeros((unit, traits_here), F32)
            return carry

        lax.fori_loop(0, (last - first) // unit, part, 0, unroll=4)

    clear(0, own_at)
    clear(own_at + snps, field.shape[0])

    for i, (d, m) in enumerate(stat_peers):
        @pl.when(jnp.logical_not(in_range(g - d)))
        def _(i=i):
            stats_in[i] = jnp.zeros(stats_in.shape[1:], F32)

    @pl.when(core == 0)
    def _():
        up_copy.wait_recv()

        def add(u, carry):
            cols = pl.ds(pl.multiple_of(u * tile, tile), tile)
            value = coef[:, cols] + pair_low[:, cols].astype(F32)
            mean[:, cols] = value
            pair_out[:, cols] = value.astype(BF16)
            return carry

        lax.fori_loop(0, tiles, add, 0, unroll=2)

        @pl.when(side == 1)
        def _():
            pl.semaphore_wait(ready, 1)

        over_copy.start()

    def pass_on(p):
        if p < 2:
            arrived(reach + even, p, 1 - parity)

            @pl.when(has_far)
            def _():
                relay_far(p).start()
        else:
            @pl.when(has_far)
            def _():
                arrived(reach + 2 * even, p, parity)
                relay_near(p).start()

    def widen(slot, p, same, i):
        at, size = piece(p, parity if same else 1 - parity)
        in_a = p in (0, 2, 4, 6)
        base = at_a[i] - first_a[1 - same] if in_a else at_b[i] - first_b[1 - same]

        def part(k, carry):
            r = pl.multiple_of(at + k * unit, unit)
            field[pl.ds(pl.multiple_of(base + r, unit), unit), :] = ext[slot, pl.ds(r, unit), :].astype(F32)
            return carry

        lax.fori_loop(0, size // unit, part, 0)

    def range_product(link, u, length, first, second=None):
        deep = length + 128
        within = pl.ds(pl.multiple_of(lax.rem(u, half) * tile, tile), tile)
        rows = pl.ds(pl.multiple_of(u * tile, tile), tile)
        begin = starts_ref[0, u] - g * snps + reach * snps
        where, at = first
        if second is not None:
            here = jnp.clip(begin + width - where, 0, 1) * jnp.clip(where + length - begin, 0, 1)
            where = second[0] + here * (where - second[0])
            at = second[1] + here * (at - second[1])
        skip = lax.div(jnp.clip(where - begin, 0, width - deep), 128) * 128
        from_row = at + jnp.clip(begin + skip - where, -deep, length)
        total = jnp.zeros((tile, traits_here), F32)
        for c in range(0, deep, 512):
            step = min(512, deep - c)
            window = field[pl.ds(from_row + c, step), :].astype(BF16)
            total = total + jnp.dot(
                link[within, pl.ds(skip + c, step)], window, preferred_element_type=F32
            )
        return rows, total

    def each_tile(body, parts=(0, 1), unroll=2):
        for i in parts:
            lax.fori_loop(i * half, (i + 1) * half, functools.partial(body, links[i]), 0, unroll=unroll)

    def own_tile(link, u, carry):
        rows, total = range_product(link, u, snps, (reach * snps, own_at))
        band[rows, :] = total
        return carry

    def own_pass(i):
        for u in range(i * half, (i + 1) * half):
            link_copy(u).wait()
        each_tile(own_tile, (i,))

    load_small[0].wait()
    own_pass(0)

    @pl.when(core == 0)
    def _():
        pass_on(0)
        pass_on(2)

    own_pass(1)

    @pl.when(core == 0)
    def _():
        pl.semaphore_signal(ready, inc=1, device_id=other_core, device_id_type=MESH)

    @pl.when(core == 1)
    def _():
        pl.semaphore_wait(ready, 1)
        send_halo((2,), (), ())
        pl.semaphore_wait(ready, 1)
        send_halo((1, 3), (3, 4, 5), (7,))
        pass_on(0)
        pass_on(2)

    def pair_product(link, u, slots_here, i, in_a):
        length, firsts, bases = (ahead, first_a, at_a) if in_a else (behind, first_b, at_b)
        return range_product(
            link, u, length,
            (slots_here[0] * snps + firsts[1], bases[i]), (slots_here[1] * snps + firsts[0], bases[i + 1]),
        )

    beside = (reach + even, reach - 2 * even)
    beyond = (reach - even, reach + 2 * even)

    def add_tile(link, u, carry, slots_here, i, in_a):
        rows, total = pair_product(link, u, slots_here, i, in_a)
        band[rows, :] = band[rows, :] + total
        return carry

    def beside_pass(in_a):
        for p in (0, 2) if in_a else (1, 3):
            widen(beside[0], p, 0, 0)

        @pl.when(has_back)
        def _():
            p = 6 if in_a else 7
            arrived(beside[1], p, parity)
            widen(beside[1], p, 1, 1)

        each_tile(functools.partial(add_tile, slots_here=beside, i=0, in_a=in_a), unroll=4)

    def beyond_ready(in_a):
        @pl.when(has_far)
        def _():
            arrived(beyond[1], 4 if in_a else 5, parity)
            for p in (2, 4) if in_a else (3, 5):
                widen(beyond[1], p, 1, 3)

        @pl.when(has_back)
        def _():
            for p in (0, 2) if in_a else (1, 3):
                arrived(beyond[0], p, 1 - parity)
                widen(beyond[0], p, 0, 2)

    arrived(beside[0], 2, 1 - parity)
    beside_pass(True)
    pass_on(1)
    pass_on(3)

    @pl.when(core == 0)
    def _():
        pl.semaphore_signal(ready, inc=1, device_id=other_core, device_id_type=MESH)

    arrived(beside[0], 3, 1 - parity)
    beside_pass(False)
    beyond_ready(True)
    each_tile(functools.partial(add_tile, slots_here=beyond, i=2, in_a=True), unroll=4)

    @pl.when(core == 0)
    def _():
        over_copy.wait_recv()

        def add(u, carry):
            cols = pl.ds(pl.multiple_of(u * tile, tile), tile)
            mean[:, cols] = (mean[:, cols] + pair_in[:, cols].astype(F32)) / ancs
            return carry

        lax.fori_loop(0, tiles, add, 0, unroll=2)
        down_copy.start()

    @pl.when(core == 1)
    def _():
        down_copy.wait_recv()

    load_sums.wait()
    for load in load_small[1:]:
        load.wait()

    def prepare(u, carry):
        cols = pl.ds(pl.multiple_of(u * tile, tile), tile)
        proposal[:, cols] = (
            (1.0 - step_size - step_size * merging) * coef[:, cols]
            + step_size * sums[:, cols] + (step_size * merging) * mean[:, cols]
        )
        return carry

    lax.fori_loop(0, tiles, prepare, 0, unroll=2)

    lanes = stats_out.shape[1]
    mine = lax.broadcasted_iota(jnp.int32, (groups, snps), 0) == ids_ref[...]
    counts = jnp.sum(jnp.where(mine, 1.0, 0.0), axis=1, keepdims=True)
    on_lane = lax.broadcasted_iota(jnp.int32, (groups, lanes), 0) == lax.broadcasted_iota(
        jnp.int32, (groups, lanes), 1
    )
    stats_out[1:2, :] = jnp.sum(jnp.where(on_lane, counts, 0.0), axis=0, keepdims=True)

    beyond_ready(False)

    def last_tile(link, u, carry):
        rows, total = pair_product(link, u, beyond, 2, False)
        value = proposal[:, rows] - step_size * (band[rows, :] + total).T
        proposal[:, rows] = value
        row[:, rows] = jnp.sum(value * value, axis=0, keepdims=True)
        return carry

    each_tile(last_tile, unroll=4)

    squares = jnp.sum(jnp.where(mine, row[...], 0.0), axis=1, keepdims=True)
    stats_out[0:1, :] = jnp.sum(jnp.where(on_lane, squares, 0.0), axis=0, keepdims=True)

    def stats_copy(i):
        d, m = stat_peers[i]
        return pltpu.make_async_remote_copy(
            src_ref=stats_out, dst_ref=stats_in.at[i],
            send_sem=stats_send.at[i], recv_sem=stats_recv.at[i],
            device_id={**genome(g + d), "trait": lax.rem(t + m, traits_n)}, device_id_type=MESH,
        )

    for i, (d, m) in enumerate(stat_peers):
        @pl.when(in_range(g + d))
        def _(i=i):
            stats_copy(i).start()

    load_dosage.wait()
    for i, (d, m) in enumerate(stat_peers):
        @pl.when(in_range(g - d))
        def _(i=i):
            stats_copy(i).wait_recv()

    stats = stats_out[...]
    for i in range(len(stat_peers)):
        stats = stats + stats_in[i]
    all_squares = stats[0:1, :groups]
    all_counts = stats[1:2, :groups] / traits_n
    threshold = step_size * weight_ref[...] * jnp.sqrt(all_counts * (traits_here * traits_n))
    shrink = jnp.maximum(0.0, 1.0 - threshold / jnp.sqrt(all_squares + epsilon))
    same = lax.broadcasted_iota(jnp.int32, (groups, groups), 0) == lax.broadcasted_iota(
        jnp.int32, (groups, groups), 1
    )
    shrink = jnp.sum(jnp.where(same, shrink, 0.0), axis=1, keepdims=True)
    row[...] = jnp.sum(jnp.where(mine, shrink, 0.0), axis=0, keepdims=True)

    def shrink_tile(u, carry):
        cols = pl.ds(pl.multiple_of(u * tile, tile), tile)
        value = proposal[:, cols] * row[:, cols]
        updated_ref[0, :, cols] = value
        low[:, cols] = value.astype(BF16)
        return carry

    lax.fori_loop(0, tiles, shrink_tile, 0, unroll=2)

    scale = 1.0 / math.sqrt(snps * genomes)
    own_side, other_side_g = parity, lax.rem(near, 2)

    def pair_at(i):
        here = g // 2
        is_last = jnp.clip(i - (pairs - 2), 0, 1)
        return (1 - is_last) * (i + jnp.clip(i - here + 1, 0, 1)) + is_last * here

    cuts = side_out.shape[1]
    sub = traits_here // cuts
    last_pair = pairs - 1

    def partial(person):
        at = pl.ds(pl.multiple_of(person * persons_per, persons_per), persons_per)
        return lax.dot_general(
            low[...], dosage[at, :], (((1,), (1,)), ((), ())), preferred_element_type=F32
        ) * scale

    def side_copy(i, c):
        return pltpu.make_async_remote_copy(
            src_ref=side_out.at[i, c], dst_ref=side_in.at[i, c],
            send_sem=side_send.at[i, c], recv_sem=side_recv.at[i, c],
            device_id={"genome": near}, device_id_type=MESH,
        )

    def part_copy(i, c):
        to = pair_at(i)
        slot = lax.rem(g // 2 - to + pairs, pairs) - 1
        return pltpu.make_async_remote_copy(
            src_ref=part_out.at[i, c], dst_ref=part_in.at[slot, c],
            send_sem=part_send.at[i, c], recv_sem=part_recv.at[slot, c],
            device_id={"genome": 2 * to + own_side}, device_id_type=MESH,
        )

    def part_arrived(i, c):
        return pltpu.make_async_remote_copy(
            src_ref=part_out.at[i, c], dst_ref=part_in.at[i, c],
            send_sem=part_send.at[i, c], recv_sem=part_recv.at[i, c],
            device_id={"genome": near}, device_id_type=MESH,
        )

    def send_side(i, carry):
        value = partial(2 * pair_at(i) + other_side_g).astype(BF16)
        for c in range(cuts):
            side_out[i, c] = value[c * sub:(c + 1) * sub]
            side_copy(i, c).start()
        return carry

    def send_part(i, carry):
        mine_here = partial(2 * pair_at(i) + own_side)
        for c in range(cuts):
            side_copy(i, c).wait_recv()
            part_out[i, c] = (mine_here[c * sub:(c + 1) * sub] + side_in[i, c].astype(F32)).astype(BF16)
            part_copy(i, c).start()
        return carry

    lax.fori_loop(0, pairs, send_side, 0)
    lax.fori_loop(0, last_pair, send_part, 0)

    last = partial(2 * pair_at(last_pair) + own_side)
    for c in range(cuts):
        side_copy(last_pair, c).wait_recv()

        def add_part(k, total, c=c):
            part_arrived(k, c).wait_recv()
            return total + part_in[k, c].astype(F32)

        own_total = last[c * sub:(c + 1) * sub] + side_in[last_pair, c].astype(F32)
        score_ref[0, c * sub:(c + 1) * sub, :] = lax.fori_loop(0, pairs - 1, add_part, own_total)

    for p in range(4):
        near_copy(p).wait_send()

    @pl.when(has_back)
    def _():
        for p in (2, 3, 4, 5):
            back_copy(p).wait_send()

    @pl.when(has_far)
    def _():
        for p in (6, 7):
            far_copy(p).wait_send()
        for p in (0, 1):
            relay_far(p).wait_send()
        for p in (2, 3):
            relay_near(p).wait_send()

    @pl.when(core == 1)
    def _():
        up_copy.wait_send()

    @pl.when(core == 0)
    def _():
        over_copy.wait_send()
        down_copy.wait_send()

    for i, (d, m) in enumerate(stat_peers):
        @pl.when(in_range(g + d))
        def _(i=i):
            stats_copy(i).wait_send()

    def sent_side(i, carry):
        for c in range(cuts):
            side_copy(i, c).wait_send()
        return carry

    def sent_part(i, carry):
        for c in range(cuts):
            part_copy(i, c).wait_send()
        return carry

    lax.fori_loop(0, pairs, sent_side, 0)
    lax.fori_loop(0, pairs - 1, sent_part, 0)


def store_kernel(updated_in, score_in, updated_out, score_out, sem):
    parts = sem.shape[0] - 1
    rows = updated_in.shape[1] // parts
    copies = [pltpu.make_async_copy(score_in, score_out, sem.at[parts])]
    for i in range(parts):
        part = pl.ds(i * rows, rows)
        copies.append(pltpu.make_async_copy(updated_in.at[:, part], updated_out.at[:, part], sem.at[i]))
    for copy in copies:
        copy.start()
    for copy in copies:
        copy.wait()


def per_device(coefficients, sumstats, linkage, band_start, group_ids, group_weight, dosage):
    _, traits_here, snps = coefficients.shape
    width = linkage.shape[2]
    genomes = lax.axis_size("genome")
    ancs = lax.axis_size("anc")
    traits_n = lax.axis_size("trait")
    persons = dosage.shape[1]
    persons_per = persons // genomes
    groups = group_weight.shape[1]
    reach = -(-width // snps)
    assert reach == 2 and genomes % 2 == 0 and coefficients.shape[0] == 1 and ancs == 4
    tile = snps // band_start.shape[1]
    slots = 2 * reach + 1
    pairs = genomes // 2
    field_rows = 11 * snps + 10 * 128
    group_reach = min(-(-longest_run // snps), genomes - 1)
    cuts = 2
    stat_n = (2 * group_reach + 1) * traits_n - 1
    lanes = -(-groups // 128) * 128
    sizes = (genomes, ancs, traits_n, reach, tile, groups)
    hbm = pl.BlockSpec(memory_space=pltpu.HBM)
    vmem = pl.BlockSpec(memory_space=pltpu.VMEM)
    dma = pltpu.SemaphoreType.DMA
    args = (coefficients, sumstats, linkage, band_start, group_ids, group_weight, dosage)
    args = tuple(pltpu.with_memory_space_constraint(x, pltpu.HBM) for x in args)
    out_shape = (
        jax.ShapeDtypeStruct((1, traits_here, snps), F32),
        jax.ShapeDtypeStruct((1, traits_here, persons_per), F32),
    )
    updated, scores = pl.pallas_call(
        functools.partial(step_kernel, sizes),
        out_shape=out_shape,
        in_specs=[hbm] * 7,
        out_specs=(vmem, vmem),
        scratch_shapes=[
            pltpu.VMEM((traits_here, snps), F32),
            pltpu.VMEM((traits_here, snps), F32),
            pltpu.VMEM((snps // 2, width), BF16),
            pltpu.VMEM((snps // 2, width), BF16),
            pltpu.SMEM(band_start.shape, jnp.int32),
            pltpu.VMEM(group_ids.shape, jnp.int32),
            pltpu.VMEM(group_weight.shape, F32),
            pltpu.VMEM((persons, snps), BF16),
            pltpu.VMEM((slots, snps, traits_here), BF16),
            pltpu.VMEM((field_rows, traits_here), F32),
            pltpu.VMEM((snps, traits_here), F32),
            pltpu.VMEM((traits_here, snps), F32),
            pltpu.VMEM((traits_here, snps), BF16),
            pltpu.VMEM((traits_here, snps), BF16),
            pltpu.VMEM((traits_here, snps), BF16),
            pltpu.VMEM((traits_here, snps), F32),
            pltpu.VMEM((traits_here, snps), BF16),
            pltpu.VMEM((1, snps), F32),
            pltpu.VMEM((2, lanes), F32),
            pltpu.VMEM((stat_n, 2, lanes), F32),
            pltpu.VMEM((pairs, cuts, traits_here // cuts, persons_per), BF16),
            pltpu.VMEM((pairs, cuts, traits_here // cuts, persons_per), BF16),
            pltpu.VMEM((pairs - 1, cuts, traits_here // cuts, persons_per), BF16),
            pltpu.VMEM((pairs - 1, cuts, traits_here // cuts, persons_per), BF16),
            dma((4,)), dma((5,)), dma((snps // tile,)), pltpu.SemaphoreType.REGULAR,
            dma((14,)), dma((slots, 8)), dma((3,)), dma((3,)),
            dma((stat_n,)), dma((stat_n,)), dma((pairs, cuts)), dma((pairs, cuts)), dma((pairs - 1, cuts)), dma((pairs - 1, cuts)),
        ],
        compiler_params=pltpu.CompilerParams(
            collective_id=0, has_side_effects=True, vmem_limit_bytes=52 * 1024 * 1024
        ),
    )(*args)
    return pl.pallas_call(
        store_kernel,
        out_shape=out_shape,
        in_specs=[vmem, vmem],
        out_specs=(hbm, hbm),
        scratch_shapes=[dma((5,))],
    )(*(pltpu.with_memory_space_constraint(x, pltpu.VMEM) for x in (updated, scores)))


def solution(mesh):
    in_specs = (
        P("anc", "trait", "genome"),
        P("anc", "trait", "genome"),
        P("anc", "genome", None),
        P("anc", "genome"),
        P("anc", "genome"),
        P("anc", None),
        P("anc", None, "genome"),
    )
    out_specs = (P("anc", "trait", "genome"), P("anc", "trait", "genome"))
    return jax.shard_map(
        per_device, mesh=mesh, in_specs=in_specs, out_specs=out_specs, check_vma=False
    )
```

```python
import functools
import math

import jax
import jax.numpy as jnp
from jax import lax
from jax.experimental import pallas as pl
from jax.experimental.pallas import tpu as pltpu
from jax.sharding import PartitionSpec as P

step_size = 0.5
merging = 0.5
epsilon = 1e-06
longest_run = 8192

MESH = pl.DeviceIdType.MESH
F32 = jnp.float32
BF16 = jnp.bfloat16


def step_kernel(
    sizes,
    coef_hbm, sums_hbm, link_hbm, starts_hbm, ids_hbm, weight_hbm, dosage_hbm,
    updated_ref, score_ref,
    coef, sums, link_first, link_second, starts_ref, ids_ref, weight_ref, dosage, ext, field, band, mean, pair_out, pair_low, pair_in,
    proposal, low, row, stats_out, stats_in, side_out, side_in, part_out, part_in,
    coef_sem, load_sem, link_sem, ready,
    halo_send, halo_recv, pair_send, pair_recv, stats_send, stats_recv, side_send, side_recv, part_send, part_recv,
):
    genomes, ancs, traits_n, reach, tile, groups = sizes
    traits_here, snps = coef.shape
    links = (link_first, link_second)
    width = link_first.shape[1]
    tiles = snps // tile
    half = tiles // 2
    persons_per = dosage.shape[0] // genomes
    pairs = genomes // 2
    g = lax.axis_index("genome")
    a = lax.axis_index("anc")
    t = lax.axis_index("trait")
    core, side = lax.rem(a, 2), a // 2
    parity = lax.rem(g, 2)
    even = 1 - 2 * parity
    near, far, back, across = g + even, g + 2 * even, g - 2 * even, g - even

    def in_range(p):
        return jnp.logical_and(p >= 0, p < genomes)

    def genome(p):
        return {"genome": jnp.clip(p, 0, genomes - 1)}

    group_reach = min(-(-longest_run // snps), genomes - 1)
    stat_peers = [
        (d, m) for m in range(traits_n) for d in range(-group_reach, group_reach + 1) if (d, m) != (0, 0)
    ]
    if genomes > 8 or traits_n > 1:
        greet = [(k, m) for m in range(traits_n) for k in range(genomes) if (k, m) != (0, 0)]
    else:
        greet = []

    coef_parts = coef_sem.shape[0]
    part_cols = snps // coef_parts

    def coef_copy(i):
        cols = pl.ds(i * part_cols, part_cols)
        return pltpu.make_async_copy(coef_hbm.at[0, :, cols], coef.at[:, cols], coef_sem.at[i])

    for i in range(coef_parts):
        coef_copy(i).start()
    barrier = pltpu.get_barrier_semaphore()
    if greet:
        for k, m in greet:
            pl.semaphore_signal(
                barrier, inc=1, device_id_type=MESH,
                device_id={"genome": lax.rem(g + k, genomes), "trait": lax.rem(t + m, traits_n)},
            )
        expected = len(greet)
    else:
        pl.semaphore_signal(barrier, inc=1, device_id=genome(near), device_id_type=MESH)
        for peer in (far, back):
            @pl.when(in_range(peer))
            def _(peer=peer):
                pl.semaphore_signal(barrier, inc=1, device_id=genome(peer), device_id_type=MESH)
        expected = 1 + in_range(far).astype(jnp.int32) + in_range(back).astype(jnp.int32)

    @pl.when(core == 0)
    def _():
        pl.semaphore_signal(barrier, inc=1, device_id={"anc": a + 1}, device_id_type=MESH)

    @pl.when(jnp.logical_and(core == 0, side == 1))
    def _():
        pl.semaphore_signal(barrier, inc=1, device_id={"anc": a - 2}, device_id_type=MESH)

    expected = expected + core + (1 - core) * (1 - side)

    load_small = [
        pltpu.make_async_copy(starts_hbm, starts_ref, load_sem.at[0]),
        pltpu.make_async_copy(ids_hbm, ids_ref, load_sem.at[1]),
        pltpu.make_async_copy(weight_hbm, weight_ref, load_sem.at[2]),
    ]
    load_sums = pltpu.make_async_copy(sums_hbm.at[0], sums, load_sem.at[3])
    load_dosage = pltpu.make_async_copy(dosage_hbm.at[0], dosage, load_sem.at[4])

    def link_copy(u):
        return pltpu.make_async_copy(
            link_hbm.at[0, pl.ds(u * tile, tile), :], links[u // half].at[pl.ds(u % half * tile, tile), :],
            link_sem.at[u],
        )

    unit = snps // 16
    far_rows = width - tile - snps
    ahead = 11 * unit
    behind = snps - ahead
    ahead = 11 * unit
    behind = snps - ahead
    own_at = snps + 128
    at_a = [own_at + 2 * snps + 128 + i * (2 * ahead + 128) for i in range(4)]
    at_b = [at_a[3] + 2 * ahead + 128 + i * (2 * behind + 128) for i in range(4)]
    assert at_b[3] + 2 * behind + 128 == field.shape[0] and 13 * unit < far_rows <= 16 * unit
    first_a = (parity * behind, (1 - parity) * behind)
    first_b = ((1 - parity) * ahead, parity * ahead)

    def own_block(u, carry):
        cols = pl.ds(pl.multiple_of(u * tile, tile), tile)
        flat = coef[:, cols].T.astype(BF16)
        ext[reach, cols, :] = flat
        field[pl.ds(pl.multiple_of(own_at + u * tile, unit), tile), :] = flat.astype(F32)
        return carry

    for i in range(coef_parts):
        coef_copy(i).wait()
        if i == coef_parts - 1:
            for load in load_small:
                load.start()
            for u in range(tiles):
                link_copy(u).start()
            load_sums.start()
            load_dosage.start()
        lax.fori_loop(i * tiles // coef_parts, (i + 1) * tiles // coef_parts, own_block, 0, unroll=2)

    pieces = [
        (5 * unit, 6 * unit), (13 * unit, 3 * unit), (0, 5 * unit), (11 * unit, 2 * unit),
        (5 * unit, 6 * unit), (13 * unit, far_rows - 13 * unit),
        (snps - far_rows, ahead + far_rows - snps), (ahead, behind),
    ]

    def piece(p, odd):
        at, size = pieces[p]
        return pl.multiple_of((1 - odd) * at + odd * (snps - at - size), unit), size

    def halo_copy(src_slot, dst_slot, p, odd, peer, send):
        at, size = piece(p, odd)
        rows = pl.ds(at, size)
        return pltpu.make_async_remote_copy(
            src_ref=ext.at[src_slot, rows, :], dst_ref=ext.at[dst_slot, rows, :],
            send_sem=halo_send.at[send], recv_sem=halo_recv.at[dst_slot, p],
            device_id=genome(peer), device_id_type=MESH,
        )

    def near_copy(p):
        return halo_copy(reach, reach - even, p, parity, near, p)

    def back_copy(p):
        return halo_copy(reach, reach + 2 * even, p, parity, back, 4 + p - 2)

    def far_copy(p):
        return halo_copy(reach, reach - 2 * even, p, parity, far, 8 + p - 6)

    def relay_far(p):
        return halo_copy(reach + even, reach - even, p, 1 - parity, far, 10 + p)

    def relay_near(p):
        return halo_copy(reach + 2 * even, reach + even, p, parity, near, 12 + p - 2)

    def arrived(slot, p, odd):
        halo_copy(reach, slot, p, odd, near, 0).wait_recv()

    has_far, has_back = in_range(far), in_range(back)

    pl.semaphore_wait(barrier, expected)

    def send_halo(nears, backs, fars):
        for k in range(4):
            for p in nears[k:k + 1]:
                near_copy(p).start()
            for p in backs[k:k + 1]:
                @pl.when(has_back)
                def _(p=p):
                    back_copy(p).start()
            for p in fars[k:k + 1]:
                @pl.when(has_far)
                def _(p=p):
                    far_copy(p).start()

    other_core = {"anc": a + 1 - 2 * core}
    other_side = {"anc": lax.rem(a + 2, ancs)}
    up_copy = pltpu.make_async_remote_copy(
        src_ref=pair_out, dst_ref=pair_low, send_sem=pair_send.at[0], recv_sem=pair_recv.at[0],
        device_id=other_core, device_id_type=MESH,
    )
    over_copy = pltpu.make_async_remote_copy(
        src_ref=pair_out, dst_ref=pair_in, send_sem=pair_send.at[1], recv_sem=pair_recv.at[1],
        device_id=other_side, device_id_type=MESH,
    )
    down_copy = pltpu.make_async_remote_copy(
        src_ref=mean, dst_ref=mean, send_sem=pair_send.at[2], recv_sem=pair_recv.at[2],
        device_id=other_core, device_id_type=MESH,
    )

    @pl.when(core == 0)
    def _():
        send_halo((0, 2, 1, 3), (2, 3, 4, 5), (6, 7))

        @pl.when(side == 0)
        def _():
            pl.semaphore_signal(ready, inc=1, device_id={"anc": a + 2}, device_id_type=MESH)

    @pl.when(core == 1)
    def _():
        send_halo((0,), (2,), (6,))

        def round_tile(u, carry):
            cols = pl.ds(pl.multiple_of(u * tile, tile), tile)
            pair_out[:, cols] = coef[:, cols].astype(BF16)
            return carry

        lax.fori_loop(0, tiles, round_tile, 0, unroll=2)
        up_copy.start()

    def clear(first, last):
        def part(i, carry):
            at = pl.multiple_of(first + i * unit, unit)
            field[pl.ds(at, unit), :] = jnp.zeros((unit, traits_here), F32)
            return carry

        lax.fori_loop(0, (last - first) // unit, part, 0, unroll=4)

    clear(0, own_at)
    clear(own_at + snps, field.shape[0])

    for i, (d, m) in enumerate(stat_peers):
        @pl.when(jnp.logical_not(in_range(g - d)))
        def _(i=i):
            stats_in[i] = jnp.zeros(stats_in.shape[1:], F32)

    @pl.when(core == 0)
    def _():
        up_copy.wait_recv()

        def add(u, carry):
            cols = pl.ds(pl.multiple_of(u * tile, tile), tile)
            value = coef[:, cols] + pair_low[:, cols].astype(F32)
            mean[:, cols] = value
            pair_out[:, cols] = value.astype(BF16)
            return carry

        lax.fori_loop(0, tiles, add, 0, unroll=2)

        @pl.when(side == 1)
        def _():
            pl.semaphore_wait(ready, 1)

        over_copy.start()

    def pass_on(p):
        if p < 2:
            arrived(reach + even, p, 1 - parity)

            @pl.when(has_far)
            def _():
                relay_far(p).start()
        else:
            @pl.when(has_far)
            def _():
                arrived(reach + 2 * even, p, parity)
                relay_near(p).start()

    def widen(slot, p, same, i):
        at, size = piece(p, parity if same else 1 - parity)
        in_a = p in (0, 2, 4, 6)
        base = at_a[i] - first_a[1 - same] if in_a else at_b[i] - first_b[1 - same]

        def part(k, carry):
            r = pl.multiple_of(at + k * unit, unit)
            field[pl.ds(pl.multiple_of(base + r, unit), unit), :] = ext[slot, pl.ds(r, unit), :].astype(F32)
            return carry

        lax.fori_loop(0, size // unit, part, 0)

    def range_product(link, u, length, first, second=None):
        deep = length + 128
        within = pl.ds(pl.multiple_of(lax.rem(u, half) * tile, tile), tile)
        rows = pl.ds(pl.multiple_of(u * tile, tile), tile)
        begin = starts_ref[0, u] - g * snps + reach * snps
        where, at = first
        if second is not None:
            here = jnp.clip(begin + width - where, 0, 1) * jnp.clip(where + length - begin, 0, 1)
            where = second[0] + here * (where - second[0])
            at = second[1] + here * (at - second[1])
        skip = lax.div(jnp.clip(where - begin, 0, width - deep), 128) * 128
        from_row = at + jnp.clip(begin + skip - where, -deep, length)
        total = jnp.zeros((tile, traits_here), F32)
        for c in range(0, deep, 512):
            step = min(512, deep - c)
            window = field[pl.ds(from_row + c, step), :].astype(BF16)
            total = total + jnp.dot(
                link[within, pl.ds(skip + c, step)], window, preferred_element_type=F32
            )
        return rows, total

    def each_tile(body, parts=(0, 1), unroll=2):
        for i in parts:
            lax.fori_loop(i * half, (i + 1) * half, functools.partial(body, links[i]), 0, unroll=unroll)

    def own_tile(link, u, carry):
        rows, total = range_product(link, u, snps, (reach * snps, own_at))
        band[rows, :] = total
        return carry

    def own_pass(i):
        for u in range(i * half, (i + 1) * half):
            link_copy(u).wait()
        each_tile(own_tile, (i,))

    load_small[0].wait()
    own_pass(0)

    @pl.when(core == 0)
    def _():
        pass_on(0)
        pass_on(2)

    own_pass(1)

    @pl.when(core == 0)
    def _():
        pl.semaphore_signal(ready, inc=1, device_id=other_core, device_id_type=MESH)

    @pl.when(core == 1)
    def _():
        pl.semaphore_wait(ready, 1)
        send_halo((2,), (), ())
        pl.semaphore_wait(ready, 1)
        send_halo((1, 3), (3, 4, 5), (7,))
        pass_on(0)
        pass_on(2)

    def pair_product(link, u, slots_here, i, in_a):
        length, firsts, bases = (ahead, first_a, at_a) if in_a else (behind, first_b, at_b)
        return range_product(
            link, u, length,
            (slots_here[0] * snps + firsts[1], bases[i]), (slots_here[1] * snps + firsts[0], bases[i + 1]),
        )

    beside = (reach + even, reach - 2 * even)
    beyond = (reach - even, reach + 2 * even)

    def add_tile(link, u, carry, slots_here, i, in_a):
        rows, total = pair_product(link, u, slots_here, i, in_a)
        band[rows, :] = band[rows, :] + total
        return carry

    def beside_pass(in_a):
        for p in (0, 2) if in_a else (1, 3):
            widen(beside[0], p, 0, 0)

        @pl.when(has_back)
        def _():
            p = 6 if in_a else 7
            arrived(beside[1], p, parity)
            widen(beside[1], p, 1, 1)

        each_tile(functools.partial(add_tile, slots_here=beside, i=0, in_a=in_a), unroll=4)

    def beyond_ready(in_a):
        @pl.when(has_far)
        def _():
            arrived(beyond[1], 4 if in_a else 5, parity)
            for p in (2, 4) if in_a else (3, 5):
                widen(beyond[1], p, 1, 3)

        @pl.when(has_back)
        def _():
            for p in (0, 2) if in_a else (1, 3):
                arrived(beyond[0], p, 1 - parity)
                widen(beyond[0], p, 0, 2)

    arrived(beside[0], 2, 1 - parity)
    beside_pass(True)
    pass_on(1)
    pass_on(3)

    @pl.when(core == 0)
    def _():
        pl.semaphore_signal(ready, inc=1, device_id=other_core, device_id_type=MESH)

    arrived(beside[0], 3, 1 - parity)
    beside_pass(False)

    @pl.when(core == 0)
    def _():
        over_copy.wait_recv()

        def add(u, carry):
            cols = pl.ds(pl.multiple_of(u * tile, tile), tile)
            mean[:, cols] = (mean[:, cols] + pair_in[:, cols].astype(F32)) / ancs
            return carry

        lax.fori_loop(0, tiles, add, 0, unroll=2)
        down_copy.start()

    @pl.when(core == 1)
    def _():
        down_copy.wait_recv()

    load_sums.wait()
    for load in load_small[1:]:
        load.wait()

    def prepare(u, carry):
        cols = pl.ds(pl.multiple_of(u * tile, tile), tile)
        proposal[:, cols] = (
            (1.0 - step_size - step_size * merging) * coef[:, cols]
            + step_size * sums[:, cols] + (step_size * merging) * mean[:, cols]
        )
        return carry

    lax.fori_loop(0, tiles, prepare, 0, unroll=2)

    lanes = stats_out.shape[1]
    mine = lax.broadcasted_iota(jnp.int32, (groups, snps), 0) == ids_ref[...]
    counts = jnp.sum(jnp.where(mine, 1.0, 0.0), axis=1, keepdims=True)
    on_lane = lax.broadcasted_iota(jnp.int32, (groups, lanes), 0) == lax.broadcasted_iota(
        jnp.int32, (groups, lanes), 1
    )
    stats_out[1:2, :] = jnp.sum(jnp.where(on_lane, counts, 0.0), axis=0, keepdims=True)

    beyond_ready(True)
    each_tile(functools.partial(add_tile, slots_here=beyond, i=2, in_a=True), unroll=4)

    beyond_ready(False)

    def last_tile(link, u, carry):
        rows, total = pair_product(link, u, beyond, 2, False)
        value = proposal[:, rows] - step_size * (band[rows, :] + total).T
        proposal[:, rows] = value
        row[:, rows] = jnp.sum(value * value, axis=0, keepdims=True)
        return carry

    each_tile(last_tile, unroll=4)

    squares = jnp.sum(jnp.where(mine, row[...], 0.0), axis=1, keepdims=True)
    stats_out[0:1, :] = jnp.sum(jnp.where(on_lane, squares, 0.0), axis=0, keepdims=True)

    def stats_copy(i):
        d, m = stat_peers[i]
        return pltpu.make_async_remote_copy(
            src_ref=stats_out, dst_ref=stats_in.at[i],
            send_sem=stats_send.at[i], recv_sem=stats_recv.at[i],
            device_id={**genome(g + d), "trait": lax.rem(t + m, traits_n)}, device_id_type=MESH,
        )

    for i, (d, m) in enumerate(stat_peers):
        @pl.when(in_range(g + d))
        def _(i=i):
            stats_copy(i).start()

    load_dosage.wait()
    for i, (d, m) in enumerate(stat_peers):
        @pl.when(in_range(g - d))
        def _(i=i):
            stats_copy(i).wait_recv()

    stats = stats_out[...]
    for i in range(len(stat_peers)):
        stats = stats + stats_in[i]
    all_squares = stats[0:1, :groups]
    all_counts = stats[1:2, :groups] / traits_n
    threshold = step_size * weight_ref[...] * jnp.sqrt(all_counts * (traits_here * traits_n))
    shrink = jnp.maximum(0.0, 1.0 - threshold / jnp.sqrt(all_squares + epsilon))
    same = lax.broadcasted_iota(jnp.int32, (groups, groups), 0) == lax.broadcasted_iota(
        jnp.int32, (groups, groups), 1
    )
    shrink = jnp.sum(jnp.where(same, shrink, 0.0), axis=1, keepdims=True)
    row[...] = jnp.sum(jnp.where(mine, shrink, 0.0), axis=0, keepdims=True)

    def round_updated(u, carry):
        cols = pl.ds(pl.multiple_of(u * tile, tile), tile)
        low[:, cols] = (proposal[:, cols] * row[:, cols]).astype(BF16)
        return carry

    def keep_updated(u, carry):
        cols = pl.ds(pl.multiple_of(u * tile, tile), tile)
        updated_ref[0, :, cols] = proposal[:, cols] * row[:, cols]
        return carry

    lax.fori_loop(0, tiles, round_updated, 0, unroll=4)

    scale = 1.0 / math.sqrt(snps * genomes)
    own_side, other_side_g = parity, lax.rem(near, 2)

    def pair_at(i):
        here = g // 2
        is_last = jnp.clip(i - (pairs - 2), 0, 1)
        return (1 - is_last) * (i + jnp.clip(i - here + 1, 0, 1)) + is_last * here

    cuts = side_out.shape[1]
    sub = traits_here // cuts
    last_pair = pairs - 1

    def partial(person):
        at = pl.ds(pl.multiple_of(person * persons_per, persons_per), persons_per)
        return lax.dot_general(
            low[...], dosage[at, :], (((1,), (1,)), ((), ())), preferred_element_type=F32
        ) * scale

    def side_copy(i, c):
        return pltpu.make_async_remote_copy(
            src_ref=side_out.at[i, c], dst_ref=side_in.at[i, c],
            send_sem=side_send.at[i, c], recv_sem=side_recv.at[i, c],
            device_id={"genome": near}, device_id_type=MESH,
        )

    def part_copy(i, c):
        to = pair_at(i)
        slot = lax.rem(g // 2 - to + pairs, pairs) - 1
        return pltpu.make_async_remote_copy(
            src_ref=part_out.at[i, c], dst_ref=part_in.at[slot, c],
            send_sem=part_send.at[i, c], recv_sem=part_recv.at[slot, c],
            device_id={"genome": 2 * to + own_side}, device_id_type=MESH,
        )

    def part_arrived(i, c):
        return pltpu.make_async_remote_copy(
            src_ref=part_out.at[i, c], dst_ref=part_in.at[i, c],
            send_sem=part_send.at[i, c], recv_sem=part_recv.at[i, c],
            device_id={"genome": near}, device_id_type=MESH,
        )

    def send_side(i, carry):
        value = partial(2 * pair_at(i) + other_side_g).astype(BF16)
        for c in range(cuts):
            side_out[i, c] = value[c * sub:(c + 1) * sub]
            side_copy(i, c).start()
        return carry

    def send_part(i, carry):
        mine_here = partial(2 * pair_at(i) + own_side)
        for c in range(cuts):
            side_copy(i, c).wait_recv()
            part_out[i, c] = (mine_here[c * sub:(c + 1) * sub] + side_in[i, c].astype(F32)).astype(BF16)
            part_copy(i, c).start()
        return carry

    lax.fori_loop(0, pairs, send_side, 0)
    lax.fori_loop(0, last_pair, send_part, 0)
    lax.fori_loop(0, tiles, keep_updated, 0, unroll=2)

    last = partial(2 * pair_at(last_pair) + own_side)
    for c in range(cuts):
        side_copy(last_pair, c).wait_recv()

        def add_part(k, total, c=c):
            part_arrived(k, c).wait_recv()
            return total + part_in[k, c].astype(F32)

        own_total = last[c * sub:(c + 1) * sub] + side_in[last_pair, c].astype(F32)
        score_ref[0, c * sub:(c + 1) * sub, :] = lax.fori_loop(0, pairs - 1, add_part, own_total)

    for p in range(4):
        near_copy(p).wait_send()

    @pl.when(has_back)
    def _():
        for p in (2, 3, 4, 5):
            back_copy(p).wait_send()

    @pl.when(has_far)
    def _():
        for p in (6, 7):
            far_copy(p).wait_send()
        for p in (0, 1):
            relay_far(p).wait_send()
        for p in (2, 3):
            relay_near(p).wait_send()

    @pl.when(core == 1)
    def _():
        up_copy.wait_send()

    @pl.when(core == 0)
    def _():
        over_copy.wait_send()
        down_copy.wait_send()

    for i, (d, m) in enumerate(stat_peers):
        @pl.when(in_range(g + d))
        def _(i=i):
            stats_copy(i).wait_send()

    def sent_side(i, carry):
        for c in range(cuts):
            side_copy(i, c).wait_send()
        return carry

    def sent_part(i, carry):
        for c in range(cuts):
            part_copy(i, c).wait_send()
        return carry

    lax.fori_loop(0, pairs, sent_side, 0)
    lax.fori_loop(0, pairs - 1, sent_part, 0)


def store_kernel(updated_in, score_in, updated_out, score_out, sem):
    parts = sem.shape[0] - 1
    rows = updated_in.shape[1] // parts
    copies = [pltpu.make_async_copy(score_in, score_out, sem.at[parts])]
    for i in range(parts):
        part = pl.ds(i * rows, rows)
        copies.append(pltpu.make_async_copy(updated_in.at[:, part], updated_out.at[:, part], sem.at[i]))
    for copy in copies:
        copy.start()
    for copy in copies:
        copy.wait()


def per_device(coefficients, sumstats, linkage, band_start, group_ids, group_weight, dosage):
    _, traits_here, snps = coefficients.shape
    width = linkage.shape[2]
    genomes = lax.axis_size("genome")
    ancs = lax.axis_size("anc")
    traits_n = lax.axis_size("trait")
    persons = dosage.shape[1]
    persons_per = persons // genomes
    groups = group_weight.shape[1]
    reach = -(-width // snps)
    assert reach == 2 and genomes % 2 == 0 and coefficients.shape[0] == 1 and ancs == 4
    tile = snps // band_start.shape[1]
    slots = 2 * reach + 1
    pairs = genomes // 2
    field_rows = 11 * snps + 10 * 128
    group_reach = min(-(-longest_run // snps), genomes - 1)
    cuts = 2
    stat_n = (2 * group_reach + 1) * traits_n - 1
    lanes = -(-groups // 128) * 128
    sizes = (genomes, ancs, traits_n, reach, tile, groups)
    hbm = pl.BlockSpec(memory_space=pltpu.HBM)
    vmem = pl.BlockSpec(memory_space=pltpu.VMEM)
    dma = pltpu.SemaphoreType.DMA
    args = (coefficients, sumstats, linkage, band_start, group_ids, group_weight, dosage)
    args = tuple(pltpu.with_memory_space_constraint(x, pltpu.HBM) for x in args)
    out_shape = (
        jax.ShapeDtypeStruct((1, traits_here, snps), F32),
        jax.ShapeDtypeStruct((1, traits_here, persons_per), F32),
    )
    updated, scores = pl.pallas_call(
        functools.partial(step_kernel, sizes),
        out_shape=out_shape,
        in_specs=[hbm] * 7,
        out_specs=(vmem, vmem),
        scratch_shapes=[
            pltpu.VMEM((traits_here, snps), F32),
            pltpu.VMEM((traits_here, snps), F32),
            pltpu.VMEM((snps // 2, width), BF16),
            pltpu.VMEM((snps // 2, width), BF16),
            pltpu.SMEM(band_start.shape, jnp.int32),
            pltpu.VMEM(group_ids.shape, jnp.int32),
            pltpu.VMEM(group_weight.shape, F32),
            pltpu.VMEM((persons, snps), BF16),
            pltpu.VMEM((slots, snps, traits_here), BF16),
            pltpu.VMEM((field_rows, traits_here), F32),
            pltpu.VMEM((snps, traits_here), F32),
            pltpu.VMEM((traits_here, snps), F32),
            pltpu.VMEM((traits_here, snps), BF16),
            pltpu.VMEM((traits_here, snps), BF16),
            pltpu.VMEM((traits_here, snps), BF16),
            pltpu.VMEM((traits_here, snps), F32),
            pltpu.VMEM((traits_here, snps), BF16),
            pltpu.VMEM((1, snps), F32),
            pltpu.VMEM((2, lanes), F32),
            pltpu.VMEM((stat_n, 2, lanes), F32),
            pltpu.VMEM((pairs, cuts, traits_here // cuts, persons_per), BF16),
            pltpu.VMEM((pairs, cuts, traits_here // cuts, persons_per), BF16),
            pltpu.VMEM((pairs - 1, cuts, traits_here // cuts, persons_per), BF16),
            pltpu.VMEM((pairs - 1, cuts, traits_here // cuts, persons_per), BF16),
            dma((4,)), dma((5,)), dma((snps // tile,)), pltpu.SemaphoreType.REGULAR,
            dma((14,)), dma((slots, 8)), dma((3,)), dma((3,)),
            dma((stat_n,)), dma((stat_n,)), dma((pairs, cuts)), dma((pairs, cuts)), dma((pairs - 1, cuts)), dma((pairs - 1, cuts)),
        ],
        compiler_params=pltpu.CompilerParams(
            collective_id=0, has_side_effects=True, vmem_limit_bytes=52 * 1024 * 1024
        ),
    )(*args)
    return pl.pallas_call(
        store_kernel,
        out_shape=out_shape,
        in_specs=[vmem, vmem],
        out_specs=(hbm, hbm),
        scratch_shapes=[dma((5,))],
    )(*(pltpu.with_memory_space_constraint(x, pltpu.VMEM) for x in (updated, scores)))


def solution(mesh):
    in_specs = (
        P("anc", "trait", "genome"),
        P("anc", "trait", "genome"),
        P("anc", "genome", None),
        P("anc", "genome"),
        P("anc", "genome"),
        P("anc", None),
        P("anc", None, "genome"),
    )
    out_specs = (P("anc", "trait", "genome"), P("anc", "trait", "genome"))
    return jax.shard_map(
        per_device, mesh=mesh, in_specs=in_specs, out_specs=out_specs, check_vma=False
    )
```

```python
import functools
import math

import jax
import jax.numpy as jnp
from jax import lax
from jax.experimental import pallas as pl
from jax.experimental.pallas import tpu as pltpu
from jax.sharding import PartitionSpec as P

step_size = 0.5
merging = 0.5
epsilon = 1e-06
longest_run = 8192

MESH = pl.DeviceIdType.MESH
F32 = jnp.float32
BF16 = jnp.bfloat16


def step_kernel(
    sizes,
    coef_hbm, sums_hbm, link_hbm, starts_hbm, ids_hbm, weight_hbm, dosage_hbm,
    updated_ref, score_ref,
    coef, sums, link_first, link_second, starts_ref, ids_ref, weight_ref, dosage, ext, field, band, mean, pair_out, pair_low, pair_in,
    proposal, low, row, stats_out, stats_in, side_out, side_in, part_out, part_in,
    coef_sem, load_sem, link_sem, ready,
    halo_send, halo_recv, pair_send, pair_recv, stats_send, stats_recv, side_send, side_recv, part_send, part_recv,
):
    genomes, ancs, traits_n, reach, tile, groups = sizes
    traits_here, snps = coef.shape
    links = (link_first, link_second)
    width = link_first.shape[1]
    tiles = snps // tile
    half = tiles // 2
    persons_per = dosage.shape[0] // genomes
    pairs = genomes // 2
    g = lax.axis_index("genome")
    a = lax.axis_index("anc")
    t = lax.axis_index("trait")
    core, side = lax.rem(a, 2), a // 2
    parity = lax.rem(g, 2)
    even = 1 - 2 * parity
    near, far, back, across = g + even, g + 2 * even, g - 2 * even, g - even

    def in_range(p):
        return jnp.logical_and(p >= 0, p < genomes)

    def genome(p):
        return {"genome": jnp.clip(p, 0, genomes - 1)}

    group_reach = min(-(-longest_run // snps), genomes - 1)
    stat_peers = [
        (d, m) for m in range(traits_n) for d in range(-group_reach, group_reach + 1) if (d, m) != (0, 0)
    ]
    if genomes > 8 or traits_n > 1:
        greet = [(k, m) for m in range(traits_n) for k in range(genomes) if (k, m) != (0, 0)]
    else:
        greet = []

    coef_parts = coef_sem.shape[0]
    part_cols = snps // coef_parts

    def coef_copy(i):
        cols = pl.ds(i * part_cols, part_cols)
        return pltpu.make_async_copy(coef_hbm.at[0, :, cols], coef.at[:, cols], coef_sem.at[i])

    for i in range(coef_parts):
        coef_copy(i).start()
    barrier = pltpu.get_barrier_semaphore()
    if greet:
        for k, m in greet:
            pl.semaphore_signal(
                barrier, inc=1, device_id_type=MESH,
                device_id={"genome": lax.rem(g + k, genomes), "trait": lax.rem(t + m, traits_n)},
            )
        expected = len(greet)
    else:
        pl.semaphore_signal(barrier, inc=1, device_id=genome(near), device_id_type=MESH)
        for peer in (far, back):
            @pl.when(in_range(peer))
            def _(peer=peer):
                pl.semaphore_signal(barrier, inc=1, device_id=genome(peer), device_id_type=MESH)
        expected = 1 + in_range(far).astype(jnp.int32) + in_range(back).astype(jnp.int32)

    @pl.when(core == 0)
    def _():
        pl.semaphore_signal(barrier, inc=1, device_id={"anc": a + 1}, device_id_type=MESH)

    @pl.when(jnp.logical_and(core == 0, side == 1))
    def _():
        pl.semaphore_signal(barrier, inc=1, device_id={"anc": a - 2}, device_id_type=MESH)

    expected = expected + core + (1 - core) * (1 - side)

    load_small = [
        pltpu.make_async_copy(starts_hbm, starts_ref, load_sem.at[0]),
        pltpu.make_async_copy(ids_hbm, ids_ref, load_sem.at[1]),
        pltpu.make_async_copy(weight_hbm, weight_ref, load_sem.at[2]),
    ]
    load_sums = pltpu.make_async_copy(sums_hbm.at[0], sums, load_sem.at[3])
    load_dosage = pltpu.make_async_copy(dosage_hbm.at[0], dosage, load_sem.at[4])

    def link_copy(u):
        return pltpu.make_async_copy(
            link_hbm.at[0, pl.ds(u * tile, tile), :], links[u // half].at[pl.ds(u % half * tile, tile), :],
            link_sem.at[u],
        )

    unit = snps // 16
    far_rows = width - tile - snps
    ahead = 11 * unit
    behind = snps - ahead
    ahead = 11 * unit
    behind = snps - ahead
    own_at = snps + 128
    at_a = [own_at + 2 * snps + 128 + i * (2 * ahead + 128) for i in range(4)]
    at_b = [at_a[3] + 2 * ahead + 128 + i * (2 * behind + 128) for i in range(4)]
    assert at_b[3] + 2 * behind + 128 == field.shape[0] and 13 * unit < far_rows <= 16 * unit
    first_a = (parity * behind, (1 - parity) * behind)
    first_b = ((1 - parity) * ahead, parity * ahead)

    def own_block(u, carry):
        cols = pl.ds(pl.multiple_of(u * tile, tile), tile)
        flat = coef[:, cols].T.astype(BF16)
        ext[reach, cols, :] = flat
        field[pl.ds(pl.multiple_of(own_at + u * tile, unit), tile), :] = flat.astype(F32)
        return carry

    for i in range(coef_parts):
        coef_copy(i).wait()
        if i == coef_parts - 1:
            for load in load_small:
                load.start()
            for u in range(tiles):
                link_copy(u).start()
            load_sums.start()
            load_dosage.start()
        lax.fori_loop(i * tiles // coef_parts, (i + 1) * tiles // coef_parts, own_block, 0, unroll=2)

    pieces = [
        (5 * unit, 6 * unit), (13 * unit, 3 * unit), (0, 5 * unit), (11 * unit, 2 * unit),
        (5 * unit, 6 * unit), (13 * unit, far_rows - 13 * unit),
        (snps - far_rows, ahead + far_rows - snps), (ahead, behind),
    ]

    def piece(p, odd):
        at, size = pieces[p]
        return pl.multiple_of((1 - odd) * at + odd * (snps - at - size), unit), size

    def halo_copy(src_slot, dst_slot, p, odd, peer, send):
        at, size = piece(p, odd)
        rows = pl.ds(at, size)
        return pltpu.make_async_remote_copy(
            src_ref=ext.at[src_slot, rows, :], dst_ref=ext.at[dst_slot, rows, :],
            send_sem=halo_send.at[send], recv_sem=halo_recv.at[dst_slot, p],
            device_id=genome(peer), device_id_type=MESH,
        )

    def near_copy(p):
        return halo_copy(reach, reach - even, p, parity, near, p)

    def back_copy(p):
        return halo_copy(reach, reach + 2 * even, p, parity, back, 4 + p - 2)

    def far_copy(p):
        return halo_copy(reach, reach - 2 * even, p, parity, far, 8 + p - 6)

    def relay_far(p):
        return halo_copy(reach + even, reach - even, p, 1 - parity, far, 10 + p)

    def relay_near(p):
        return halo_copy(reach + 2 * even, reach + even, p, parity, near, 12 + p - 2)

    def arrived(slot, p, odd):
        halo_copy(reach, slot, p, odd, near, 0).wait_recv()

    has_far, has_back = in_range(far), in_range(back)

    pl.semaphore_wait(barrier, expected)

    def send_halo(nears, backs, fars):
        for k in range(4):
            for p in nears[k:k + 1]:
                near_copy(p).start()
            for p in backs[k:k + 1]:
                @pl.when(has_back)
                def _(p=p):
                    back_copy(p).start()
            for p in fars[k:k + 1]:
                @pl.when(has_far)
                def _(p=p):
                    far_copy(p).start()

    other_core = {"anc": a + 1 - 2 * core}
    other_side = {"anc": lax.rem(a + 2, ancs)}
    up_copy = pltpu.make_async_remote_copy(
        src_ref=pair_out, dst_ref=pair_low, send_sem=pair_send.at[0], recv_sem=pair_recv.at[0],
        device_id=other_core, device_id_type=MESH,
    )
    over_copy = pltpu.make_async_remote_copy(
        src_ref=pair_out, dst_ref=pair_in, send_sem=pair_send.at[1], recv_sem=pair_recv.at[1],
        device_id=other_side, device_id_type=MESH,
    )
    down_copy = pltpu.make_async_remote_copy(
        src_ref=mean, dst_ref=mean, send_sem=pair_send.at[2], recv_sem=pair_recv.at[2],
        device_id=other_core, device_id_type=MESH,
    )

    @pl.when(core == 0)
    def _():
        send_halo((0, 2, 1, 3), (2, 3, 4, 5), (6, 7))

        @pl.when(side == 0)
        def _():
            pl.semaphore_signal(ready, inc=1, device_id={"anc": a + 2}, device_id_type=MESH)

    @pl.when(core == 1)
    def _():
        send_halo((0,), (2,), (6,))

        def round_tile(u, carry):
            cols = pl.ds(pl.multiple_of(u * tile, tile), tile)
            pair_out[:, cols] = coef[:, cols].astype(BF16)
            return carry

        lax.fori_loop(0, tiles, round_tile, 0, unroll=2)
        up_copy.start()

    def clear(first, last):
        def part(i, carry):
            at = pl.multiple_of(first + i * unit, unit)
            field[pl.ds(at, unit), :] = jnp.zeros((unit, traits_here), F32)
            return carry

        lax.fori_loop(0, (last - first) // unit, part, 0, unroll=4)

    clear(0, own_at)
    clear(own_at + snps, field.shape[0])

    for i, (d, m) in enumerate(stat_peers):
        @pl.when(jnp.logical_not(in_range(g - d)))
        def _(i=i):
            stats_in[i] = jnp.zeros(stats_in.shape[1:], F32)

    @pl.when(core == 0)
    def _():
        up_copy.wait_recv()

        def add(u, carry):
            cols = pl.ds(pl.multiple_of(u * tile, tile), tile)
            value = coef[:, cols] + pair_low[:, cols].astype(F32)
            mean[:, cols] = value
            pair_out[:, cols] = value.astype(BF16)
            return carry

        lax.fori_loop(0, tiles, add, 0, unroll=2)

        @pl.when(side == 1)
        def _():
            pl.semaphore_wait(ready, 1)

        over_copy.start()

    def pass_on(p):
        if p < 2:
            arrived(reach + even, p, 1 - parity)

            @pl.when(has_far)
            def _():
                relay_far(p).start()
        else:
            @pl.when(has_far)
            def _():
                arrived(reach + 2 * even, p, parity)
                relay_near(p).start()

    def widen(slot, p, same, i):
        at, size = piece(p, parity if same else 1 - parity)
        in_a = p in (0, 2, 4, 6)
        base = at_a[i] - first_a[1 - same] if in_a else at_b[i] - first_b[1 - same]

        def part(k, carry):
            r = pl.multiple_of(at + k * unit, unit)
            field[pl.ds(pl.multiple_of(base + r, unit), unit), :] = ext[slot, pl.ds(r, unit), :].astype(F32)
            return carry

        lax.fori_loop(0, size // unit, part, 0)

    def range_product(link, u, length, first, second=None):
        deep = length + 128
        within = pl.ds(pl.multiple_of(lax.rem(u, half) * tile, tile), tile)
        rows = pl.ds(pl.multiple_of(u * tile, tile), tile)
        begin = starts_ref[0, u] - g * snps + reach * snps
        where, at = first
        if second is not None:
            here = jnp.clip(begin + width - where, 0, 1) * jnp.clip(where + length - begin, 0, 1)
            where = second[0] + here * (where - second[0])
            at = second[1] + here * (at - second[1])
        skip = lax.div(jnp.clip(where - begin, 0, width - deep), 128) * 128
        from_row = at + jnp.clip(begin + skip - where, -deep, length)
        total = jnp.zeros((tile, traits_here), F32)
        for c in range(0, deep, 512):
            step = min(512, deep - c)
            window = field[pl.ds(from_row + c, step), :].astype(BF16)
            total = total + jnp.dot(
                link[within, pl.ds(skip + c, step)], window, preferred_element_type=F32
            )
        return rows, total

    def each_tile(body, parts=(0, 1), unroll=2):
        for i in parts:
            lax.fori_loop(i * half, (i + 1) * half, functools.partial(body, links[i]), 0, unroll=unroll)

    def own_tile(link, u, carry):
        rows, total = range_product(link, u, snps, (reach * snps, own_at))
        band[rows, :] = total
        return carry

    def own_pass(i):
        for u in range(i * half, (i + 1) * half):
            link_copy(u).wait()
        each_tile(own_tile, (i,), unroll=4)

    load_small[0].wait()
    own_pass(0)

    @pl.when(core == 0)
    def _():
        pass_on(0)
        pass_on(2)

    own_pass(1)

    @pl.when(core == 0)
    def _():
        pl.semaphore_signal(ready, inc=1, device_id=other_core, device_id_type=MESH)

    @pl.when(core == 1)
    def _():
        pl.semaphore_wait(ready, 1)
        send_halo((2,), (), ())
        pl.semaphore_wait(ready, 1)
        send_halo((1, 3), (3, 4, 5), (7,))
        pass_on(0)
        pass_on(2)

    def pair_product(link, u, slots_here, i, in_a):
        length, firsts, bases = (ahead, first_a, at_a) if in_a else (behind, first_b, at_b)
        return range_product(
            link, u, length,
            (slots_here[0] * snps + firsts[1], bases[i]), (slots_here[1] * snps + firsts[0], bases[i + 1]),
        )

    beside = (reach + even, reach - 2 * even)
    beyond = (reach - even, reach + 2 * even)

    def add_tile(link, u, carry, slots_here, i, in_a):
        rows, total = pair_product(link, u, slots_here, i, in_a)
        band[rows, :] = band[rows, :] + total
        return carry

    def beside_pass(in_a):
        for p in (0, 2) if in_a else (1, 3):
            widen(beside[0], p, 0, 0)

        @pl.when(has_back)
        def _():
            p = 6 if in_a else 7
            arrived(beside[1], p, parity)
            widen(beside[1], p, 1, 1)

        each_tile(functools.partial(add_tile, slots_here=beside, i=0, in_a=in_a), unroll=4)

    def beyond_ready(in_a):
        @pl.when(has_far)
        def _():
            arrived(beyond[1], 4 if in_a else 5, parity)
            for p in (2, 4) if in_a else (3, 5):
                widen(beyond[1], p, 1, 3)

        @pl.when(has_back)
        def _():
            for p in (0, 2) if in_a else (1, 3):
                arrived(beyond[0], p, 1 - parity)
                widen(beyond[0], p, 0, 2)

    arrived(beside[0], 2, 1 - parity)
    beside_pass(True)
    pass_on(1)
    pass_on(3)

    @pl.when(core == 0)
    def _():
        pl.semaphore_signal(ready, inc=1, device_id=other_core, device_id_type=MESH)

    arrived(beside[0], 3, 1 - parity)
    beside_pass(False)

    @pl.when(core == 0)
    def _():
        over_copy.wait_recv()

        def add(u, carry):
            cols = pl.ds(pl.multiple_of(u * tile, tile), tile)
            mean[:, cols] = (mean[:, cols] + pair_in[:, cols].astype(F32)) / ancs
            return carry

        lax.fori_loop(0, tiles, add, 0, unroll=2)
        down_copy.start()

    @pl.when(core == 1)
    def _():
        down_copy.wait_recv()

    load_sums.wait()
    for load in load_small[1:]:
        load.wait()

    def prepare(u, carry):
        cols = pl.ds(pl.multiple_of(u * tile, tile), tile)
        proposal[:, cols] = (
            (1.0 - step_size - step_size * merging) * coef[:, cols]
            + step_size * sums[:, cols] + (step_size * merging) * mean[:, cols]
        )
        return carry

    lax.fori_loop(0, tiles, prepare, 0, unroll=2)

    lanes = stats_out.shape[1]
    mine = lax.broadcasted_iota(jnp.int32, (groups, snps), 0) == ids_ref[...]
    counts = jnp.sum(jnp.where(mine, 1.0, 0.0), axis=1, keepdims=True)
    on_lane = lax.broadcasted_iota(jnp.int32, (groups, lanes), 0) == lax.broadcasted_iota(
        jnp.int32, (groups, lanes), 1
    )
    stats_out[1:2, :] = jnp.sum(jnp.where(on_lane, counts, 0.0), axis=0, keepdims=True)

    beyond_ready(True)
    each_tile(functools.partial(add_tile, slots_here=beyond, i=2, in_a=True), unroll=4)

    beyond_ready(False)

    def last_tile(link, u, carry):
        rows, total = pair_product(link, u, beyond, 2, False)
        value = proposal[:, rows] - step_size * (band[rows, :] + total).T
        proposal[:, rows] = value
        row[:, rows] = jnp.sum(value * value, axis=0, keepdims=True)
        return carry

    each_tile(last_tile, unroll=4)

    squares = jnp.sum(jnp.where(mine, row[...], 0.0), axis=1, keepdims=True)
    stats_out[0:1, :] = jnp.sum(jnp.where(on_lane, squares, 0.0), axis=0, keepdims=True)

    def stats_copy(i):
        d, m = stat_peers[i]
        return pltpu.make_async_remote_copy(
            src_ref=stats_out, dst_ref=stats_in.at[i],
            send_sem=stats_send.at[i], recv_sem=stats_recv.at[i],
            device_id={**genome(g + d), "trait": lax.rem(t + m, traits_n)}, device_id_type=MESH,
        )

    for i, (d, m) in enumerate(stat_peers):
        @pl.when(in_range(g + d))
        def _(i=i):
            stats_copy(i).start()

    load_dosage.wait()
    for i, (d, m) in enumerate(stat_peers):
        @pl.when(in_range(g - d))
        def _(i=i):
            stats_copy(i).wait_recv()

    stats = stats_out[...]
    for i in range(len(stat_peers)):
        stats = stats + stats_in[i]
    all_squares = stats[0:1, :groups]
    all_counts = stats[1:2, :groups] / traits_n
    threshold = step_size * weight_ref[...] * jnp.sqrt(all_counts * (traits_here * traits_n))
    shrink = jnp.maximum(0.0, 1.0 - threshold / jnp.sqrt(all_squares + epsilon))
    same = lax.broadcasted_iota(jnp.int32, (groups, groups), 0) == lax.broadcasted_iota(
        jnp.int32, (groups, groups), 1
    )
    shrink = jnp.sum(jnp.where(same, shrink, 0.0), axis=1, keepdims=True)
    row[...] = jnp.sum(jnp.where(mine, shrink, 0.0), axis=0, keepdims=True)

    def round_updated(u, carry):
        cols = pl.ds(pl.multiple_of(u * tile, tile), tile)
        low[:, cols] = (proposal[:, cols] * row[:, cols]).astype(BF16)
        return carry

    def keep_updated(u, carry):
        cols = pl.ds(pl.multiple_of(u * tile, tile), tile)
        updated_ref[0, :, cols] = proposal[:, cols] * row[:, cols]
        return carry

    lax.fori_loop(0, tiles, round_updated, 0, unroll=4)

    scale = 1.0 / math.sqrt(snps * genomes)
    own_side, other_side_g = parity, lax.rem(near, 2)

    def pair_at(i):
        here = g // 2
        is_last = jnp.clip(i - (pairs - 2), 0, 1)
        return (1 - is_last) * (i + jnp.clip(i - here + 1, 0, 1)) + is_last * here

    cuts = side_out.shape[1]
    sub = traits_here // cuts
    last_pair = pairs - 1

    def partial(person):
        at = pl.ds(pl.multiple_of(person * persons_per, persons_per), persons_per)
        return lax.dot_general(
            low[...], dosage[at, :], (((1,), (1,)), ((), ())), preferred_element_type=F32
        ) * scale

    def side_copy(i, c):
        return pltpu.make_async_remote_copy(
            src_ref=side_out.at[i, c], dst_ref=side_in.at[i, c],
            send_sem=side_send.at[i, c], recv_sem=side_recv.at[i, c],
            device_id={"genome": near}, device_id_type=MESH,
        )

    def part_copy(i, c):
        to = pair_at(i)
        slot = lax.rem(g // 2 - to + pairs, pairs) - 1
        return pltpu.make_async_remote_copy(
            src_ref=part_out.at[i, c], dst_ref=part_in.at[slot, c],
            send_sem=part_send.at[i, c], recv_sem=part_recv.at[slot, c],
            device_id={"genome": 2 * to + own_side}, device_id_type=MESH,
        )

    def part_arrived(i, c):
        return pltpu.make_async_remote_copy(
            src_ref=part_out.at[i, c], dst_ref=part_in.at[i, c],
            send_sem=part_send.at[i, c], recv_sem=part_recv.at[i, c],
            device_id={"genome": near}, device_id_type=MESH,
        )

    def send_side(i, carry):
        value = partial(2 * pair_at(i) + other_side_g).astype(BF16)
        for c in range(cuts):
            side_out[i, c] = value[c * sub:(c + 1) * sub]
            side_copy(i, c).start()
        return carry

    def send_part(i, carry):
        mine_here = partial(2 * pair_at(i) + own_side)
        for c in range(cuts):
            side_copy(i, c).wait_recv()
            part_out[i, c] = (mine_here[c * sub:(c + 1) * sub] + side_in[i, c].astype(F32)).astype(BF16)
            part_copy(i, c).start()
        return carry

    lax.fori_loop(0, pairs, send_side, 0)
    lax.fori_loop(0, last_pair, send_part, 0)
    lax.fori_loop(0, tiles, keep_updated, 0, unroll=2)

    last = partial(2 * pair_at(last_pair) + own_side)
    for c in range(cuts):
        side_copy(last_pair, c).wait_recv()

        def add_part(k, total, c=c):
            part_arrived(k, c).wait_recv()
            return total + part_in[k, c].astype(F32)

        own_total = last[c * sub:(c + 1) * sub] + side_in[last_pair, c].astype(F32)
        score_ref[0, c * sub:(c + 1) * sub, :] = lax.fori_loop(0, pairs - 1, add_part, own_total)

    for p in range(4):
        near_copy(p).wait_send()

    @pl.when(has_back)
    def _():
        for p in (2, 3, 4, 5):
            back_copy(p).wait_send()

    @pl.when(has_far)
    def _():
        for p in (6, 7):
            far_copy(p).wait_send()
        for p in (0, 1):
            relay_far(p).wait_send()
        for p in (2, 3):
            relay_near(p).wait_send()

    @pl.when(core == 1)
    def _():
        up_copy.wait_send()

    @pl.when(core == 0)
    def _():
        over_copy.wait_send()
        down_copy.wait_send()

    for i, (d, m) in enumerate(stat_peers):
        @pl.when(in_range(g + d))
        def _(i=i):
            stats_copy(i).wait_send()

    def sent_side(i, carry):
        for c in range(cuts):
            side_copy(i, c).wait_send()
        return carry

    def sent_part(i, carry):
        for c in range(cuts):
            part_copy(i, c).wait_send()
        return carry

    lax.fori_loop(0, pairs, sent_side, 0)
    lax.fori_loop(0, pairs - 1, sent_part, 0)


def store_kernel(updated_in, score_in, updated_out, score_out, sem):
    parts = sem.shape[0] - 1
    rows = updated_in.shape[1] // parts
    copies = [pltpu.make_async_copy(score_in, score_out, sem.at[parts])]
    for i in range(parts):
        part = pl.ds(i * rows, rows)
        copies.append(pltpu.make_async_copy(updated_in.at[:, part], updated_out.at[:, part], sem.at[i]))
    for copy in copies:
        copy.start()
    for copy in copies:
        copy.wait()


def per_device(coefficients, sumstats, linkage, band_start, group_ids, group_weight, dosage):
    _, traits_here, snps = coefficients.shape
    width = linkage.shape[2]
    genomes = lax.axis_size("genome")
    ancs = lax.axis_size("anc")
    traits_n = lax.axis_size("trait")
    persons = dosage.shape[1]
    persons_per = persons // genomes
    groups = group_weight.shape[1]
    reach = -(-width // snps)
    assert reach == 2 and genomes % 2 == 0 and coefficients.shape[0] == 1 and ancs == 4
    tile = snps // band_start.shape[1]
    slots = 2 * reach + 1
    pairs = genomes // 2
    field_rows = 11 * snps + 10 * 128
    group_reach = min(-(-longest_run // snps), genomes - 1)
    cuts = 2
    stat_n = (2 * group_reach + 1) * traits_n - 1
    lanes = -(-groups // 128) * 128
    sizes = (genomes, ancs, traits_n, reach, tile, groups)
    hbm = pl.BlockSpec(memory_space=pltpu.HBM)
    vmem = pl.BlockSpec(memory_space=pltpu.VMEM)
    dma = pltpu.SemaphoreType.DMA
    args = (coefficients, sumstats, linkage, band_start, group_ids, group_weight, dosage)
    args = tuple(pltpu.with_memory_space_constraint(x, pltpu.HBM) for x in args)
    out_shape = (
        jax.ShapeDtypeStruct((1, traits_here, snps), F32),
        jax.ShapeDtypeStruct((1, traits_here, persons_per), F32),
    )
    updated, scores = pl.pallas_call(
        functools.partial(step_kernel, sizes),
        out_shape=out_shape,
        in_specs=[hbm] * 7,
        out_specs=(vmem, vmem),
        scratch_shapes=[
            pltpu.VMEM((traits_here, snps), F32),
            pltpu.VMEM((traits_here, snps), F32),
            pltpu.VMEM((snps // 2, width), BF16),
            pltpu.VMEM((snps // 2, width), BF16),
            pltpu.SMEM(band_start.shape, jnp.int32),
            pltpu.VMEM(group_ids.shape, jnp.int32),
            pltpu.VMEM(group_weight.shape, F32),
            pltpu.VMEM((persons, snps), BF16),
            pltpu.VMEM((slots, snps, traits_here), BF16),
            pltpu.VMEM((field_rows, traits_here), F32),
            pltpu.VMEM((snps, traits_here), F32),
            pltpu.VMEM((traits_here, snps), F32),
            pltpu.VMEM((traits_here, snps), BF16),
            pltpu.VMEM((traits_here, snps), BF16),
            pltpu.VMEM((traits_here, snps), BF16),
            pltpu.VMEM((traits_here, snps), F32),
            pltpu.VMEM((traits_here, snps), BF16),
            pltpu.VMEM((1, snps), F32),
            pltpu.VMEM((2, lanes), F32),
            pltpu.VMEM((stat_n, 2, lanes), F32),
            pltpu.VMEM((pairs, cuts, traits_here // cuts, persons_per), BF16),
            pltpu.VMEM((pairs, cuts, traits_here // cuts, persons_per), BF16),
            pltpu.VMEM((pairs - 1, cuts, traits_here // cuts, persons_per), BF16),
            pltpu.VMEM((pairs - 1, cuts, traits_here // cuts, persons_per), BF16),
            dma((4,)), dma((5,)), dma((snps // tile,)), pltpu.SemaphoreType.REGULAR,
            dma((14,)), dma((slots, 8)), dma((3,)), dma((3,)),
            dma((stat_n,)), dma((stat_n,)), dma((pairs, cuts)), dma((pairs, cuts)), dma((pairs - 1, cuts)), dma((pairs - 1, cuts)),
        ],
        compiler_params=pltpu.CompilerParams(
            collective_id=0, has_side_effects=True, vmem_limit_bytes=52 * 1024 * 1024
        ),
    )(*args)
    return pl.pallas_call(
        store_kernel,
        out_shape=out_shape,
        in_specs=[vmem, vmem],
        out_specs=(hbm, hbm),
        scratch_shapes=[dma((5,))],
    )(*(pltpu.with_memory_space_constraint(x, pltpu.VMEM) for x in (updated, scores)))


def solution(mesh):
    in_specs = (
        P("anc", "trait", "genome"),
        P("anc", "trait", "genome"),
        P("anc", "genome", None),
        P("anc", "genome"),
        P("anc", "genome"),
        P("anc", None),
        P("anc", None, "genome"),
    )
    out_specs = (P("anc", "trait", "genome"), P("anc", "trait", "genome"))
    return jax.shard_map(
        per_device, mesh=mesh, in_specs=in_specs, out_specs=out_specs, check_vma=False
    )
```

```python
import functools
import math

import jax
import jax.numpy as jnp
from jax import lax
from jax.experimental import pallas as pl
from jax.experimental.pallas import tpu as pltpu
from jax.sharding import PartitionSpec as P

step_size = 0.5
merging = 0.5
epsilon = 1e-06
longest_run = 8192

MESH = pl.DeviceIdType.MESH
F32 = jnp.float32
BF16 = jnp.bfloat16


def step_kernel(
    sizes,
    coef_hbm, sums_hbm, link_hbm, starts_hbm, ids_hbm, weight_hbm, dosage_hbm,
    updated_ref, score_ref,
    coef, sums, link_first, link_second, starts_ref, ids_ref, weight_ref, dosage, ext, field, band, mean, pair_out, pair_low, pair_in,
    proposal, low, row, stats_out, stats_in, side_out, side_in, part_out, part_in,
    coef_sem, load_sem, link_sem, ready,
    halo_send, halo_recv, pair_send, pair_recv, stats_send, stats_recv, side_send, side_recv, part_send, part_recv,
):
    genomes, ancs, traits_n, reach, tile, groups = sizes
    traits_here, snps = coef.shape
    links = (link_first, link_second)
    width = link_first.shape[1]
    tiles = snps // tile
    half = tiles // 2
    persons_per = dosage.shape[0] // genomes
    pairs = genomes // 2
    g = lax.axis_index("genome")
    a = lax.axis_index("anc")
    t = lax.axis_index("trait")
    core, side = lax.rem(a, 2), a // 2
    parity = lax.rem(g, 2)
    even = 1 - 2 * parity
    near, far, back, across = g + even, g + 2 * even, g - 2 * even, g - even

    def in_range(p):
        return jnp.logical_and(p >= 0, p < genomes)

    def genome(p):
        return {"genome": jnp.clip(p, 0, genomes - 1)}

    group_reach = min(-(-longest_run // snps), genomes - 1)
    stat_peers = [
        (d, m) for m in range(traits_n) for d in range(-group_reach, group_reach + 1) if (d, m) != (0, 0)
    ]
    if genomes > 8 or traits_n > 1:
        greet = [(k, m) for m in range(traits_n) for k in range(genomes) if (k, m) != (0, 0)]
    else:
        greet = []

    coef_parts = coef_sem.shape[0]
    part_cols = snps // coef_parts

    def coef_copy(i):
        cols = pl.ds(i * part_cols, part_cols)
        return pltpu.make_async_copy(coef_hbm.at[0, :, cols], coef.at[:, cols], coef_sem.at[i])

    for i in range(coef_parts):
        coef_copy(i).start()
    barrier = pltpu.get_barrier_semaphore()
    if greet:
        for k, m in greet:
            pl.semaphore_signal(
                barrier, inc=1, device_id_type=MESH,
                device_id={"genome": lax.rem(g + k, genomes), "trait": lax.rem(t + m, traits_n)},
            )
        expected = len(greet)
    else:
        pl.semaphore_signal(barrier, inc=1, device_id=genome(near), device_id_type=MESH)
        for peer in (far, back):
            @pl.when(in_range(peer))
            def _(peer=peer):
                pl.semaphore_signal(barrier, inc=1, device_id=genome(peer), device_id_type=MESH)
        expected = 1 + in_range(far).astype(jnp.int32) + in_range(back).astype(jnp.int32)

    @pl.when(core == 0)
    def _():
        pl.semaphore_signal(barrier, inc=1, device_id={"anc": a + 1}, device_id_type=MESH)

    @pl.when(jnp.logical_and(core == 0, side == 1))
    def _():
        pl.semaphore_signal(barrier, inc=1, device_id={"anc": a - 2}, device_id_type=MESH)

    expected = expected + core + (1 - core) * (1 - side)

    load_small = [
        pltpu.make_async_copy(starts_hbm, starts_ref, load_sem.at[0]),
        pltpu.make_async_copy(ids_hbm, ids_ref, load_sem.at[1]),
        pltpu.make_async_copy(weight_hbm, weight_ref, load_sem.at[2]),
    ]
    load_sums = pltpu.make_async_copy(sums_hbm.at[0], sums, load_sem.at[3])
    load_dosage = pltpu.make_async_copy(dosage_hbm.at[0], dosage, load_sem.at[4])

    def link_copy(u):
        return pltpu.make_async_copy(
            link_hbm.at[0, pl.ds(u * tile, tile), :], links[u // half].at[pl.ds(u % half * tile, tile), :],
            link_sem.at[u],
        )

    unit = snps // 16
    far_rows = width - tile - snps
    ahead = 11 * unit
    behind = snps - ahead
    ahead = 11 * unit
    behind = snps - ahead
    own_at = snps + 128
    at_a = [own_at + 2 * snps + 128 + i * (2 * ahead + 128) for i in range(4)]
    at_b = [at_a[3] + 2 * ahead + 128 + i * (2 * behind + 128) for i in range(4)]
    assert at_b[3] + 2 * behind + 128 == field.shape[0] and 13 * unit < far_rows <= 16 * unit
    first_a = (parity * behind, (1 - parity) * behind)
    first_b = ((1 - parity) * ahead, parity * ahead)

    def own_block(u, carry):
        cols = pl.ds(pl.multiple_of(u * tile, tile), tile)
        flat = coef[:, cols].T.astype(BF16)
        ext[reach, cols, :] = flat
        field[pl.ds(pl.multiple_of(own_at + u * tile, unit), tile), :] = flat.astype(F32)
        return carry

    for i in range(coef_parts):
        coef_copy(i).wait()
        if i == coef_parts - 1:
            for load in load_small:
                load.start()
            for u in range(tiles):
                link_copy(u).start()
            load_sums.start()
            load_dosage.start()
        lax.fori_loop(i * tiles // coef_parts, (i + 1) * tiles // coef_parts, own_block, 0, unroll=2)

    pieces = [
        (5 * unit, 6 * unit), (13 * unit, 3 * unit), (0, 5 * unit), (11 * unit, 2 * unit),
        (5 * unit, 6 * unit), (13 * unit, far_rows - 13 * unit),
        (snps - far_rows, ahead + far_rows - snps), (ahead, behind),
    ]

    def piece(p, odd):
        at, size = pieces[p]
        return pl.multiple_of((1 - odd) * at + odd * (snps - at - size), unit), size

    def halo_copy(src_slot, dst_slot, p, odd, peer, send):
        at, size = piece(p, odd)
        rows = pl.ds(at, size)
        return pltpu.make_async_remote_copy(
            src_ref=ext.at[src_slot, rows, :], dst_ref=ext.at[dst_slot, rows, :],
            send_sem=halo_send.at[send], recv_sem=halo_recv.at[dst_slot, p],
            device_id=genome(peer), device_id_type=MESH,
        )

    def near_copy(p):
        return halo_copy(reach, reach - even, p, parity, near, p)

    def back_copy(p):
        return halo_copy(reach, reach + 2 * even, p, parity, back, 4 + p - 2)

    def far_copy(p):
        return halo_copy(reach, reach - 2 * even, p, parity, far, 8 + p - 6)

    def relay_far(p):
        return halo_copy(reach + even, reach - even, p, 1 - parity, far, 10 + p)

    def relay_near(p):
        return halo_copy(reach + 2 * even, reach + even, p, parity, near, 12 + p - 2)

    def arrived(slot, p, odd):
        halo_copy(reach, slot, p, odd, near, 0).wait_recv()

    has_far, has_back = in_range(far), in_range(back)

    pl.semaphore_wait(barrier, expected)

    def send_halo(nears, backs, fars):
        for k in range(4):
            for p in nears[k:k + 1]:
                near_copy(p).start()
            for p in backs[k:k + 1]:
                @pl.when(has_back)
                def _(p=p):
                    back_copy(p).start()
            for p in fars[k:k + 1]:
                @pl.when(has_far)
                def _(p=p):
                    far_copy(p).start()

    other_core = {"anc": a + 1 - 2 * core}
    other_side = {"anc": lax.rem(a + 2, ancs)}
    up_copy = pltpu.make_async_remote_copy(
        src_ref=pair_out, dst_ref=pair_low, send_sem=pair_send.at[0], recv_sem=pair_recv.at[0],
        device_id=other_core, device_id_type=MESH,
    )
    over_copy = pltpu.make_async_remote_copy(
        src_ref=pair_out, dst_ref=pair_in, send_sem=pair_send.at[1], recv_sem=pair_recv.at[1],
        device_id=other_side, device_id_type=MESH,
    )
    down_copy = pltpu.make_async_remote_copy(
        src_ref=mean, dst_ref=mean, send_sem=pair_send.at[2], recv_sem=pair_recv.at[2],
        device_id=other_core, device_id_type=MESH,
    )

    @pl.when(core == 0)
    def _():
        send_halo((0, 2, 1, 3), (2, 3, 4, 5), (6, 7))

        @pl.when(side == 0)
        def _():
            pl.semaphore_signal(ready, inc=1, device_id={"anc": a + 2}, device_id_type=MESH)

    @pl.when(core == 1)
    def _():
        send_halo((0,), (2,), (6,))

        def round_tile(u, carry):
            cols = pl.ds(pl.multiple_of(u * tile, tile), tile)
            pair_out[:, cols] = coef[:, cols].astype(BF16)
            return carry

        lax.fori_loop(0, tiles, round_tile, 0, unroll=2)
        up_copy.start()

    def clear(first, last):
        def part(i, carry):
            at = pl.multiple_of(first + i * unit, unit)
            field[pl.ds(at, unit), :] = jnp.zeros((unit, traits_here), F32)
            return carry

        lax.fori_loop(0, (last - first) // unit, part, 0, unroll=4)

    clear(0, own_at)
    clear(own_at + snps, field.shape[0])

    for i, (d, m) in enumerate(stat_peers):
        @pl.when(jnp.logical_not(in_range(g - d)))
        def _(i=i):
            stats_in[i] = jnp.zeros(stats_in.shape[1:], F32)

    @pl.when(core == 0)
    def _():
        up_copy.wait_recv()

        def add(u, carry):
            cols = pl.ds(pl.multiple_of(u * tile, tile), tile)
            value = coef[:, cols] + pair_low[:, cols].astype(F32)
            mean[:, cols] = value
            pair_out[:, cols] = value.astype(BF16)
            return carry

        lax.fori_loop(0, tiles, add, 0, unroll=2)

        @pl.when(side == 1)
        def _():
            pl.semaphore_wait(ready, 1)

        over_copy.start()

    def pass_on(p):
        if p < 2:
            arrived(reach + even, p, 1 - parity)

            @pl.when(has_far)
            def _():
                relay_far(p).start()
        else:
            @pl.when(has_far)
            def _():
                arrived(reach + 2 * even, p, parity)
                relay_near(p).start()

    def widen(slot, p, same, i):
        at, size = piece(p, parity if same else 1 - parity)
        in_a = p in (0, 2, 4, 6)
        base = at_a[i] - first_a[1 - same] if in_a else at_b[i] - first_b[1 - same]

        def part(k, carry):
            r = pl.multiple_of(at + k * unit, unit)
            field[pl.ds(pl.multiple_of(base + r, unit), unit), :] = ext[slot, pl.ds(r, unit), :].astype(F32)
            return carry

        lax.fori_loop(0, size // unit, part, 0)

    def range_product(link, u, length, first, second=None):
        deep = length + 128
        within = pl.ds(pl.multiple_of(lax.rem(u, half) * tile, tile), tile)
        rows = pl.ds(pl.multiple_of(u * tile, tile), tile)
        begin = starts_ref[0, u] - g * snps + reach * snps
        where, at = first
        if second is not None:
            here = jnp.clip(begin + width - where, 0, 1) * jnp.clip(where + length - begin, 0, 1)
            where = second[0] + here * (where - second[0])
            at = second[1] + here * (at - second[1])
        skip = lax.div(jnp.clip(where - begin, 0, width - deep), 128) * 128
        from_row = at + jnp.clip(begin + skip - where, -deep, length)
        total = jnp.zeros((tile, traits_here), F32)
        for c in range(0, deep, 512):
            step = min(512, deep - c)
            window = field[pl.ds(from_row + c, step), :].astype(BF16)
            total = total + jnp.dot(
                link[within, pl.ds(skip + c, step)], window, preferred_element_type=F32
            )
        return rows, total

    def each_tile(body, parts=(0, 1), unroll=2):
        for i in parts:
            lax.fori_loop(i * half, (i + 1) * half, functools.partial(body, links[i]), 0, unroll=unroll)

    def own_tile(link, u, carry):
        rows, total = range_product(link, u, snps, (reach * snps, own_at))
        band[rows, :] = total
        return carry

    def own_pass(i):
        for u in range(i * half, (i + 1) * half):
            link_copy(u).wait()
        each_tile(own_tile, (i,), unroll=4)

    load_small[0].wait()
    own_pass(0)

    @pl.when(core == 0)
    def _():
        pass_on(0)
        pass_on(2)

    own_pass(1)

    @pl.when(core == 0)
    def _():
        pl.semaphore_signal(ready, inc=1, device_id=other_core, device_id_type=MESH)

    @pl.when(core == 1)
    def _():
        pl.semaphore_wait(ready, 1)
        send_halo((2,), (), ())
        pl.semaphore_wait(ready, 1)
        send_halo((1, 3), (3, 4, 5), (7,))
        pass_on(0)
        pass_on(2)

    def pair_product(link, u, slots_here, i, in_a):
        length, firsts, bases = (ahead, first_a, at_a) if in_a else (behind, first_b, at_b)
        return range_product(
            link, u, length,
            (slots_here[0] * snps + firsts[1], bases[i]), (slots_here[1] * snps + firsts[0], bases[i + 1]),
        )

    beside = (reach + even, reach - 2 * even)
    beyond = (reach - even, reach + 2 * even)

    def add_tile(link, u, carry, slots_here, i, in_a):
        rows, total = pair_product(link, u, slots_here, i, in_a)
        band[rows, :] = band[rows, :] + total
        return carry

    def beside_pass(in_a):
        for p in (0, 2) if in_a else (1, 3):
            widen(beside[0], p, 0, 0)

        @pl.when(has_back)
        def _():
            p = 6 if in_a else 7
            arrived(beside[1], p, parity)
            widen(beside[1], p, 1, 1)

        each_tile(functools.partial(add_tile, slots_here=beside, i=0, in_a=in_a), unroll=4)

    def beyond_ready(in_a):
        @pl.when(has_far)
        def _():
            arrived(beyond[1], 4 if in_a else 5, parity)
            for p in (2, 4) if in_a else (3, 5):
                widen(beyond[1], p, 1, 3)

        @pl.when(has_back)
        def _():
            for p in (0, 2) if in_a else (1, 3):
                arrived(beyond[0], p, 1 - parity)
                widen(beyond[0], p, 0, 2)

    arrived(beside[0], 2, 1 - parity)
    beside_pass(True)
    pass_on(1)
    pass_on(3)

    @pl.when(core == 0)
    def _():
        pl.semaphore_signal(ready, inc=1, device_id=other_core, device_id_type=MESH)

    arrived(beside[0], 3, 1 - parity)
    beside_pass(False)

    @pl.when(core == 0)
    def _():
        over_copy.wait_recv()

        def add(u, carry):
            cols = pl.ds(pl.multiple_of(u * tile, tile), tile)
            mean[:, cols] = (mean[:, cols] + pair_in[:, cols].astype(F32)) / ancs
            return carry

        lax.fori_loop(0, tiles, add, 0, unroll=2)
        down_copy.start()

    @pl.when(core == 1)
    def _():
        down_copy.wait_recv()

    load_sums.wait()
    for load in load_small[1:]:
        load.wait()

    def prepare(u, carry):
        cols = pl.ds(pl.multiple_of(u * tile, tile), tile)
        proposal[:, cols] = (
            (1.0 - step_size - step_size * merging) * coef[:, cols]
            + step_size * sums[:, cols] + (step_size * merging) * mean[:, cols]
        )
        return carry

    lax.fori_loop(0, tiles, prepare, 0, unroll=2)

    lanes = stats_out.shape[1]
    mine = lax.broadcasted_iota(jnp.int32, (groups, snps), 0) == ids_ref[...]
    counts = jnp.sum(jnp.where(mine, 1.0, 0.0), axis=1, keepdims=True)
    on_lane = lax.broadcasted_iota(jnp.int32, (groups, lanes), 0) == lax.broadcasted_iota(
        jnp.int32, (groups, lanes), 1
    )
    stats_out[1:2, :] = jnp.sum(jnp.where(on_lane, counts, 0.0), axis=0, keepdims=True)

    beyond_ready(True)
    each_tile(functools.partial(add_tile, slots_here=beyond, i=2, in_a=True), unroll=4)

    beyond_ready(False)

    def last_tile(link, u, carry):
        rows, total = pair_product(link, u, beyond, 2, False)
        value = proposal[:, rows] - step_size * (band[rows, :] + total).T
        proposal[:, rows] = value
        row[:, rows] = jnp.sum(value * value, axis=0, keepdims=True)
        return carry

    each_tile(last_tile, unroll=4)

    squares = jnp.sum(jnp.where(mine, row[...], 0.0), axis=1, keepdims=True)
    stats_out[0:1, :] = jnp.sum(jnp.where(on_lane, squares, 0.0), axis=0, keepdims=True)

    def stats_copy(i):
        d, m = stat_peers[i]
        return pltpu.make_async_remote_copy(
            src_ref=stats_out, dst_ref=stats_in.at[i],
            send_sem=stats_send.at[i], recv_sem=stats_recv.at[i],
            device_id={**genome(g + d), "trait": lax.rem(t + m, traits_n)}, device_id_type=MESH,
        )

    for i, (d, m) in enumerate(stat_peers):
        @pl.when(in_range(g + d))
        def _(i=i):
            stats_copy(i).start()

    load_dosage.wait()
    for i, (d, m) in enumerate(stat_peers):
        @pl.when(in_range(g - d))
        def _(i=i):
            stats_copy(i).wait_recv()

    stats = stats_out[...]
    for i in range(len(stat_peers)):
        stats = stats + stats_in[i]
    all_squares = stats[0:1, :groups]
    all_counts = stats[1:2, :groups] / traits_n
    threshold = step_size * weight_ref[...] * jnp.sqrt(all_counts * (traits_here * traits_n))
    shrink = jnp.maximum(0.0, 1.0 - threshold / jnp.sqrt(all_squares + epsilon))
    same = lax.broadcasted_iota(jnp.int32, (groups, groups), 0) == lax.broadcasted_iota(
        jnp.int32, (groups, groups), 1
    )
    shrink = jnp.sum(jnp.where(same, shrink, 0.0), axis=1, keepdims=True)
    row[...] = jnp.sum(jnp.where(mine, shrink, 0.0), axis=0, keepdims=True)

    def round_updated(u, carry):
        cols = pl.ds(pl.multiple_of(u * tile, tile), tile)
        low[:, cols] = (proposal[:, cols] * row[:, cols]).astype(BF16)
        return carry

    def keep_updated(u, carry):
        cols = pl.ds(pl.multiple_of(u * tile, tile), tile)
        updated_ref[0, :, cols] = proposal[:, cols] * row[:, cols]
        return carry

    lax.fori_loop(0, tiles, round_updated, 0, unroll=4)

    scale = 1.0 / math.sqrt(snps * genomes)
    own_side, other_side_g = parity, lax.rem(near, 2)

    def pair_at(i):
        here = g // 2
        is_last = jnp.clip(i - (pairs - 2), 0, 1)
        return (1 - is_last) * (i + jnp.clip(i - here + 1, 0, 1)) + is_last * here

    cuts = side_out.shape[1]
    sub = traits_here // cuts
    last_pair = pairs - 1

    def partial(person):
        at = pl.ds(pl.multiple_of(person * persons_per, persons_per), persons_per)
        return lax.dot_general(
            low[...], dosage[at, :], (((1,), (1,)), ((), ())), preferred_element_type=F32
        ) * scale

    def side_copy(i, c):
        return pltpu.make_async_remote_copy(
            src_ref=side_out.at[i, c], dst_ref=side_in.at[i, c],
            send_sem=side_send.at[i, c], recv_sem=side_recv.at[i, c],
            device_id={"genome": near}, device_id_type=MESH,
        )

    def part_copy(i, c):
        to = pair_at(i)
        slot = lax.rem(g // 2 - to + pairs, pairs) - 1
        return pltpu.make_async_remote_copy(
            src_ref=part_out.at[i, c], dst_ref=part_in.at[slot, c],
            send_sem=part_send.at[i, c], recv_sem=part_recv.at[slot, c],
            device_id={"genome": 2 * to + own_side}, device_id_type=MESH,
        )

    def part_arrived(i, c):
        return pltpu.make_async_remote_copy(
            src_ref=part_out.at[i, c], dst_ref=part_in.at[i, c],
            send_sem=part_send.at[i, c], recv_sem=part_recv.at[i, c],
            device_id={"genome": near}, device_id_type=MESH,
        )

    def send_side(i, carry):
        value = partial(2 * pair_at(i) + other_side_g).astype(BF16)
        for c in range(cuts):
            side_out[i, c] = value[c * sub:(c + 1) * sub]
            side_copy(i, c).start()
        return carry

    def send_part(i, carry):
        mine_here = partial(2 * pair_at(i) + own_side)
        for c in range(cuts):
            side_copy(i, c).wait_recv()
            part_out[i, c] = (mine_here[c * sub:(c + 1) * sub] + side_in[i, c].astype(F32)).astype(BF16)
            part_copy(i, c).start()
        return carry

    lax.fori_loop(0, pairs, send_side, 0)
    lax.fori_loop(0, last_pair, send_part, 0)
    lax.fori_loop(0, tiles, keep_updated, 0, unroll=2)

    last = partial(2 * pair_at(last_pair) + own_side)
    for c in range(cuts):
        side_copy(last_pair, c).wait_recv()

        def add_part(k, total, c=c):
            part_arrived(k, c).wait_recv()
            return total + part_in[k, c].astype(F32)

        own_total = last[c * sub:(c + 1) * sub] + side_in[last_pair, c].astype(F32)
        score_ref[0, c * sub:(c + 1) * sub, :] = lax.fori_loop(0, pairs - 1, add_part, own_total)

    for p in range(4):
        near_copy(p).wait_send()

    @pl.when(has_back)
    def _():
        for p in (2, 3, 4, 5):
            back_copy(p).wait_send()

    @pl.when(has_far)
    def _():
        for p in (6, 7):
            far_copy(p).wait_send()
        for p in (0, 1):
            relay_far(p).wait_send()
        for p in (2, 3):
            relay_near(p).wait_send()

    @pl.when(core == 1)
    def _():
        up_copy.wait_send()

    @pl.when(core == 0)
    def _():
        over_copy.wait_send()
        down_copy.wait_send()

    for i, (d, m) in enumerate(stat_peers):
        @pl.when(in_range(g + d))
        def _(i=i):
            stats_copy(i).wait_send()

    def sent_side(i, carry):
        for c in range(cuts):
            side_copy(i, c).wait_send()
        return carry

    def sent_part(i, carry):
        for c in range(cuts):
            part_copy(i, c).wait_send()
        return carry

    lax.fori_loop(0, pairs, sent_side, 0)
    lax.fori_loop(0, pairs - 1, sent_part, 0)


def store_kernel(updated_in, score_in, updated_out, score_out, sem):
    parts = sem.shape[0] - 1
    rows = updated_in.shape[1] // parts
    copies = [pltpu.make_async_copy(score_in, score_out, sem.at[parts])]
    for i in range(parts):
        part = pl.ds(i * rows, rows)
        copies.append(pltpu.make_async_copy(updated_in.at[:, part], updated_out.at[:, part], sem.at[i]))
    for copy in copies:
        copy.start()
    for copy in copies:
        copy.wait()


def per_device(coefficients, sumstats, linkage, band_start, group_ids, group_weight, dosage):
    _, traits_here, snps = coefficients.shape
    width = linkage.shape[2]
    genomes = lax.axis_size("genome")
    ancs = lax.axis_size("anc")
    traits_n = lax.axis_size("trait")
    persons = dosage.shape[1]
    persons_per = persons // genomes
    groups = group_weight.shape[1]
    reach = -(-width // snps)
    assert reach == 2 and genomes % 2 == 0 and coefficients.shape[0] == 1 and ancs == 4
    tile = snps // band_start.shape[1]
    slots = 2 * reach + 1
    pairs = genomes // 2
    field_rows = 11 * snps + 10 * 128
    group_reach = min(-(-longest_run // snps), genomes - 1)
    cuts = 2
    stat_n = (2 * group_reach + 1) * traits_n - 1
    lanes = -(-groups // 128) * 128
    sizes = (genomes, ancs, traits_n, reach, tile, groups)
    hbm = pl.BlockSpec(memory_space=pltpu.HBM)
    vmem = pl.BlockSpec(memory_space=pltpu.VMEM)
    dma = pltpu.SemaphoreType.DMA
    args = (coefficients, sumstats, linkage, band_start, group_ids, group_weight, dosage)
    args = tuple(pltpu.with_memory_space_constraint(x, pltpu.HBM) for x in args)
    out_shape = (
        jax.ShapeDtypeStruct((1, traits_here, snps), F32),
        jax.ShapeDtypeStruct((1, traits_here, persons_per), F32),
    )
    updated, scores = pl.pallas_call(
        functools.partial(step_kernel, sizes),
        out_shape=out_shape,
        in_specs=[hbm] * 7,
        out_specs=(vmem, vmem),
        scratch_shapes=[
            pltpu.VMEM((traits_here, snps), F32),
            pltpu.VMEM((traits_here, snps), F32),
            pltpu.VMEM((snps // 2, width), BF16),
            pltpu.VMEM((snps // 2, width), BF16),
            pltpu.SMEM(band_start.shape, jnp.int32),
            pltpu.VMEM(group_ids.shape, jnp.int32),
            pltpu.VMEM(group_weight.shape, F32),
            pltpu.VMEM((persons, snps), BF16),
            pltpu.VMEM((slots, snps, traits_here), BF16),
            pltpu.VMEM((field_rows, traits_here), F32),
            pltpu.VMEM((snps, traits_here), F32),
            pltpu.VMEM((traits_here, snps), F32),
            pltpu.VMEM((traits_here, snps), BF16),
            pltpu.VMEM((traits_here, snps), BF16),
            pltpu.VMEM((traits_here, snps), BF16),
            pltpu.VMEM((traits_here, snps), F32),
            pltpu.VMEM((traits_here, snps), BF16),
            pltpu.VMEM((1, snps), F32),
            pltpu.VMEM((2, lanes), F32),
            pltpu.VMEM((stat_n, 2, lanes), F32),
            pltpu.VMEM((pairs, cuts, traits_here // cuts, persons_per), BF16),
            pltpu.VMEM((pairs, cuts, traits_here // cuts, persons_per), BF16),
            pltpu.VMEM((pairs - 1, cuts, traits_here // cuts, persons_per), BF16),
            pltpu.VMEM((pairs - 1, cuts, traits_here // cuts, persons_per), BF16),
            dma((4,)), dma((5,)), dma((snps // tile,)), pltpu.SemaphoreType.REGULAR,
            dma((14,)), dma((slots, 8)), dma((3,)), dma((3,)),
            dma((stat_n,)), dma((stat_n,)), dma((pairs, cuts)), dma((pairs, cuts)), dma((pairs - 1, cuts)), dma((pairs - 1, cuts)),
        ],
        compiler_params=pltpu.CompilerParams(
            collective_id=0, has_side_effects=True, vmem_limit_bytes=52 * 1024 * 1024
        ),
    )(*args)
    return pl.pallas_call(
        store_kernel,
        out_shape=out_shape,
        in_specs=[vmem, vmem],
        out_specs=(hbm, hbm),
        scratch_shapes=[dma((2,))],
    )(*(pltpu.with_memory_space_constraint(x, pltpu.VMEM) for x in (updated, scores)))


def solution(mesh):
    in_specs = (
        P("anc", "trait", "genome"),
        P("anc", "trait", "genome"),
        P("anc", "genome", None),
        P("anc", "genome"),
        P("anc", "genome"),
        P("anc", None),
        P("anc", None, "genome"),
    )
    out_specs = (P("anc", "trait", "genome"), P("anc", "trait", "genome"))
    return jax.shard_map(
        per_device, mesh=mesh, in_specs=in_specs, out_specs=out_specs, check_vma=False
    )
```
